8 devices in a mesh: dp: 2 (over z, y), tp: 4 (over x, core).
Axes of the slice: x: 2, y: 2, z: 1, core: 2. Of those that a mesh axis runs over, the one named last changes fastest.
Arguments:
- hidden: bfloat16 [512, 128], P(('dp', 'tp')), parts along dimension 0
- targets: int32 [512], P(('dp', 'tp')), parts along dimension 0
- loss_mask: int32 [512], P(('dp', 'tp')), parts along dimension 0
- ln_params: float32 [2, 128], replicated
- out_embed: bfloat16 [50304, 128], P('tp')
- ln_mom1: float32 [2, 128], replicated
- ln_mom2: float32 [2, 128], replicated
- embed_mom1: float32 [50304, 128], P('tp')
- embed_mom2: float32 [50304, 128], P('tp')
Outputs:
- output 1: float32 [512], P(('dp', 'tp')), parts along dimension 0
- output 2: float32 [2], P('dp'), parts along dimension 0
- output 3: bfloat16 [512, 128], P(('dp', 'tp')), parts along dimension 0
- output 4: float32 [4, 128], P('dp'), parts along dimension 0
- output 5: float32 [4, 128], P('dp'), parts along dimension 0
- output 6: float32 [4, 128], P('dp'), parts along dimension 0
- output 7: bfloat16 [100608, 128], P(('dp', 'tp')), parts along dimension 0
- output 8: float32 [100608, 128], P(('dp', 'tp')), parts along dimension 0
- output 9: float32 [100608, 128], P(('dp', 'tp')), parts along dimension 0
There are 2 independent parts. The reference program is written for one: setup_inputs(seed, part) draws one part's arguments, and reference() takes and returns one part's arrays. A program takes and returns all parts, laid end to end along the dimension named above; an argument that names none is the same for every part.
All inputs are finite; a program needn't handle non-finite values.
Results may differ from the reference program's by a relative error of at most 0.001.
Values are sent between devices in bfloat16 or wider.
A program may use at most 1 GiB of HBM per device.

```python
import math
import jax
import jax.numpy as jnp
from jax import lax

MODEL_DIM = 128
VOCAB_SIZE = 50304
SEQ_LEN = 256
ADAM_STEP = 10
ROW_BLOCK = math.gcd(SEQ_LEN, 256)
NUM_BLOCKS = SEQ_LEN // ROW_BLOCK
LN_EPS = 1e-5
BETA_ONE = 0.9
BETA_TWO = 0.95
ADAM_EPS = 1e-8
LEARN_RATE = 1e-3
WEIGHT_DECAY = 0.1


def setup_inputs(seed: int = 0, part: int = 0) -> dict:
    root_key = jax.random.key(seed)
    shared_keys = jax.random.split(root_key, 6)
    part_keys = jax.random.split(jax.random.fold_in(root_key, part), 4)
    hidden = jax.random.normal(part_keys[0], (SEQ_LEN, MODEL_DIM), jnp.float32).astype(jnp.bfloat16)
    targets = jax.random.randint(part_keys[1], (SEQ_LEN,), 0, VOCAB_SIZE, jnp.int32)
    keep_bits = jax.random.randint(part_keys[2], (SEQ_LEN,), 0, 4, jnp.int32)
    pad_len = jax.random.randint(part_keys[3], (), 0, SEQ_LEN // 4, jnp.int32)
    positions = jnp.arange(SEQ_LEN, dtype=jnp.int32)
    keep_tok = (keep_bits > 0) & (positions < SEQ_LEN - pad_len)
    loss_mask = jnp.where(positions == 0, 1, keep_tok.astype(jnp.int32)).astype(jnp.int32)
    embed_scale = 2.3 * MODEL_DIM ** -0.5
    out_embed = (jax.random.normal(shared_keys[0], (VOCAB_SIZE, MODEL_DIM), jnp.float32) * embed_scale).astype(jnp.bfloat16)
    ln_noise = jax.random.normal(shared_keys[1], (2, MODEL_DIM), jnp.float32)
    ln_params = jnp.stack([1.0 + 0.3 * ln_noise[0], 0.3 * ln_noise[1]])
    valid_est = 0.66 * SEQ_LEN
    embed_grad = (valid_est * VOCAB_SIZE) ** -0.5
    ln_grad = 2.3 * (valid_est * MODEL_DIM) ** -0.5
    ln_mom1 = jax.random.normal(shared_keys[2], (2, MODEL_DIM), jnp.float32) * ln_grad
    ln_mom2 = (0.5 + jax.random.uniform(shared_keys[3], (2, MODEL_DIM), jnp.float32)) * ln_grad ** 2
    embed_mom1 = jax.random.normal(shared_keys[4], (VOCAB_SIZE, MODEL_DIM), jnp.float32) * embed_grad
    embed_mom2 = (0.5 + jax.random.uniform(shared_keys[5], (VOCAB_SIZE, MODEL_DIM), jnp.float32)) * embed_grad ** 2
    return {"hidden": hidden, "targets": targets, "loss_mask": loss_mask, "ln_params": ln_params, "out_embed": out_embed, "ln_mom1": ln_mom1, "ln_mom2": ln_mom2, "embed_mom1": embed_mom1, "embed_mom2": embed_mom2}


def layer_norm(hidden, ln_params):
    rows_f32 = hidden.astype(jnp.float32)
    row_mean = jnp.mean(rows_f32, axis=-1, keepdims=True)
    centered = rows_f32 - row_mean
    row_var = jnp.mean(centered * centered, axis=-1, keepdims=True)
    normed = centered * lax.rsqrt(row_var + LN_EPS)
    return normed * ln_params[0] + ln_params[1]


def adam_step(param_val, grad_val, m_old, v_old, decay_rate):
    m_new = BETA_ONE * m_old + (1.0 - BETA_ONE) * grad_val
    v_new = BETA_TWO * v_old + (1.0 - BETA_TWO) * grad_val * grad_val
    m_hat = m_new / (1.0 - BETA_ONE ** ADAM_STEP)
    v_hat = v_new / (1.0 - BETA_TWO ** ADAM_STEP)
    new_param = param_val - LEARN_RATE * (m_hat / (jnp.sqrt(v_hat) + ADAM_EPS) + decay_rate * param_val)
    return new_param, m_new, v_new


def block_logits(x_block, out_embed):
    return jnp.dot(x_block, out_embed.T, preferred_element_type=jnp.float32)


def reference(hidden, targets, loss_mask, ln_params, out_embed, ln_mom1, ln_mom2, embed_mom1, embed_mom2):
    x_norm, ln_vjp = jax.vjp(layer_norm, hidden, ln_params)
    x_bf = x_norm.astype(jnp.bfloat16)
    mask_f = loss_mask.astype(jnp.float32)
    valid_count = jnp.sum(mask_f)
    vocab_ids = jnp.arange(VOCAB_SIZE, dtype=jnp.int32)
    x_blocks = x_bf.reshape(NUM_BLOCKS, ROW_BLOCK, MODEL_DIM)
    tgt_blocks = targets.reshape(NUM_BLOCKS, ROW_BLOCK)
    scale_blocks = (mask_f / valid_count).reshape(NUM_BLOCKS, ROW_BLOCK)

    def forward_block(block_in):
        x_block, tgt_block = block_in
        logits = block_logits(x_block, out_embed)
        lse_block = jax.nn.logsumexp(logits, axis=-1)
        is_target = vocab_ids[None, :] == tgt_block[:, None]
        tgt_logit = jnp.sum(jnp.where(is_target, logits, 0.0), axis=-1)
        return lse_block, tgt_logit

    lse_blocks, tgt_logits = lax.map(forward_block, (x_blocks, tgt_blocks))
    token_loss = (lse_blocks.reshape(SEQ_LEN) - tgt_logits.reshape(SEQ_LEN)) * mask_f
    mean_loss = (jnp.sum(token_loss) / valid_count).reshape(1)

    def backward_block(d_embed, block_in):
        x_block, tgt_block, lse_block, scale_block = block_in
        logits = block_logits(x_block, out_embed)
        prob_vals = jnp.exp(logits - lse_block[:, None])
        is_target = (vocab_ids[None, :] == tgt_block[:, None]).astype(jnp.float32)
        d_logits = ((prob_vals - is_target) * scale_block[:, None]).astype(jnp.bfloat16)
        d_embed = d_embed + jnp.dot(d_logits.T, x_block, preferred_element_type=jnp.float32)
        d_x = jnp.dot(d_logits, out_embed, preferred_element_type=jnp.float32)
        return d_embed, d_x

    d_embed, d_x = lax.scan(backward_block, jnp.zeros((VOCAB_SIZE, MODEL_DIM), jnp.float32), (x_blocks, tgt_blocks, lse_blocks, scale_blocks))
    d_hidden, d_ln = ln_vjp(d_x.reshape(SEQ_LEN, MODEL_DIM))
    ln_new, ln_mom1_new, ln_mom2_new = adam_step(ln_params, d_ln, ln_mom1, ln_mom2, 0.0)
    embed_f, embed_mom1_new, embed_mom2_new = adam_step(out_embed.astype(jnp.float32), d_embed, embed_mom1, embed_mom2, WEIGHT_DECAY)
    return (token_loss, mean_loss, d_hidden, ln_new, ln_mom1_new, ln_mom2_new, embed_f.astype(jnp.bfloat16), embed_mom1_new, embed_mom2_new)
```

```python
import functools

import jax
import jax.numpy as jnp
from jax import lax
from jax.experimental import pallas as pl
from jax.experimental.pallas import tpu as pltpu
from jax.sharding import PartitionSpec as P

LN_EPS = 1e-5
BETA_ONE = 0.9
BETA_TWO = 0.95
ADAM_EPS = 1e-8
LEARN_RATE = 1e-3
WEIGHT_DECAY = 0.1
ADAM_STEP = 10
LOG2E = 1.4426950408889634
TINY = 1e-37
SUB = 128
MESH = pl.DeviceIdType.MESH
F32 = jnp.float32
BF16 = jnp.bfloat16


def block_plan(rows):
    subs = rows // SUB
    per = next(k for k in (14, 7, 8, 6, 4, 3, 2, 1) if subs % k == 0)
    return subs // per, per, rows - subs * SUB


def adam_const():
    one = 1.0 - BETA_ONE ** ADAM_STEP
    two = 1.0 - BETA_TWO ** ADAM_STEP
    root = two ** 0.5
    return LEARN_RATE * root / one, ADAM_EPS * root


def adam(param, grad, m_old, v_old, decay):
    scale, eps = adam_const()
    m_new = BETA_ONE * m_old + (1.0 - BETA_ONE) * grad
    v_new = BETA_TWO * v_old + ((1.0 - BETA_TWO) * grad) * grad
    root = v_new * lax.rsqrt(v_new + TINY)
    kept = param if decay == 0.0 else (1.0 - LEARN_RATE * decay) * param
    return kept - (scale * m_new) / (root + eps), m_new, v_new


def forward_kernel(n, hid_ref, tgt_ref, msk_ref, ln_ref, lm_ref, lv_ref, e_hbm, m_hbm, v_hbm,
                   e_v, m_v, v_v, dz_v, x_v, tok_o, mean_o, dh_o, ln_o, lmo, lvo,
                   hid_s, tgt_s, msk_s, xhat_s, rstd_s, ebuf, mbuf, et_s, st_tx, st_rx, pk_tx, pk_rx,
                   load_sem, in_send, in_recv, st_send, st_recv, pk_send, pk_recv):
    me = lax.axis_index("tp")
    rows, dim = e_v.shape
    local = hid_ref.shape[0]
    toks = n * local
    nblk, per, tail = block_plan(rows)
    blk = per * SUB

    barrier = pltpu.get_barrier_semaphore()
    for d in range(1, n):
        pl.semaphore_signal(barrier, inc=1, device_id={"tp": lax.rem(me + d, n)}, device_id_type=MESH)
    e_copy = pltpu.make_async_copy(e_hbm, e_v, load_sem.at[0])
    m_copy = pltpu.make_async_copy(m_hbm, m_v, load_sem.at[1])
    v_copy = pltpu.make_async_copy(v_hbm, v_v, load_sem.at[2])
    e_copy.start()
    pl.semaphore_wait(barrier, n - 1)

    gathers = []
    for d in range(1, n):
        for k, (src, dst) in enumerate(((hid_ref, hid_s), (tgt_ref, tgt_s), (msk_ref, msk_s))):
            copy = pltpu.make_async_remote_copy(
                src_ref=src, dst_ref=dst.at[me], send_sem=in_send.at[k, d - 1], recv_sem=in_recv.at[k, d - 1],
                device_id={"tp": lax.rem(me + d, n)}, device_id_type=MESH)
            copy.start()
            gathers.append(copy)
    hid_s[me] = hid_ref[...]
    tgt_s[me] = tgt_ref[...]
    msk_s[me] = msk_ref[...]
    e_copy.wait()
    m_copy.start()
    v_copy.start()

    def turn(base, size):
        et_s[:, pl.ds(base, size)] = e_v[pl.ds(base, size), :].T

    def turn_block(i, carry):
        turn(pl.multiple_of(i * blk, blk), blk)
        return carry

    lax.fori_loop(0, nblk, turn_block, 0)
    if tail:
        turn(nblk * blk, tail)

    for copy in gathers:
        copy.wait_recv()

    hid = hid_s[...].reshape(toks, dim).astype(F32)
    cent = hid - jnp.mean(hid, axis=-1, keepdims=True)
    rstd = lax.rsqrt(jnp.mean(cent * cent, axis=-1, keepdims=True) + LN_EPS)
    xhat = cent * rstd
    x_f = xhat * ln_ref[0:1, :] + ln_ref[1:2, :]
    x_v[...] = x_f.astype(BF16)
    xhat_s[...] = xhat
    rstd_s[...] = jnp.broadcast_to(rstd, (toks, dim))
    tgt = jnp.concatenate([tgt_s[j] for j in range(n)], axis=1)
    msk = jnp.concatenate([msk_s[j] for j in range(n)], axis=1).astype(F32)
    count = jnp.sum(msk, axis=1, keepdims=True)
    scale = msk / count
    rel = tgt - me * rows

    def fwd(base, slot, subs, size, top, total):
        z = lax.dot_general(e_v[pl.ds(base, subs * size), :], x_v[...], (((1,), (1,)), ((), ())),
                            preferred_element_type=F32)
        for k in range(subs):
            zk = z[k * size:(k + 1) * size].reshape(size // 8, 8, toks)
            new = jnp.maximum(top, jnp.max(zk, axis=0))
            ek = jnp.exp2((zk - new[None]) * LOG2E)
            ebuf[pl.ds(base + k * size, size), :] = ek.reshape(size, toks)
            mbuf[slot + k] = new
            total = total * jnp.exp2((top - new) * LOG2E) + jnp.sum(ek, axis=0)
            top = new
        return top, total

    def fwd_block(i, carry):
        return fwd(pl.multiple_of(i * blk, blk), i * per, per, SUB, *carry)

    carry = (jnp.full((8, toks), -jnp.inf, F32), jnp.zeros((8, toks), F32))
    carry = lax.fori_loop(0, nblk, fwd_block, carry)
    if tail:
        carry = fwd(nblk * blk, nblk * per, 1, tail, *carry)
    top8, sum8 = carry
    top = jnp.max(top8, axis=0, keepdims=True)
    total = jnp.sum(sum8 * jnp.exp2((top8 - top) * LOG2E), axis=0, keepdims=True)
    st_tx[0:1, :] = top
    st_tx[1:2, :] = total
    st_rx[me] = st_tx[...]
    stats = []
    for d in range(1, n):
        copy = pltpu.make_async_remote_copy(
            src_ref=st_tx, dst_ref=st_rx.at[me], send_sem=st_send.at[d - 1], recv_sem=st_recv.at[d - 1],
            device_id={"tp": lax.rem(me + d, n)}, device_id_type=MESH)
        copy.start()
        stats.append(copy)

    iota = lax.broadcasted_iota(jnp.int32, (SUB, toks), 0)

    def pick(base, subs, size, acc):
        hot = jnp.concatenate(
            [(iota[:size] == rel - (base + k * size)).astype(F32).astype(BF16) for k in range(subs)], axis=0)
        return acc + jnp.dot(et_s[:, pl.ds(base, subs * size)], hot, preferred_element_type=F32)

    def pick_block(i, acc):
        return pick(pl.multiple_of(i * blk, blk), per, SUB, acc)

    rows_t = lax.fori_loop(0, nblk, pick_block, jnp.zeros((dim, toks), F32))
    if tail:
        rows_t = pick(nblk * blk, 1, tail, rows_t)
    tgt_z = jnp.sum(x_v[...].astype(F32).T * rows_t, axis=0, keepdims=True)
    inside = (rel >= 0) & (rel < rows)
    tgt_z = jnp.where(inside, tgt_z, 0.0)

    for copy in stats:
        copy.wait_recv()
    tops = [st_rx[j, 0:1, :] for j in range(n)]
    top = functools.reduce(jnp.maximum, tops)
    total = sum(st_rx[j, 1:2, :] * jnp.exp2((tops[j] - top) * LOG2E) for j in range(n))
    lse = top + jnp.log(total)
    hot_val = (jnp.exp2((tgt_z - lse) * LOG2E) - 1.0) * scale

    def back(base, slot, subs, size, acc):
        for k in range(subs):
            fac = jnp.exp2((mbuf[slot + k] - lse) * LOG2E) * scale
            ek = ebuf[pl.ds(base + k * size, size), :].reshape(size // 8, 8, toks)
            dz = (ek * fac[None]).reshape(size, toks)
            dz = jnp.where(iota[:size] == rel - (base + k * size), hot_val, dz)
            dz_v[pl.ds(base + k * size, size), :] = dz.astype(BF16)
        return acc + jnp.dot(et_s[:, pl.ds(base, subs * size)], dz_v[pl.ds(base, subs * size), :],
                             preferred_element_type=F32)

    def back_block(i, acc):
        return back(pl.multiple_of(i * blk, blk), i * per, per, SUB, acc)

    dx_t = lax.fori_loop(0, nblk, back_block, jnp.zeros((dim, toks), F32))
    if tail:
        dx_t = back(nblk * blk, nblk * per, 1, tail, dx_t)
    dx = dx_t.T
    xhat = xhat_s[...]
    extra = jnp.concatenate(
        [jnp.sum(dx * xhat, axis=0, keepdims=True), jnp.sum(dx, axis=0, keepdims=True)]
        + [tgt_z[:, c * dim:(c + 1) * dim] for c in range(toks // dim)]
        + [jnp.zeros((6 - toks // dim, dim), F32)], axis=0)
    for j in range(n):
        pk_tx[j, 0:local, :] = dx[j * local:(j + 1) * local]
        pk_tx[j, local:local + 8, :] = extra
    parts = []
    for d in range(1, n):
        peer = lax.rem(me + d, n)
        copy = pltpu.make_async_remote_copy(
            src_ref=pk_tx.at[peer], dst_ref=pk_rx.at[me], send_sem=pk_send.at[d - 1], recv_sem=pk_recv.at[d - 1],
            device_id={"tp": peer}, device_id_type=MESH)
        copy.start()
        parts.append(copy)
    pk_rx[me] = pk_tx[me]
    for copy in parts:
        copy.wait_recv()

    dx = sum(pk_rx[j, 0:local, :] for j in range(n))
    extra = sum(pk_rx[j, local:local + 8, :] for j in range(n))
    tgt_z = jnp.concatenate([extra[2 + c:3 + c] for c in range(toks // dim)], axis=1)
    loss = (lse - tgt_z) * msk
    mean_o[...] = jnp.sum(loss, axis=1, keepdims=True) / count
    tok_o[...] = sum(jnp.where(me == j, loss[:, j * local:(j + 1) * local], 0.0) for j in range(n))
    own = pl.ds(pl.multiple_of(me * local, local), local)
    xhat = xhat_s[own, :]
    dxh = dx * ln_ref[0:1, :]
    dh = rstd_s[own, :] * (dxh - jnp.mean(dxh, axis=-1, keepdims=True)
                           - xhat * jnp.mean(dxh * xhat, axis=-1, keepdims=True))
    dh_o[...] = dh.astype(BF16)
    p_new, m_new, v_new = adam(ln_ref[...], extra[0:2], lm_ref[...], lv_ref[...], 0.0)
    ln_o[...] = p_new
    lmo[...] = m_new
    lvo[...] = v_new
    m_copy.wait()
    v_copy.wait()
    for copy in gathers + stats + parts:
        copy.wait_send()


def update_kernel(e_v, m_v, v_v, dz_v, x_v, *rest):
    small_in, big_out, small_out, (e_s, m_s, v_s, sem, small_sem) = rest[:6], rest[6:9], rest[9:15], rest[15:]
    rows, dim = e_v.shape
    nblk, per, tail = block_plan(rows)
    blk = per * SUB
    smalls = [pltpu.make_async_copy(a, b, small_sem.at[k]) for k, (a, b) in enumerate(zip(small_in, small_out))]
    for copy in smalls:
        copy.start()
    stages = (e_s, m_s, v_s)

    def step(base, size):
        sl = pl.ds(base, size)
        g = jnp.dot(dz_v[sl, :], x_v[...], preferred_element_type=F32)
        p_new, m_new, v_new = adam(e_v[sl, :].astype(F32), g, m_v[sl, :], v_v[sl, :], WEIGHT_DECAY)
        e_s[sl, :] = p_new.astype(BF16)
        m_s[sl, :] = m_new
        v_s[sl, :] = v_new
        for k in range(3):
            pltpu.make_async_copy(stages[k].at[sl], big_out[k].at[sl], sem.at[k]).start()

    def step_block(i, carry):
        step(pl.multiple_of(i * blk, blk), blk)
        return carry

    lax.fori_loop(0, nblk, step_block, 0)
    if tail:
        step(nblk * blk, tail)
    for k in range(3):
        pltpu.make_async_copy(stages[k], big_out[k], sem.at[k]).wait()
    for copy in smalls:
        copy.wait()


def solution(mesh):
    n = mesh.shape["tp"]
    row_spec = P(("dp", "tp"), None)
    tok_spec = P(("dp", "tp"))
    vocab_spec = P("tp", None)
    repl_spec = P()
    part_spec = P("dp", None)
    vmem = pl.BlockSpec(memory_space=pltpu.VMEM)
    anyw = pl.BlockSpec(memory_space=pltpu.HBM)

    def device_step(hidden, targets, loss_mask, ln_params, out_embed, ln_mom1, ln_mom2, embed_mom1, embed_mom2):
        local, dim = hidden.shape
        rows = out_embed.shape[0]
        toks = n * local
        nblk, per, tail = block_plan(rows)
        pad = -(-rows // 128) * 128
        big = [pltpu.VMEM((rows, dim), BF16), pltpu.VMEM((rows, dim), F32), pltpu.VMEM((rows, dim), F32),
               pltpu.VMEM((rows, toks), BF16), pltpu.VMEM((toks, dim), BF16)]
        small = [((1, local), F32), ((1, 1), F32), ((local, dim), BF16), ((2, dim), F32), ((2, dim), F32),
                 ((2, dim), F32)]
        dma = pltpu.SemaphoreType.DMA
        mids = pl.pallas_call(
            functools.partial(forward_kernel, n),
            name="forward",
            out_shape=big + [pltpu.VMEM(*s) for s in small],
            in_specs=[vmem] * 6 + [anyw] * 3,
            out_specs=[vmem] * 11,
            scratch_shapes=[
                pltpu.VMEM((n, local, dim), BF16), pltpu.VMEM((n, 1, local), jnp.int32),
                pltpu.VMEM((n, 1, local), jnp.int32), pltpu.VMEM((toks, dim), F32), pltpu.VMEM((toks, dim), F32),
                pltpu.VMEM((rows, toks), F32), pltpu.VMEM((nblk * per + 1, 8, toks), F32),
                pltpu.VMEM((dim, pad), BF16),
                pltpu.VMEM((2, toks), F32), pltpu.VMEM((n, 2, toks), F32),
                pltpu.VMEM((n, local + 8, dim), F32), pltpu.VMEM((n, local + 8, dim), F32),
                dma((3,)), dma((3, n - 1)), dma((3, n - 1)), dma((n - 1,)), dma((n - 1,)), dma((n - 1,)),
                dma((n - 1,)),
            ],
            compiler_params=pltpu.CompilerParams(
                collective_id=0, has_side_effects=True, vmem_limit_bytes=24 << 20),
        )(hidden, targets.reshape(1, local), loss_mask.reshape(1, local), ln_params, ln_mom1, ln_mom2,
          out_embed, embed_mom1, embed_mom2)
        hbm = lambda shape, dtype: jax.ShapeDtypeStruct(shape, dtype)
        outs = pl.pallas_call(
            update_kernel,
            name="update",
            out_shape=[hbm((rows, dim), BF16), hbm((rows, dim), F32), hbm((rows, dim), F32)]
            + [hbm(*s) for s in small],
            in_specs=[vmem] * 11,
            out_specs=[anyw] * 9,
            scratch_shapes=[pltpu.VMEM((rows, dim), BF16), pltpu.VMEM((rows, dim), F32), pltpu.VMEM((rows, dim), F32),
                            dma((3,)), dma((6,))],
            compiler_params=pltpu.CompilerParams(vmem_limit_bytes=20 << 20),
        )(*[pltpu.with_memory_space_constraint(a, pltpu.VMEM) for a in mids])
        e_new, m_new, v_new, tok, mean, dh, ln_new, lm_new, lv_new = outs
        return (tok.reshape(local), mean.reshape(1), dh, ln_new, lm_new, lv_new, e_new, m_new, v_new)

    return jax.shard_map(device_step, mesh=mesh, in_specs=(row_spec, tok_spec, tok_spec, repl_spec, vocab_spec, repl_spec, repl_spec, vocab_spec, vocab_spec), out_specs=(tok_spec, P("dp"), row_spec, part_spec, part_spec, part_spec, row_spec, row_spec, row_spec), check_vma=False)
```

```python
import functools

import jax
import jax.numpy as jnp
from jax import lax
from jax.experimental import pallas as pl
from jax.experimental.pallas import tpu as pltpu
from jax.sharding import PartitionSpec as P

LN_EPS = 1e-5
BETA_ONE = 0.9
BETA_TWO = 0.95
ADAM_EPS = 1e-8
LEARN_RATE = 1e-3
WEIGHT_DECAY = 0.1
ADAM_STEP = 10
LOG2E = 1.4426950408889634
TINY = 1e-37
SUB = 128
MESH = pl.DeviceIdType.MESH
F32 = jnp.float32
BF16 = jnp.bfloat16


def block_plan(rows):
    subs = rows // SUB
    per = next(k for k in (14, 7, 8, 6, 4, 3, 2, 1) if subs % k == 0)
    return subs // per, per, rows - subs * SUB


def adam_const():
    one = 1.0 - BETA_ONE ** ADAM_STEP
    two = 1.0 - BETA_TWO ** ADAM_STEP
    root = two ** 0.5
    return LEARN_RATE * root / one, ADAM_EPS * root


def adam(param, grad, m_old, v_old, decay):
    scale, eps = adam_const()
    m_new = BETA_ONE * m_old + (1.0 - BETA_ONE) * grad
    v_new = BETA_TWO * v_old + ((1.0 - BETA_TWO) * grad) * grad
    root = v_new * lax.rsqrt(v_new + TINY)
    kept = param if decay == 0.0 else (1.0 - LEARN_RATE * decay) * param
    return kept - (scale * m_new) / (root + eps), m_new, v_new


def forward_kernel(n, hid_hbm, tgt_hbm, msk_hbm, ln_hbm, lm_hbm, lv_hbm, e_hbm, m_hbm, v_hbm,
                   e_v, m_v, v_v, dz_v, x_v, tok_o, mean_o, dh_o, ln_o, lmo, lvo,
                   hid_ref, tgt_ref, msk_ref, ln_ref, lm_ref, lv_ref, hid_s, tgt_s, msk_s, xhat_s, rstd_s, ebuf, mbuf, et_s, st_tx, st_rx, pk_tx, pk_rx,
                   load_sem, in_send, in_recv, st_send, st_recv, pk_send, pk_recv):
    me = lax.axis_index("tp")
    rows, dim = e_v.shape
    local = hid_ref.shape[0]
    toks = n * local
    nblk, per, tail = block_plan(rows)
    blk = per * SUB

    barrier = pltpu.get_barrier_semaphore()
    for d in range(1, n):
        pl.semaphore_signal(barrier, inc=1, device_id={"tp": lax.rem(me + d, n)}, device_id_type=MESH)
    firsts = [pltpu.make_async_copy(a, b, load_sem.at[3 + k]) for k, (a, b) in enumerate((
        (hid_hbm, hid_ref), (tgt_hbm, tgt_ref), (msk_hbm, msk_ref), (ln_hbm, ln_ref), (lm_hbm, lm_ref),
        (lv_hbm, lv_ref)))]
    for copy in firsts:
        copy.start()
    e_copy = pltpu.make_async_copy(e_hbm, e_v, load_sem.at[0])
    m_copy = pltpu.make_async_copy(m_hbm, m_v, load_sem.at[1])
    v_copy = pltpu.make_async_copy(v_hbm, v_v, load_sem.at[2])
    e_copy.start()
    for copy in firsts:
        copy.wait()
    pl.semaphore_wait(barrier, n - 1)

    gathers = []
    for d in range(1, n):
        for k, (src, dst) in enumerate(((hid_ref, hid_s), (tgt_ref, tgt_s), (msk_ref, msk_s))):
            copy = pltpu.make_async_remote_copy(
                src_ref=src, dst_ref=dst.at[me], send_sem=in_send.at[k, d - 1], recv_sem=in_recv.at[k, d - 1],
                device_id={"tp": lax.rem(me + d, n)}, device_id_type=MESH)
            copy.start()
            gathers.append(copy)
    hid_s[me] = hid_ref[...]
    tgt_s[me] = tgt_ref[...]
    msk_s[me] = msk_ref[...]
    e_copy.wait()
    m_copy.start()
    v_copy.start()

    def turn(base, size):
        et_s[:, pl.ds(base, size)] = e_v[pl.ds(base, size), :].T

    def turn_block(i, carry):
        turn(pl.multiple_of(i * blk, blk), blk)
        return carry

    lax.fori_loop(0, nblk, turn_block, 0)
    if tail:
        turn(nblk * blk, tail)

    for copy in gathers:
        copy.wait_recv()

    hid = hid_s[...].reshape(toks, dim).astype(F32)
    cent = hid - jnp.mean(hid, axis=-1, keepdims=True)
    rstd = lax.rsqrt(jnp.mean(cent * cent, axis=-1, keepdims=True) + LN_EPS)
    xhat = cent * rstd
    x_f = xhat * ln_ref[0:1, :] + ln_ref[1:2, :]
    x_v[...] = x_f.astype(BF16)
    xhat_s[...] = xhat
    rstd_s[...] = jnp.broadcast_to(rstd, (toks, dim))
    tgt = jnp.concatenate([tgt_s[j] for j in range(n)], axis=1)
    msk = jnp.concatenate([msk_s[j] for j in range(n)], axis=1).astype(F32)
    count = jnp.sum(msk, axis=1, keepdims=True)
    scale = msk / count
    rel = tgt - me * rows

    def fwd(base, slot, subs, size, top, total):
        z = lax.dot_general(e_v[pl.ds(base, subs * size), :], x_v[...], (((1,), (1,)), ((), ())),
                            preferred_element_type=F32)
        for k in range(subs):
            zk = z[k * size:(k + 1) * size].reshape(size // 8, 8, toks)
            new = jnp.maximum(top, jnp.max(zk, axis=0))
            ek = jnp.exp2((zk - new[None]) * LOG2E)
            ebuf[pl.ds(base + k * size, size), :] = ek.reshape(size, toks)
            mbuf[slot + k] = new
            total = total * jnp.exp2((top - new) * LOG2E) + jnp.sum(ek, axis=0)
            top = new
        return top, total

    def fwd_block(i, carry):
        return fwd(pl.multiple_of(i * blk, blk), i * per, per, SUB, *carry)

    carry = (jnp.full((8, toks), -jnp.inf, F32), jnp.zeros((8, toks), F32))
    carry = lax.fori_loop(0, nblk, fwd_block, carry)
    if tail:
        carry = fwd(nblk * blk, nblk * per, 1, tail, *carry)
    top8, sum8 = carry
    top = jnp.max(top8, axis=0, keepdims=True)
    total = jnp.sum(sum8 * jnp.exp2((top8 - top) * LOG2E), axis=0, keepdims=True)
    st_tx[0:1, :] = top
    st_tx[1:2, :] = total
    st_rx[me] = st_tx[...]
    stats = []
    for d in range(1, n):
        copy = pltpu.make_async_remote_copy(
            src_ref=st_tx, dst_ref=st_rx.at[me], send_sem=st_send.at[d - 1], recv_sem=st_recv.at[d - 1],
            device_id={"tp": lax.rem(me + d, n)}, device_id_type=MESH)
        copy.start()
        stats.append(copy)

    iota = lax.broadcasted_iota(jnp.int32, (SUB, toks), 0)

    def pick(base, subs, size, acc):
        hot = jnp.concatenate(
            [(iota[:size] == rel - (base + k * size)).astype(F32).astype(BF16) for k in range(subs)], axis=0)
        return acc + jnp.dot(et_s[:, pl.ds(base, subs * size)], hot, preferred_element_type=F32)

    def pick_block(i, acc):
        return pick(pl.multiple_of(i * blk, blk), per, SUB, acc)

    rows_t = lax.fori_loop(0, nblk, pick_block, jnp.zeros((dim, toks), F32))
    if tail:
        rows_t = pick(nblk * blk, 1, tail, rows_t)
    tgt_z = jnp.sum(x_v[...].astype(F32).T * rows_t, axis=0, keepdims=True)
    inside = (rel >= 0) & (rel < rows)
    tgt_z = jnp.where(inside, tgt_z, 0.0)

    for copy in stats:
        copy.wait_recv()
    tops = [st_rx[j, 0:1, :] for j in range(n)]
    top = functools.reduce(jnp.maximum, tops)
    total = sum(st_rx[j, 1:2, :] * jnp.exp2((tops[j] - top) * LOG2E) for j in range(n))
    lse = top + jnp.log(total)
    hot_val = (jnp.exp2((tgt_z - lse) * LOG2E) - 1.0) * scale

    def back(base, slot, subs, size, acc):
        for k in range(subs):
            fac = jnp.exp2((mbuf[slot + k] - lse) * LOG2E) * scale
            ek = ebuf[pl.ds(base + k * size, size), :].reshape(size // 8, 8, toks)
            dz = (ek * fac[None]).reshape(size, toks)
            dz = jnp.where(iota[:size] == rel - (base + k * size), hot_val, dz)
            dz_v[pl.ds(base + k * size, size), :] = dz.astype(BF16)
        return acc + jnp.dot(et_s[:, pl.ds(base, subs * size)], dz_v[pl.ds(base, subs * size), :],
                             preferred_element_type=F32)

    def back_block(i, acc):
        return back(pl.multiple_of(i * blk, blk), i * per, per, SUB, acc)

    dx_t = lax.fori_loop(0, nblk, back_block, jnp.zeros((dim, toks), F32))
    if tail:
        dx_t = back(nblk * blk, nblk * per, 1, tail, dx_t)
    dx = dx_t.T
    xhat = xhat_s[...]
    extra = jnp.concatenate(
        [jnp.sum(dx * xhat, axis=0, keepdims=True), jnp.sum(dx, axis=0, keepdims=True)]
        + [tgt_z[:, c * dim:(c + 1) * dim] for c in range(toks // dim)]
        + [jnp.zeros((6 - toks // dim, dim), F32)], axis=0)
    for j in range(n):
        pk_tx[j, 0:local, :] = dx[j * local:(j + 1) * local]
        pk_tx[j, local:local + 8, :] = extra
    parts = []
    for d in range(1, n):
        peer = lax.rem(me + d, n)
        copy = pltpu.make_async_remote_copy(
            src_ref=pk_tx.at[peer], dst_ref=pk_rx.at[me], send_sem=pk_send.at[d - 1], recv_sem=pk_recv.at[d - 1],
            device_id={"tp": peer}, device_id_type=MESH)
        copy.start()
        parts.append(copy)
    pk_rx[me] = pk_tx[me]
    for copy in parts:
        copy.wait_recv()

    dx = sum(pk_rx[j, 0:local, :] for j in range(n))
    extra = sum(pk_rx[j, local:local + 8, :] for j in range(n))
    tgt_z = jnp.concatenate([extra[2 + c:3 + c] for c in range(toks // dim)], axis=1)
    loss = (lse - tgt_z) * msk
    mean_o[...] = jnp.sum(loss, axis=1, keepdims=True) / count
    tok_o[...] = sum(jnp.where(me == j, loss[:, j * local:(j + 1) * local], 0.0) for j in range(n))
    own = pl.ds(pl.multiple_of(me * local, local), local)
    xhat = xhat_s[own, :]
    dxh = dx * ln_ref[0:1, :]
    dh = rstd_s[own, :] * (dxh - jnp.mean(dxh, axis=-1, keepdims=True)
                           - xhat * jnp.mean(dxh * xhat, axis=-1, keepdims=True))
    dh_o[...] = dh.astype(BF16)
    p_new, m_new, v_new = adam(ln_ref[...], extra[0:2], lm_ref[...], lv_ref[...], 0.0)
    ln_o[...] = p_new
    lmo[...] = m_new
    lvo[...] = v_new
    m_copy.wait()
    v_copy.wait()
    for copy in gathers + stats + parts:
        copy.wait_send()


def update_kernel(e_v, m_v, v_v, dz_v, x_v, *rest):
    small_in, big_out, small_out, (e_s, m_s, v_s, sem, small_sem) = rest[:6], rest[6:9], rest[9:15], rest[15:]
    rows, dim = e_v.shape
    nblk, per, tail = block_plan(rows)
    blk = per * SUB
    smalls = [pltpu.make_async_copy(a, b, small_sem.at[k]) for k, (a, b) in enumerate(zip(small_in, small_out))]
    for copy in smalls:
        copy.start()
    stages = (e_s, m_s, v_s)

    def step(base, size):
        sl = pl.ds(base, size)
        g = jnp.dot(dz_v[sl, :], x_v[...], preferred_element_type=F32)
        p_new, m_new, v_new = adam(e_v[sl, :].astype(F32), g, m_v[sl, :], v_v[sl, :], WEIGHT_DECAY)
        e_s[sl, :] = p_new.astype(BF16)
        m_s[sl, :] = m_new
        v_s[sl, :] = v_new
        for k in range(3):
            pltpu.make_async_copy(stages[k].at[sl], big_out[k].at[sl], sem.at[k]).start()

    def step_block(i, carry):
        step(pl.multiple_of(i * blk, blk), blk)
        return carry

    lax.fori_loop(0, nblk, step_block, 0)
    if tail:
        step(nblk * blk, tail)
    for k in range(3):
        pltpu.make_async_copy(stages[k], big_out[k], sem.at[k]).wait()
    for copy in smalls:
        copy.wait()


def solution(mesh):
    n = mesh.shape["tp"]
    row_spec = P(("dp", "tp"), None)
    tok_spec = P(("dp", "tp"))
    vocab_spec = P("tp", None)
    repl_spec = P()
    part_spec = P("dp", None)
    vmem = pl.BlockSpec(memory_space=pltpu.VMEM)
    anyw = pl.BlockSpec(memory_space=pltpu.HBM)

    def device_step(hidden, targets, loss_mask, ln_params, out_embed, ln_mom1, ln_mom2, embed_mom1, embed_mom2):
        local, dim = hidden.shape
        rows = out_embed.shape[0]
        toks = n * local
        nblk, per, tail = block_plan(rows)
        pad = -(-rows // 128) * 128
        big = [pltpu.VMEM((rows, dim), BF16), pltpu.VMEM((rows, dim), F32), pltpu.VMEM((rows, dim), F32),
               pltpu.VMEM((rows, toks), BF16), pltpu.VMEM((toks, dim), BF16)]
        small = [((1, local), F32), ((1, 1), F32), ((local, dim), BF16), ((2, dim), F32), ((2, dim), F32),
                 ((2, dim), F32)]
        dma = pltpu.SemaphoreType.DMA
        mids = pl.pallas_call(
            functools.partial(forward_kernel, n),
            name="forward",
            out_shape=big + [pltpu.VMEM(*s) for s in small],
            in_specs=[anyw] * 9,
            out_specs=[vmem] * 11,
            scratch_shapes=[
                pltpu.VMEM((local, dim), BF16), pltpu.VMEM((1, local), jnp.int32), pltpu.VMEM((1, local), jnp.int32),
                pltpu.VMEM((2, dim), F32), pltpu.VMEM((2, dim), F32), pltpu.VMEM((2, dim), F32),
                pltpu.VMEM((n, local, dim), BF16), pltpu.VMEM((n, 1, local), jnp.int32),
                pltpu.VMEM((n, 1, local), jnp.int32), pltpu.VMEM((toks, dim), F32), pltpu.VMEM((toks, dim), F32),
                pltpu.VMEM((rows, toks), F32), pltpu.VMEM((nblk * per + 1, 8, toks), F32),
                pltpu.VMEM((dim, pad), BF16),
                pltpu.VMEM((2, toks), F32), pltpu.VMEM((n, 2, toks), F32),
                pltpu.VMEM((n, local + 8, dim), F32), pltpu.VMEM((n, local + 8, dim), F32),
                dma((9,)), dma((3, n - 1)), dma((3, n - 1)), dma((n - 1,)), dma((n - 1,)), dma((n - 1,)),
                dma((n - 1,)),
            ],
            compiler_params=pltpu.CompilerParams(
                collective_id=0, has_side_effects=True, vmem_limit_bytes=24 << 20),
        )(*[pltpu.with_memory_space_constraint(a, pltpu.HBM) for a in (
            hidden, targets.reshape(1, local), loss_mask.reshape(1, local), ln_params, ln_mom1, ln_mom2,
            out_embed, embed_mom1, embed_mom2)])
        hbm = lambda shape, dtype: jax.ShapeDtypeStruct(shape, dtype)
        outs = pl.pallas_call(
            update_kernel,
            name="update",
            out_shape=[hbm((rows, dim), BF16), hbm((rows, dim), F32), hbm((rows, dim), F32)]
            + [hbm(*s) for s in small],
            in_specs=[vmem] * 11,
            out_specs=[anyw] * 9,
            scratch_shapes=[pltpu.VMEM((rows, dim), BF16), pltpu.VMEM((rows, dim), F32), pltpu.VMEM((rows, dim), F32),
                            dma((3,)), dma((6,))],
            compiler_params=pltpu.CompilerParams(vmem_limit_bytes=20 << 20),
        )(*[pltpu.with_memory_space_constraint(a, pltpu.VMEM) for a in mids])
        e_new, m_new, v_new, tok, mean, dh, ln_new, lm_new, lv_new = outs
        return (tok.reshape(local), mean.reshape(1), dh, ln_new, lm_new, lv_new, e_new, m_new, v_new)

    return jax.shard_map(device_step, mesh=mesh, in_specs=(row_spec, tok_spec, tok_spec, repl_spec, vocab_spec, repl_spec, repl_spec, vocab_spec, vocab_spec), out_specs=(tok_spec, P("dp"), row_spec, part_spec, part_spec, part_spec, row_spec, row_spec, row_spec), check_vma=False)
```

```python
import functools

import jax
import jax.numpy as jnp
from jax import lax
from jax.experimental import pallas as pl
from jax.experimental.pallas import tpu as pltpu
from jax.sharding import PartitionSpec as P

LN_EPS = 1e-5
BETA_ONE = 0.9
BETA_TWO = 0.95
ADAM_EPS = 1e-8
LEARN_RATE = 1e-3
WEIGHT_DECAY = 0.1
ADAM_STEP = 10
LOG2E = 1.4426950408889634
TINY = 1e-37
SUB = 128
MESH = pl.DeviceIdType.MESH
F32 = jnp.float32
BF16 = jnp.bfloat16


def block_plan(rows):
    subs = rows // SUB
    per = next(k for k in (14, 7, 8, 6, 4, 3, 2, 1) if subs % k == 0)
    return subs // per, per, rows - subs * SUB


def adam_const():
    one = 1.0 - BETA_ONE ** ADAM_STEP
    two = 1.0 - BETA_TWO ** ADAM_STEP
    root = two ** 0.5
    return LEARN_RATE * root / one, ADAM_EPS * root


def adam(param, grad, m_old, v_old, decay):
    scale, eps = adam_const()
    m_new = BETA_ONE * m_old + (1.0 - BETA_ONE) * grad
    v_new = BETA_TWO * v_old + ((1.0 - BETA_TWO) * grad) * grad
    root = v_new * lax.rsqrt(v_new + TINY)
    kept = param if decay == 0.0 else (1.0 - LEARN_RATE * decay) * param
    return kept - (scale * m_new) / (root + eps), m_new, v_new


def forward_kernel(n, hid_hbm, tgt_hbm, msk_hbm, ln_hbm, lm_hbm, lv_hbm, e_hbm, m_hbm, v_hbm,
                   e_v, m_v, v_v, dz_v, x_v, xh_o, rs_o, lse_o, msk_o, ln_ref, lm_ref, lv_ref, *rest):
    pks, rest = rest[:n], rest[n:]
    (hid_ref, tgt_ref, msk_ref, hid_s, tgt_s, msk_s, xhat_s, rstd_s, ebuf, mbuf, et_s, st_tx, st_rx, pk_tx,
     load_sem, in_send, in_recv, st_send, st_recv) = rest
    me = lax.axis_index("tp")
    rows, dim = e_v.shape
    local = hid_ref.shape[0]
    toks = n * local
    nblk, per, tail = block_plan(rows)
    blk = per * SUB

    barrier = pltpu.get_barrier_semaphore()
    for d in range(1, n):
        pl.semaphore_signal(barrier, inc=1, device_id={"tp": lax.rem(me + d, n)}, device_id_type=MESH)
    firsts = [pltpu.make_async_copy(a, b, load_sem.at[3 + k]) for k, (a, b) in enumerate((
        (hid_hbm, hid_ref), (tgt_hbm, tgt_ref), (msk_hbm, msk_ref), (ln_hbm, ln_ref), (lm_hbm, lm_ref),
        (lv_hbm, lv_ref)))]
    for copy in firsts:
        copy.start()
    e_copy = pltpu.make_async_copy(e_hbm, e_v, load_sem.at[0])
    m_copy = pltpu.make_async_copy(m_hbm, m_v, load_sem.at[1])
    v_copy = pltpu.make_async_copy(v_hbm, v_v, load_sem.at[2])
    e_copy.start()
    for copy in firsts:
        copy.wait()
    pl.semaphore_wait(barrier, n - 1)

    gathers = []
    for d in range(1, n):
        for k, (src, dst) in enumerate(((hid_ref, hid_s), (tgt_ref, tgt_s), (msk_ref, msk_s))):
            copy = pltpu.make_async_remote_copy(
                src_ref=src, dst_ref=dst.at[me], send_sem=in_send.at[k, d - 1], recv_sem=in_recv.at[k, d - 1],
                device_id={"tp": lax.rem(me + d, n)}, device_id_type=MESH)
            copy.start()
            gathers.append(copy)
    hid_s[me] = hid_ref[...]
    tgt_s[me] = tgt_ref[...]
    msk_s[me] = msk_ref[...]
    e_copy.wait()
    m_copy.start()
    v_copy.start()

    def turn(base, size):
        et_s[:, pl.ds(base, size)] = e_v[pl.ds(base, size), :].T

    def turn_block(i, carry):
        turn(pl.multiple_of(i * blk, blk), blk)
        return carry

    lax.fori_loop(0, nblk, turn_block, 0)
    if tail:
        turn(nblk * blk, tail)

    for copy in gathers:
        copy.wait_recv()

    hid = hid_s[...].reshape(toks, dim).astype(F32)
    cent = hid - jnp.mean(hid, axis=-1, keepdims=True)
    rstd = lax.rsqrt(jnp.mean(cent * cent, axis=-1, keepdims=True) + LN_EPS)
    xhat = cent * rstd
    x_f = xhat * ln_ref[0:1, :] + ln_ref[1:2, :]
    x_v[...] = x_f.astype(BF16)
    xhat_s[...] = xhat
    rstd_s[...] = jnp.broadcast_to(rstd, (toks, dim))
    tgt = jnp.concatenate([tgt_s[j] for j in range(n)], axis=1)
    msk = jnp.concatenate([msk_s[j] for j in range(n)], axis=1).astype(F32)
    count = jnp.sum(msk, axis=1, keepdims=True)
    scale = msk / count
    rel = tgt - me * rows

    def fwd(base, slot, subs, size, top, total):
        z = lax.dot_general(e_v[pl.ds(base, subs * size), :], x_v[...], (((1,), (1,)), ((), ())),
                            preferred_element_type=F32)
        for k in range(subs):
            zk = z[k * size:(k + 1) * size].reshape(size // 8, 8, toks)
            new = jnp.maximum(top, jnp.max(zk, axis=0))
            ek = jnp.exp2((zk - new[None]) * LOG2E)
            ebuf[pl.ds(base + k * size, size), :] = ek.reshape(size, toks)
            mbuf[slot + k] = new
            total = total * jnp.exp2((top - new) * LOG2E) + jnp.sum(ek, axis=0)
            top = new
        return top, total

    def fwd_block(i, carry):
        return fwd(pl.multiple_of(i * blk, blk), i * per, per, SUB, *carry)

    carry = (jnp.full((8, toks), -jnp.inf, F32), jnp.zeros((8, toks), F32))
    for i in range(nblk):
        carry = fwd(i * blk, i * per, per, SUB, *carry)
    if tail:
        carry = fwd(nblk * blk, nblk * per, 1, tail, *carry)
    top8, sum8 = carry
    top = jnp.max(top8, axis=0, keepdims=True)
    total = jnp.sum(sum8 * jnp.exp2((top8 - top) * LOG2E), axis=0, keepdims=True)
    st_tx[0:1, :] = top
    st_tx[1:2, :] = total
    st_rx[me] = st_tx[...]
    stats = []
    for d in range(1, n):
        copy = pltpu.make_async_remote_copy(
            src_ref=st_tx, dst_ref=st_rx.at[me], send_sem=st_send.at[d - 1], recv_sem=st_recv.at[d - 1],
            device_id={"tp": lax.rem(me + d, n)}, device_id_type=MESH)
        copy.start()
        stats.append(copy)

    iota = lax.broadcasted_iota(jnp.int32, (SUB, toks), 0)

    def pick(base, subs, size, acc):
        hot = jnp.concatenate(
            [(iota[:size] == rel - (base + k * size)).astype(F32).astype(BF16) for k in range(subs)], axis=0)
        return acc + jnp.dot(et_s[:, pl.ds(base, subs * size)], hot, preferred_element_type=F32)

    def pick_block(i, acc):
        return pick(pl.multiple_of(i * blk, blk), per, SUB, acc)

    rows_t = lax.fori_loop(0, nblk, pick_block, jnp.zeros((dim, toks), F32))
    if tail:
        rows_t = pick(nblk * blk, 1, tail, rows_t)
    tgt_z = jnp.sum(x_v[...].astype(F32).T * rows_t, axis=0, keepdims=True)
    inside = (rel >= 0) & (rel < rows)
    tgt_z = jnp.where(inside, tgt_z, 0.0)

    for copy in stats:
        copy.wait_recv()
    tops = [st_rx[j, 0:1, :] for j in range(n)]
    top = functools.reduce(jnp.maximum, tops)
    total = sum(st_rx[j, 1:2, :] * jnp.exp2((tops[j] - top) * LOG2E) for j in range(n))
    lse = top + jnp.log(total)
    hot_val = (jnp.exp2((tgt_z - lse) * LOG2E) - 1.0) * scale

    hot16 = jnp.broadcast_to(hot_val, (16, toks)).astype(BF16)[None]
    zero = jnp.zeros((16, toks), jnp.int32)
    iota16 = lax.broadcasted_iota(jnp.int32, (SUB, toks), 0).astype(jnp.int16).reshape(SUB // 16, 16, toks)
    near = jnp.where(inside, rel, -15000)

    def back(base, slot, subs, size, acc):
        vals = []
        for k in range(subs):
            fac = jnp.exp2((mbuf[slot + k] - lse) * LOG2E) * scale
            ek = ebuf[pl.ds(base + k * size, size), :].reshape(size // 8, 8, toks)
            dz = (ek * fac[None]).reshape(size // 16, 16, toks).astype(BF16)
            here = (zero + (near - (base + k * size))).astype(jnp.int16)[None]
            dz = jnp.where(iota16[:size // 16] == here, hot16, dz).reshape(size, toks)
            dz_v[pl.ds(base + k * size, size), :] = dz
            vals.append(dz)
            if len(vals) * size == 256 or k == subs - 1:
                done = (k + 1 - len(vals)) * size
                acc = acc + jnp.dot(et_s[:, pl.ds(base + done, len(vals) * size)], jnp.concatenate(vals, axis=0),
                                    preferred_element_type=F32)
                vals = []
        return acc

    def back_block(i, acc):
        return back(pl.multiple_of(i * blk, blk), i * per, per, SUB, acc)

    dx_t = jnp.zeros((dim, toks), F32)
    for i in range(nblk):
        dx_t = back(i * blk, i * per, per, SUB, dx_t)
    if tail:
        dx_t = back(nblk * blk, nblk * per, 1, tail, dx_t)
    dx = dx_t.T
    xhat = xhat_s[...]
    extra = jnp.concatenate(
        [jnp.sum(dx * xhat, axis=0, keepdims=True), jnp.sum(dx, axis=0, keepdims=True)]
        + [tgt_z[:, c * dim:(c + 1) * dim] for c in range(toks // dim)]
        + [jnp.zeros((6 - toks // dim, dim), F32)], axis=0)
    for j in range(n):
        pk_tx[j, 0:local, :] = dx[j * local:(j + 1) * local]
        pk_tx[j, local:local + 8, :] = extra
    own = pl.ds(pl.multiple_of(me * local, local), local)
    xh_o[...] = xhat_s[own, :]
    rs_o[...] = rstd_s[own, :]
    lse_o[...] = lse
    msk_o[...] = msk
    for d in range(n):
        pks[d][...] = pk_tx[lax.rem(me + d, n)]
    m_copy.wait()
    v_copy.wait()
    for copy in gathers + stats:
        copy.wait_send()


def update_kernel(e_v, m_v, v_v, dz_v, x_v, *rest):
    big_out, (e_s, m_s, v_s, sem) = rest[:3], rest[3:]
    rows, dim = e_v.shape
    nblk, per, tail = block_plan(rows)
    blk = per * SUB
    stages = (e_s, m_s, v_s)

    def step(base, size):
        sl = pl.ds(base, size)
        g = jnp.dot(dz_v[sl, :], x_v[...], preferred_element_type=F32)
        p_new, m_new, v_new = adam(e_v[sl, :].astype(F32), g, m_v[sl, :], v_v[sl, :], WEIGHT_DECAY)
        e_s[sl, :] = p_new.astype(BF16)
        m_s[sl, :] = m_new
        v_s[sl, :] = v_new
        for k in range(3):
            pltpu.make_async_copy(stages[k].at[sl], big_out[k].at[sl], sem.at[k]).start()

    def step_block(i, carry):
        step(pl.multiple_of(i * blk, blk), blk)
        return carry

    lax.fori_loop(0, nblk, step_block, 0)
    if tail:
        step(nblk * blk, tail)
    for k in range(3):
        pltpu.make_async_copy(stages[k], big_out[k], sem.at[k]).wait()


def finish_kernel(n, xh_ref, rs_ref, lse_ref, msk_ref, ln_ref, lm_ref, lv_ref, *rest):
    pks, (tok_o, mean_o, dh_o, ln_o, lmo, lvo, pk_rx) = rest[:n], rest[n:]
    me = lax.axis_index("tp")
    local, dim = xh_ref.shape
    toks = n * local
    for d in range(n):
        pk_rx[lax.rem(me - d + n, n)] = pks[d][...]
    dx = sum(pk_rx[j, 0:local, :] for j in range(n))
    extra = sum(pk_rx[j, local:local + 8, :] for j in range(n))
    tgt_z = jnp.concatenate([extra[2 + c:3 + c] for c in range(toks // dim)], axis=1)
    msk = msk_ref[...]
    loss = (lse_ref[...] - tgt_z) * msk
    mean_o[...] = jnp.sum(loss, axis=1, keepdims=True) / jnp.sum(msk, axis=1, keepdims=True)
    tok_o[...] = sum(jnp.where(me == j, loss[:, j * local:(j + 1) * local], 0.0) for j in range(n))
    xhat = xh_ref[...]
    dxh = dx * ln_ref[0:1, :]
    dh = rs_ref[...] * (dxh - jnp.mean(dxh, axis=-1, keepdims=True)
                        - xhat * jnp.mean(dxh * xhat, axis=-1, keepdims=True))
    dh_o[...] = dh.astype(BF16)
    p_new, m_new, v_new = adam(ln_ref[...], extra[0:2], lm_ref[...], lv_ref[...], 0.0)
    ln_o[...] = p_new
    lmo[...] = m_new
    lvo[...] = v_new


def solution(mesh):
    n = mesh.shape["tp"]
    row_spec = P(("dp", "tp"), None)
    tok_spec = P(("dp", "tp"))
    vocab_spec = P("tp", None)
    repl_spec = P()
    part_spec = P("dp", None)
    vmem = pl.BlockSpec(memory_space=pltpu.VMEM)
    anyw = pl.BlockSpec(memory_space=pltpu.HBM)

    def device_step(hidden, targets, loss_mask, ln_params, out_embed, ln_mom1, ln_mom2, embed_mom1, embed_mom2):
        local, dim = hidden.shape
        rows = out_embed.shape[0]
        toks = n * local
        nblk, per, tail = block_plan(rows)
        pad = -(-rows // 128) * 128
        big = [pltpu.VMEM((rows, dim), BF16), pltpu.VMEM((rows, dim), F32), pltpu.VMEM((rows, dim), F32),
               pltpu.VMEM((rows, toks), BF16), pltpu.VMEM((toks, dim), BF16)]
        mid = [((local, dim), F32), ((local, dim), F32), ((1, toks), F32), ((1, toks), F32), ((2, dim), F32),
               ((2, dim), F32), ((2, dim), F32)]
        small = [((1, local), F32), ((1, 1), F32), ((local, dim), BF16), ((2, dim), F32), ((2, dim), F32),
                 ((2, dim), F32)]
        pack = [((local + 8, dim), F32)] * n
        dma = pltpu.SemaphoreType.DMA
        hbm = lambda shape, dtype: jax.ShapeDtypeStruct(shape, dtype)
        mids = pl.pallas_call(
            functools.partial(forward_kernel, n),
            name="forward",
            out_shape=big + [pltpu.VMEM(*s) for s in mid] + [hbm(*s) for s in pack],
            in_specs=[anyw] * 9,
            out_specs=[vmem] * (12 + n),
            scratch_shapes=[
                pltpu.VMEM((local, dim), BF16), pltpu.VMEM((1, local), jnp.int32), pltpu.VMEM((1, local), jnp.int32),
                pltpu.VMEM((n, local, dim), BF16), pltpu.VMEM((n, 1, local), jnp.int32),
                pltpu.VMEM((n, 1, local), jnp.int32), pltpu.VMEM((toks, dim), F32), pltpu.VMEM((toks, dim), F32),
                pltpu.VMEM((rows, toks), F32), pltpu.VMEM((nblk * per + 1, 8, toks), F32),
                pltpu.VMEM((dim, pad), BF16),
                pltpu.VMEM((2, toks), F32), pltpu.VMEM((n, 2, toks), F32),
                pltpu.VMEM((n, local + 8, dim), F32),
                dma((9,)), dma((3, n - 1)), dma((3, n - 1)), dma((n - 1,)), dma((n - 1,)),
            ],
            compiler_params=pltpu.CompilerParams(
                collective_id=0, has_side_effects=True, vmem_limit_bytes=24 << 20),
        )(*[pltpu.with_memory_space_constraint(a, pltpu.HBM) for a in (
            hidden, targets.reshape(1, local), loss_mask.reshape(1, local), ln_params, ln_mom1, ln_mom2,
            out_embed, embed_mom1, embed_mom2)])
        big_in, mid_in, packs = mids[:5], mids[5:12], mids[12:]
        got = [packs[0]] + [
            lax.ppermute(packs[d], "tp", [(i, (i + d) % n) for i in range(n)]) for d in range(1, n)]
        e_new, m_new, v_new = pl.pallas_call(
            update_kernel,
            name="update",
            out_shape=[hbm((rows, dim), BF16), hbm((rows, dim), F32), hbm((rows, dim), F32)],
            in_specs=[vmem] * 5,
            out_specs=[anyw] * 3,
            scratch_shapes=[pltpu.VMEM((rows, dim), BF16), pltpu.VMEM((rows, dim), F32), pltpu.VMEM((rows, dim), F32),
                            dma((3,))],
            compiler_params=pltpu.CompilerParams(vmem_limit_bytes=20 << 20),
            cost_estimate=pl.CostEstimate(flops=50_000_000_000, bytes_accessed=32_000_000, transcendentals=0),
        )(*[pltpu.with_memory_space_constraint(a, pltpu.VMEM) for a in big_in])
        tok, mean, dh, ln_new, lm_new, lv_new = pl.pallas_call(
            functools.partial(finish_kernel, n),
            name="finish",
            out_shape=[hbm(*s) for s in small],
            in_specs=[vmem] * (7 + n),
            out_specs=[vmem] * 6,
            scratch_shapes=[pltpu.VMEM((n, local + 8, dim), F32)],
            compiler_params=pltpu.CompilerParams(vmem_limit_bytes=4 << 20),
        )(*mid_in, *got)
        return (tok.reshape(local), mean.reshape(1), dh, ln_new, lm_new, lv_new, e_new, m_new, v_new)

    return jax.shard_map(device_step, mesh=mesh, in_specs=(row_spec, tok_spec, tok_spec, repl_spec, vocab_spec, repl_spec, repl_spec, vocab_spec, vocab_spec), out_specs=(tok_spec, P("dp"), row_spec, part_spec, part_spec, part_spec, row_spec, row_spec, row_spec), check_vma=False)
```

```python
import functools

import jax
import jax.numpy as jnp
from jax import lax
from jax.experimental import pallas as pl
from jax.experimental.pallas import tpu as pltpu
from jax.sharding import PartitionSpec as P

LN_EPS = 1e-5
BETA_ONE = 0.9
BETA_TWO = 0.95
ADAM_EPS = 1e-8
LEARN_RATE = 1e-3
WEIGHT_DECAY = 0.1
ADAM_STEP = 10
LOG2E = 1.4426950408889634
TINY = 1e-37
SUB = 128
CHUNK = 896
EARLY = 2
DOT = 896
MESH = pl.DeviceIdType.MESH
F32 = jnp.float32
BF16 = jnp.bfloat16


def pair_plan(rows):
    half = rows // 2
    return half, half // SUB, half % SUB


def row_blocks(rows):
    full = rows // CHUNK
    return [(i * CHUNK, CHUNK) for i in range(full)] + ([(full * CHUNK, rows - full * CHUNK)] if rows % CHUNK else [])


def adam_const():
    one = 1.0 - BETA_ONE ** ADAM_STEP
    two = 1.0 - BETA_TWO ** ADAM_STEP
    root = two ** 0.5
    return LEARN_RATE * root / one, ADAM_EPS * root


def adam(param, grad, m_old, v_old, decay):
    scale, eps = adam_const()
    m_new = BETA_ONE * m_old + (1.0 - BETA_ONE) * grad
    v_new = BETA_TWO * v_old + ((1.0 - BETA_TWO) * grad) * grad
    root = v_new * lax.rsqrt(v_new + TINY)
    kept = param if decay == 0.0 else (1.0 - LEARN_RATE * decay) * param
    return kept - (scale * m_new) / (root + eps), m_new, v_new


def adam_rows(base, size, e_in, m_in, v_in, dz_v, x_v, e_out, m_out, v_out, shift):
    sl, to = pl.ds(base, size), pl.ds(base - shift, size)
    g = jnp.dot(dz_v[sl, :], x_v[...], preferred_element_type=F32)
    p_new, m_new, v_new = adam(e_in[sl, :].astype(F32), g, m_in[sl, :], v_in[sl, :], WEIGHT_DECAY)
    e_out[to, :] = p_new.astype(BF16)
    m_out[to, :] = m_new
    v_out[to, :] = v_new


def place():
    me = lax.axis_index("tp")
    side, core = me // 2, lax.rem(me, 2)
    far = 2 - 2 * side
    return me, core, (me + 1 - 2 * core, far + core, far + 1 - core)


def swap(v):
    half = v.shape[1] // 2
    return jnp.concatenate([v[:, half:], v[:, :half]], axis=1)


def forward_kernel(n, hid_hbm, tgt_hbm, msk_hbm, ln_hbm, lm_hbm, lv_hbm, e_hbm, m_hbm, v_hbm,
                   e_v, m_v, v_v, dz_v, x_v, keep_o, away_o, xh_o, rs_o, lse_o, msk_o, ln_ref, lm_ref, lv_ref,
                   hid_ref, tgt_ref, msk_ref, hid_s, tgt_s, msk_s, xhat_s, rstd_s, dx_s, xd_s, ebuf, mbuf, et_s,
                   st_tx, st_rx, pk_tx, pk_rx,
                   load_sem, in_send, in_recv, st_send, st_recv, pk_send, pk_recv):
    me, core, peers = place()
    rows, dim = e_v.shape
    local = hid_ref.shape[0]
    toks = n * local
    wide = toks // 2
    half, subs, tail = pair_plan(rows)
    units = [((i // subs) * half + (i % subs) * SUB, i * SUB, SUB) for i in range(2 * subs)]

    barrier = pltpu.get_barrier_semaphore()
    for peer in peers:
        pl.semaphore_signal(barrier, inc=1, device_id={"tp": peer}, device_id_type=MESH)
    firsts = [pltpu.make_async_copy(a, b, load_sem.at[3 + k]) for k, (a, b) in enumerate((
        (hid_hbm, hid_ref), (tgt_hbm, tgt_ref), (msk_hbm, msk_ref), (ln_hbm, ln_ref), (lm_hbm, lm_ref),
        (lv_hbm, lv_ref)))]
    for copy in firsts:
        copy.start()
    e_copy = pltpu.make_async_copy(e_hbm, e_v, load_sem.at[0])
    m_copy = pltpu.make_async_copy(m_hbm, m_v, load_sem.at[1])
    v_copy = pltpu.make_async_copy(v_hbm, v_v, load_sem.at[2])
    e_copy.start()
    for copy in firsts:
        copy.wait()
    pl.semaphore_wait(barrier, n - 1)

    def send(src, dst, peer, send_sem, recv_sem):
        copy = pltpu.make_async_remote_copy(src_ref=src, dst_ref=dst, send_sem=send_sem, recv_sem=recv_sem,
                                            device_id={"tp": peer}, device_id_type=MESH)
        copy.start()
        return copy

    gathers = []
    for k, (src, dst) in enumerate(((hid_ref, hid_s), (tgt_ref, tgt_s), (msk_ref, msk_s))):
        dst[core] = src[...]
        for r, peer in enumerate(peers):
            gathers.append(send(src, dst.at[2 + core if r else core], peer, in_send.at[k, r], in_recv.at[k, r]))
    xd_s[...] = jnp.zeros(xd_s.shape, BF16)
    e_copy.wait()
    m_copy.start()
    v_copy.start()

    def norm(h):
        lanes = slice(h * wide, (h + 1) * wide)
        hid = hid_s[2 * h:2 * h + 2].reshape(wide, dim).astype(F32)
        cent = hid - jnp.mean(hid, axis=-1, keepdims=True)
        rstd = lax.rsqrt(jnp.mean(cent * cent, axis=-1, keepdims=True) + LN_EPS)
        xhat = cent * rstd
        x_b = (xhat * ln_ref[0:1, :] + ln_ref[1:2, :]).astype(BF16)
        x_v[lanes, :] = x_b
        x_t = x_b.T
        xd_s[h, 0:dim, 0:wide] = x_t
        xd_s[h, dim:2 * dim, wide:2 * wide] = x_t
        xhat_s[lanes, :] = xhat
        rstd_s[lanes, :] = jnp.broadcast_to(rstd, (wide, dim))

    def forward(h):
        top = jnp.full((8, toks), -jnp.inf, F32)
        total = jnp.zeros((8, toks), F32)
        for first in range(0, half, DOT):
            span = min(DOT, half - first)
            pair = jnp.concatenate([e_v[pl.ds(first, span), :], e_v[pl.ds(half + first, span), :]], axis=1)
            z = jnp.dot(pair, xd_s[h], preferred_element_type=F32)
            for k in range(0, span, SUB):
                size = min(SUB, span - k)
                zk = z[k:k + size].reshape(size // 8, 8, toks)
                new = jnp.maximum(top, jnp.max(zk, axis=0))
                ek = jnp.exp2((zk - new[None]) * LOG2E)
                ebuf[h, pl.ds(first + k, size), :] = ek.reshape(size, toks)
                mbuf[h, (first + k) // SUB] = new
                total = total * jnp.exp2((top - new) * LOG2E) + jnp.sum(ek, axis=0)
                top = new
        peak = jnp.max(top, axis=0, keepdims=True)
        peak = jnp.maximum(peak[:, :wide], peak[:, wide:])
        peak2 = jnp.concatenate([peak, peak], axis=1)
        total = jnp.sum(total * jnp.exp2((top - peak2) * LOG2E), axis=0, keepdims=True)
        st_tx[0:1, h * wide:(h + 1) * wide] = peak
        st_tx[1:2, h * wide:(h + 1) * wide] = total[:, :wide] + total[:, wide:]

    gathers[0].wait_recv()
    norm(0)
    forward(0)
    for copy in gathers[1:]:
        copy.wait_recv()
    norm(1)
    forward(1)
    stats = [send(st_tx, st_rx.at[r], peer, st_send.at[r], st_recv.at[r]) for r, peer in enumerate(peers)]

    tgt = jnp.concatenate([tgt_s[j] for j in range(n)], axis=1)
    msk = jnp.concatenate([msk_s[j] for j in range(n)], axis=1).astype(F32)
    count = jnp.sum(msk, axis=1, keepdims=True)
    scale = msk / count
    rel = tgt - me * rows
    inside = (rel >= 0) & (rel < rows)
    near = jnp.where(inside, rel, -15000)
    for low, col, size in units:
        et_s[:, pl.ds(col, size)] = e_v[pl.ds(low, size), :].T
    ends = [h * half + subs * SUB for h in range(2)]
    if tail:
        et_s[:, pl.ds(2 * subs * SUB, 2 * tail)] = jnp.concatenate([e_v[pl.ds(low, tail), :] for low in ends], axis=0).T

    flat = jnp.zeros((16, toks), jnp.int32)
    iota16 = lax.broadcasted_iota(jnp.int32, (SUB, toks), 0).astype(jnp.int16).reshape(SUB // 16, 16, toks)

    def hit(low, size):
        return iota16[:size // 16] == (flat + (near - low)).astype(jnp.int16)[None]

    def gather_sum(value):
        accs = [jnp.zeros((dim, toks), F32)] * 2
        groups = [units[i:i + 2] for i in range(0, len(units), 2)]
        if tail:
            groups.append([(low, 2 * subs * SUB + h * tail, tail) for h, low in enumerate(ends)])
        for i, group in enumerate(groups):
            vals = jnp.concatenate([value(low, size) for low, _, size in group], axis=0)
            accs[i % 2] = accs[i % 2] + jnp.dot(et_s[:, pl.ds(group[0][1], vals.shape[0])], vals,
                                                preferred_element_type=F32)
        return accs[0] - accs[1] * -1.0

    ones, none = jnp.ones((1, 16, toks), BF16), jnp.zeros((1, 16, toks), BF16)
    rows_t = gather_sum(lambda low, size: jnp.where(hit(low, size), ones, none).reshape(size, toks))
    tgt_z = jnp.sum(x_v[...].astype(F32).T * rows_t, axis=0, keepdims=True)
    tgt_z = jnp.where(inside, tgt_z, 0.0)

    for copy in stats:
        copy.wait_recv()
    both = [st_tx[...], st_rx[0], swap(st_rx[1]), swap(st_rx[2])]
    peak = jnp.maximum(jnp.maximum(both[0][0:1], both[1][0:1]), jnp.maximum(both[2][0:1], both[3][0:1]))
    sums = [v[1:2] * jnp.exp2((v[0:1] - peak) * LOG2E) for v in both]
    lse = peak + jnp.log((sums[0] + sums[1]) + (sums[2] + sums[3]))
    hot_val = (jnp.exp2((tgt_z - lse) * LOG2E) - 1.0) * scale
    hot16 = jnp.broadcast_to(hot_val, (16, toks)).astype(BF16)[None]

    def grads(low, size):
        h, first = low // half, low % half
        sides = slice(h * wide, (h + 1) * wide)
        seen = jnp.concatenate([mbuf[c, first // SUB, :, sides] for c in range(2)], axis=1)
        fac = jnp.exp2((seen - lse) * LOG2E) * scale
        ek = jnp.concatenate([ebuf[c, pl.ds(first, size), sides] for c in range(2)], axis=1)
        dz = (ek.reshape(size // 8, 8, toks) * fac[None]).reshape(size // 16, 16, toks).astype(BF16)
        dz = jnp.where(hit(low, size), hot16, dz).reshape(size, toks)
        dz_v[pl.ds(low, size), :] = dz
        return dz

    dx = gather_sum(grads).T
    extra = jnp.concatenate(
        [jnp.sum(dx * xhat_s[...], axis=0, keepdims=True), jnp.sum(dx, axis=0, keepdims=True)]
        + [tgt_z[:, c * dim:(c + 1) * dim] for c in range(toks // dim)]
        + [jnp.zeros((6 - toks // dim, dim), F32)], axis=0)
    dx_s[...] = dx
    for c in range(2):
        pk_tx[c, 0:local, :] = dx_s[pl.ds(pl.multiple_of(c * wide + (1 - core) * local, local), local), :]
        pk_tx[c, local:local + 8, :] = extra
    part = send(pk_tx, pk_rx, peers[0], pk_send, pk_recv)

    own = pl.ds(pl.multiple_of(core * local, local), local)
    xh_o[...] = xhat_s[own, :]
    rs_o[...] = rstd_s[own, :]
    msk_o[...] = msk
    lse_o[...] = lse
    m_copy.wait()
    v_copy.wait()
    for base, size in row_blocks(rows)[:EARLY]:
        adam_rows(base, size, e_v, m_v, v_v, dz_v, x_v, e_v, m_v, v_v, 0)

    part.wait_recv()
    for c, out in enumerate((keep_o, away_o)):
        mine = pl.ds(pl.multiple_of(c * wide + core * local, local), local)
        out[0:local, :] = dx_s[mine, :] + pk_rx[c, 0:local, :]
        out[local:local + 8, :] = extra + pk_rx[c, local:local + 8, :]
    for copy in gathers + stats + [part]:
        copy.wait_send()


def update_kernel(e_v, m_v, v_v, dz_v, x_v, e_o, m_o, v_o, e_s, m_s, v_s, sem):
    rows = e_v.shape[0]
    blocks = row_blocks(rows)
    shift = blocks[EARLY][0]
    outs = (e_o, m_o, v_o)
    copies = []
    for b, (base, size) in enumerate(blocks[:EARLY]):
        for k, src in enumerate((e_v, m_v, v_v)):
            copy = pltpu.make_async_copy(src.at[pl.ds(base, size)], outs[k].at[pl.ds(base, size)], sem.at[k, b])
            copy.start()
            copies.append(copy)
    for b, (base, size) in enumerate(blocks[EARLY:]):
        adam_rows(base, size, e_v, m_v, v_v, dz_v, x_v, e_s, m_s, v_s, shift)
        for k, src in enumerate((e_s, m_s, v_s)):
            copy = pltpu.make_async_copy(src.at[pl.ds(base - shift, size)], outs[k].at[pl.ds(base, size)],
                                         sem.at[k, EARLY + b])
            copy.start()
            copies.append(copy)

    for copy in copies:
        copy.wait()


def finish_kernel(n, keep_ref, xh_ref, rs_ref, lse_ref, msk_ref, ln_ref, lm_ref, lv_ref, got_ref,
                  tok_o, mean_o, dh_o, ln_o, lmo, lvo):
    _, core, _ = place()
    local, dim = xh_ref.shape
    wide = n * local // 2
    keep, got = keep_ref[...], got_ref[...]
    both = keep + got
    dx, extra = both[0:local], both[local:local + 8]
    near, far = keep[local + 2:local + 4], got[local + 2:local + 4]
    tgt_z = jnp.concatenate([near[0:1] + far[1:2], near[1:2] + far[0:1]], axis=1)
    msk = msk_ref[...]
    loss = (lse_ref[...] - tgt_z) * msk
    mean_o[...] = jnp.sum(loss[:, :wide] + loss[:, wide:], axis=1, keepdims=True) / jnp.sum(msk, axis=1, keepdims=True)
    tok_o[...] = jnp.where(core == 0, loss[:, :local], loss[:, local:wide])
    xhat = xh_ref[...]
    dxh = dx * ln_ref[0:1, :]
    dh = rs_ref[...] * (dxh - jnp.mean(dxh, axis=-1, keepdims=True)
                        - xhat * jnp.mean(dxh * xhat, axis=-1, keepdims=True))
    dh_o[...] = dh.astype(BF16)
    p_new, m_new, v_new = adam(ln_ref[...], extra[0:2], lm_ref[...], lv_ref[...], 0.0)
    ln_o[...] = p_new
    lmo[...] = m_new
    lvo[...] = v_new


def solution(mesh):
    n = mesh.shape["tp"]
    row_spec = P(("dp", "tp"), None)
    tok_spec = P(("dp", "tp"))
    vocab_spec = P("tp", None)
    repl_spec = P()
    part_spec = P("dp", None)
    vmem = pl.BlockSpec(memory_space=pltpu.VMEM)
    hbm = pl.BlockSpec(memory_space=pltpu.HBM)

    def device_step(hidden, targets, loss_mask, ln_params, out_embed, ln_mom1, ln_mom2, embed_mom1, embed_mom2):
        local, dim = hidden.shape
        rows = out_embed.shape[0]
        toks = n * local
        half = rows // 2
        blocks = row_blocks(rows)
        late = rows - blocks[EARLY][0]
        big = [((rows, dim), BF16), ((rows, dim), F32), ((rows, dim), F32)]
        pack = ((local + 8, dim), F32)
        mid = big + [((rows, toks), BF16), ((toks, dim), BF16), pack, pack, ((local, dim), F32), ((local, dim), F32),
                     ((1, toks), F32), ((1, toks), F32), ((2, dim), F32), ((2, dim), F32), ((2, dim), F32)]
        small = [((1, local), F32), ((1, 1), F32), ((local, dim), BF16), ((2, dim), F32), ((2, dim), F32),
                 ((2, dim), F32)]
        dma = pltpu.SemaphoreType.DMA
        peers = n - 1
        mids = pl.pallas_call(
            functools.partial(forward_kernel, n),
            name="forward",
            out_shape=[pltpu.VMEM(*s) for s in mid],
            in_specs=[hbm] * 9,
            out_specs=[vmem] * len(mid),
            scratch_shapes=[
                pltpu.VMEM((local, dim), BF16), pltpu.VMEM((1, local), jnp.int32), pltpu.VMEM((1, local), jnp.int32),
                pltpu.VMEM((n, local, dim), BF16), pltpu.VMEM((n, 1, local), jnp.int32),
                pltpu.VMEM((n, 1, local), jnp.int32), pltpu.VMEM((toks, dim), F32), pltpu.VMEM((toks, dim), F32),
                pltpu.VMEM((toks, dim), F32),
                pltpu.VMEM((2, 2 * dim, toks), BF16), pltpu.VMEM((2, half, toks), F32),
                pltpu.VMEM((2, -(-half // SUB), 8, toks), F32), pltpu.VMEM((dim, -(-rows // 128) * 128), BF16),
                pltpu.VMEM((2, toks), F32), pltpu.VMEM((peers, 2, toks), F32),
                pltpu.VMEM((n // 2, local + 8, dim), F32), pltpu.VMEM((n // 2, local + 8, dim), F32),
                dma((9,)), dma((3, peers)), dma((3, peers)), dma((peers,)), dma((peers,)), dma, dma,
            ],
            compiler_params=pltpu.CompilerParams(
                collective_id=0, has_side_effects=True, vmem_limit_bytes=26 << 20),
        )(*[pltpu.with_memory_space_constraint(a, pltpu.HBM) for a in (
            hidden, targets.reshape(1, local), loss_mask.reshape(1, local), ln_params, ln_mom1, ln_mom2,
            out_embed, embed_mom1, embed_mom2)])
        got = lax.ppermute(mids[6], "tp", [(i, (i + n // 2) % n) for i in range(n)])
        e_new, m_new, v_new = pl.pallas_call(
            update_kernel,
            name="update",
            out_shape=[jax.ShapeDtypeStruct(*s) for s in big],
            in_specs=[vmem] * 5,
            out_specs=[hbm] * 3,
            scratch_shapes=[
                pltpu.VMEM((late, dim), BF16), pltpu.VMEM((late, dim), F32), pltpu.VMEM((late, dim), F32),
                dma((3, len(blocks)))],
            compiler_params=pltpu.CompilerParams(vmem_limit_bytes=20 << 20),
            cost_estimate=pl.CostEstimate(flops=50_000_000_000, bytes_accessed=32_000_000, transcendentals=0),
        )(*[pltpu.with_memory_space_constraint(a, pltpu.VMEM) for a in mids[:5]])
        tok, mean, dh, ln_new, lm_new, lv_new = pl.pallas_call(
            functools.partial(finish_kernel, n),
            name="finish",
            out_shape=[jax.ShapeDtypeStruct(*s) for s in small],
            in_specs=[vmem] * 9,
            out_specs=[vmem] * 6,
            compiler_params=pltpu.CompilerParams(vmem_limit_bytes=4 << 20),
        )(mids[5], *mids[7:], got)
        return (tok.reshape(local), mean.reshape(1), dh, ln_new, lm_new, lv_new, e_new, m_new, v_new)

    return jax.shard_map(device_step, mesh=mesh, in_specs=(row_spec, tok_spec, tok_spec, repl_spec, vocab_spec, repl_spec, repl_spec, vocab_spec, vocab_spec), out_specs=(tok_spec, P("dp"), row_spec, part_spec, part_spec, part_spec, row_spec, row_spec, row_spec), check_vma=False)
```

```python
import functools

import jax
import jax.numpy as jnp
from jax import lax
from jax.experimental import pallas as pl
from jax.experimental.pallas import tpu as pltpu
from jax.sharding import PartitionSpec as P

LN_EPS = 1e-5
BETA_ONE = 0.9
BETA_TWO = 0.95
ADAM_EPS = 1e-8
LEARN_RATE = 1e-3
WEIGHT_DECAY = 0.1
ADAM_STEP = 10
LOG2E = 1.4426950408889634
TINY = 1e-37
SUB = 128
CHUNK = 448
EARLY = 4
DOT = 896
MESH = pl.DeviceIdType.MESH
F32 = jnp.float32
BF16 = jnp.bfloat16


def pair_plan(rows):
    half = rows // 2
    return half, half // SUB, half % SUB


def row_blocks(rows):
    full = rows // CHUNK
    return [(i * CHUNK, CHUNK) for i in range(full)] + ([(full * CHUNK, rows - full * CHUNK)] if rows % CHUNK else [])


def adam_const():
    one = 1.0 - BETA_ONE ** ADAM_STEP
    two = 1.0 - BETA_TWO ** ADAM_STEP
    root = two ** 0.5
    return LEARN_RATE * root / one, ADAM_EPS * root


def adam(param, grad, m_old, v_old, decay):
    scale, eps = adam_const()
    m_new = BETA_ONE * m_old + (1.0 - BETA_ONE) * grad
    v_new = BETA_TWO * v_old + ((1.0 - BETA_TWO) * grad) * grad
    root = v_new * lax.rsqrt(v_new + TINY)
    kept = param if decay == 0.0 else (1.0 - LEARN_RATE * decay) * param
    return kept - (scale * m_new) / (root + eps), m_new, v_new


def adam_rows(base, size, e_in, m_in, v_in, dz_v, x_v, e_out, m_out, v_out, shift):
    sl, to = pl.ds(base, size), pl.ds(base - shift, size)
    g = jnp.dot(dz_v[sl, :], x_v[...], preferred_element_type=F32)
    p_new, m_new, v_new = adam(e_in[sl, :].astype(F32), g, m_in[sl, :], v_in[sl, :], WEIGHT_DECAY)
    e_out[to, :] = p_new.astype(BF16)
    m_out[to, :] = m_new
    v_out[to, :] = v_new


def place():
    me = lax.axis_index("tp")
    side, core = me // 2, lax.rem(me, 2)
    far = 2 - 2 * side
    return me, core, (me + 1 - 2 * core, far + core, far + 1 - core)


def swap(v):
    half = v.shape[1] // 2
    return jnp.concatenate([v[:, half:], v[:, :half]], axis=1)


def forward_kernel(n, hid_hbm, tgt_hbm, msk_hbm, ln_hbm, lm_hbm, lv_hbm, e_hbm, m_hbm, v_hbm,
                   e_v, m_v, v_v, dz_v, x_v, keep_o, away_o, xh_o, rs_o, lse_o, msk_o, lns_o,
                   hid_s, ids_s, xhat_s, rstd_s, dx_s, xd_s, ebuf, mbuf, et_s, st_tx, st_rx, pk_tx, pk_rx,
                   load_sem, hid_send, near_recv, far_recv, ids_send, ids_recv, st_send, st_recv, pk_send, pk_recv):
    me, core, peers = place()
    rows, dim = e_v.shape
    local = hid_hbm.shape[0]
    toks = n * local
    wide = toks // 2
    half, subs, tail = pair_plan(rows)
    units = [((i // subs) * half + (i % subs) * SUB, i * SUB, SUB) for i in range(2 * subs)]

    barrier = pltpu.get_barrier_semaphore()
    for peer in peers:
        pl.semaphore_signal(barrier, inc=1, device_id={"tp": peer}, device_id_type=MESH)
    e_copy = pltpu.make_async_copy(e_hbm, e_v, load_sem.at[0])
    m_copy = pltpu.make_async_copy(m_hbm, m_v, load_sem.at[1])
    v_copy = pltpu.make_async_copy(v_hbm, v_v, load_sem.at[2])
    pltpu.make_async_copy(hid_hbm, hid_s.at[core], near_recv).start()
    e_copy.start()
    for k, src in enumerate((ln_hbm, lm_hbm, lv_hbm)):
        pltpu.make_async_copy(src, lns_o.at[k], load_sem.at[3]).start()
    for k, src in enumerate((tgt_hbm, msk_hbm)):
        pltpu.make_async_copy(src, ids_s.at[core, k], ids_recv).start()
    pl.semaphore_wait(barrier, n - 1)

    def send(src, dst, peer, send_sem, recv_sem):
        copy = pltpu.make_async_remote_copy(src_ref=src, dst_ref=dst, send_sem=send_sem, recv_sem=recv_sem,
                                            device_id={"tp": peer}, device_id_type=MESH)
        copy.start()
        return copy

    def all_of(ref, sem):
        pltpu.make_async_copy(ref, ref, sem).wait()

    for r in (1, 2, 0):
        send(hid_hbm, hid_s.at[2 + core if r else core], peers[r], hid_send, far_recv if r else near_recv)
    for k, src in enumerate((tgt_hbm, msk_hbm)):
        for r, peer in enumerate(peers):
            send(src, ids_s.at[2 + core if r else core, k], peer, ids_send, ids_recv)
    xd_s[...] = jnp.zeros(xd_s.shape, BF16)
    e_copy.wait()
    m_copy.start()
    v_copy.start()

    def norm(h):
        lanes = slice(h * wide, (h + 1) * wide)
        hid = hid_s[2 * h:2 * h + 2].reshape(wide, dim).astype(F32)
        cent = hid - jnp.mean(hid, axis=-1, keepdims=True)
        rstd = lax.rsqrt(jnp.mean(cent * cent, axis=-1, keepdims=True) + LN_EPS)
        xhat = cent * rstd
        x_b = (xhat * lns_o[0, 0:1, :] + lns_o[0, 1:2, :]).astype(BF16)
        x_v[lanes, :] = x_b
        x_t = x_b.T
        xd_s[h, 0:dim, 0:wide] = x_t
        xd_s[h, dim:2 * dim, wide:2 * wide] = x_t
        xhat_s[lanes, :] = xhat
        rstd_s[lanes, :] = jnp.broadcast_to(rstd, (wide, dim))

    def forward(h):
        top = jnp.full((8, toks), -jnp.inf, F32)
        total = jnp.zeros((8, toks), F32)
        for first in range(0, half, DOT):
            span = min(DOT, half - first)
            pair = jnp.concatenate([e_v[pl.ds(first, span), :], e_v[pl.ds(half + first, span), :]], axis=1)
            z = jnp.dot(pair, xd_s[h], preferred_element_type=F32)
            for k in range(0, span, SUB):
                size = min(SUB, span - k)
                zk = z[k:k + size].reshape(size // 8, 8, toks)
                new = jnp.maximum(top, jnp.max(zk, axis=0))
                ek = jnp.exp2((zk - new[None]) * LOG2E)
                ebuf[h, pl.ds(first + k, size), :] = ek.reshape(size, toks)
                mbuf[h, (first + k) // SUB] = new
                total = total * jnp.exp2((top - new) * LOG2E) + jnp.sum(ek, axis=0)
                top = new
        peak = jnp.max(top, axis=0, keepdims=True)
        peak = jnp.maximum(peak[:, :wide], peak[:, wide:])
        peak2 = jnp.concatenate([peak, peak], axis=1)
        total = jnp.sum(total * jnp.exp2((top - peak2) * LOG2E), axis=0, keepdims=True)
        st_tx[0:1, h * wide:(h + 1) * wide] = peak
        st_tx[1:2, h * wide:(h + 1) * wide] = total[:, :wide] + total[:, wide:]

    all_of(lns_o, load_sem.at[3])
    all_of(hid_s.at[pl.ds(0, 2)], near_recv)
    norm(0)
    forward(0)
    all_of(hid_s.at[pl.ds(2, 2)], far_recv)
    norm(1)
    forward(1)
    for r, peer in enumerate(peers):
        send(st_tx, st_rx.at[r], peer, st_send, st_recv)
    all_of(ids_s, ids_recv)

    tgt = jnp.concatenate([ids_s[j, 0] for j in range(n)], axis=1)
    msk = jnp.concatenate([ids_s[j, 1] for j in range(n)], axis=1).astype(F32)
    count = jnp.sum(msk, axis=1, keepdims=True)
    scale = msk / count
    rel = tgt - me * rows
    inside = (rel >= 0) & (rel < rows)
    near = jnp.where(inside, rel, -15000)
    for low, col, size in units:
        et_s[:, pl.ds(col, size)] = e_v[pl.ds(low, size), :].T
    ends = [h * half + subs * SUB for h in range(2)]
    if tail:
        et_s[:, pl.ds(2 * subs * SUB, 2 * tail)] = jnp.concatenate([e_v[pl.ds(low, tail), :] for low in ends], axis=0).T

    flat = jnp.zeros((16, toks), jnp.int32)
    iota16 = lax.broadcasted_iota(jnp.int32, (SUB, toks), 0).astype(jnp.int16).reshape(SUB // 16, 16, toks)

    def hit(low, size):
        return iota16[:size // 16] == (flat + (near - low)).astype(jnp.int16)[None]

    def gather_sum(value):
        accs = [jnp.zeros((dim, toks), F32)] * 2
        groups = [units[i:i + 2] for i in range(0, len(units), 2)]
        if tail:
            groups.append([(low, 2 * subs * SUB + h * tail, tail) for h, low in enumerate(ends)])
        for i, group in enumerate(groups):
            vals = jnp.concatenate([value(low, size) for low, _, size in group], axis=0)
            accs[i % 2] = accs[i % 2] + jnp.dot(et_s[:, pl.ds(group[0][1], vals.shape[0])], vals,
                                                preferred_element_type=F32)
        return accs[0] - accs[1] * -1.0

    ones, none = jnp.ones((1, 16, toks), BF16), jnp.zeros((1, 16, toks), BF16)
    rows_t = gather_sum(lambda low, size: jnp.where(hit(low, size), ones, none).reshape(size, toks))
    tgt_z = jnp.sum(x_v[...].astype(F32).T * rows_t, axis=0, keepdims=True)
    tgt_z = jnp.where(inside, tgt_z, 0.0)

    all_of(st_rx, st_recv)
    both = [st_tx[...], st_rx[0], swap(st_rx[1]), swap(st_rx[2])]
    peak = jnp.maximum(jnp.maximum(both[0][0:1], both[1][0:1]), jnp.maximum(both[2][0:1], both[3][0:1]))
    sums = [v[1:2] * jnp.exp2((v[0:1] - peak) * LOG2E) for v in both]
    lse = peak + jnp.log((sums[0] + sums[1]) + (sums[2] + sums[3]))
    hot_val = (jnp.exp2((tgt_z - lse) * LOG2E) - 1.0) * scale
    hot16 = jnp.broadcast_to(hot_val, (16, toks)).astype(BF16)[None]

    def grads(low, size):
        h, first = low // half, low % half
        sides = slice(h * wide, (h + 1) * wide)
        seen = jnp.concatenate([mbuf[c, first // SUB, :, sides] for c in range(2)], axis=1)
        fac = jnp.exp2((seen - lse) * LOG2E) * scale
        ek = jnp.concatenate([ebuf[c, pl.ds(first, size), sides] for c in range(2)], axis=1)
        dz = (ek.reshape(size // 8, 8, toks) * fac[None]).reshape(size // 16, 16, toks).astype(BF16)
        dz = jnp.where(hit(low, size), hot16, dz).reshape(size, toks)
        dz_v[pl.ds(low, size), :] = dz
        return dz

    dx = gather_sum(grads).T
    extra = jnp.concatenate(
        [jnp.sum(dx * xhat_s[...], axis=0, keepdims=True), jnp.sum(dx, axis=0, keepdims=True)]
        + [tgt_z[:, c * dim:(c + 1) * dim] for c in range(toks // dim)]
        + [jnp.zeros((6 - toks // dim, dim), F32)], axis=0)
    dx_s[...] = dx
    for c in range(2):
        pk_tx[c, 0:local, :] = dx_s[pl.ds(pl.multiple_of(c * wide + (1 - core) * local, local), local), :]
        pk_tx[c, local:local + 8, :] = extra
    part = send(pk_tx, pk_rx, peers[0], pk_send, pk_recv)

    own = pl.ds(pl.multiple_of(core * local, local), local)
    xh_o[...] = xhat_s[own, :]
    rs_o[...] = rstd_s[own, :]
    msk_o[...] = msk
    lse_o[...] = lse
    m_copy.wait()
    v_copy.wait()
    for base, size in row_blocks(rows)[:EARLY]:
        adam_rows(base, size, e_v, m_v, v_v, dz_v, x_v, e_v, m_v, v_v, 0)

    part.wait_recv()
    for c, out in enumerate((keep_o, away_o)):
        mine = pl.ds(pl.multiple_of(c * wide + core * local, local), local)
        out[0:local, :] = dx_s[mine, :] + pk_rx[c, 0:local, :]
        out[local:local + 8, :] = extra + pk_rx[c, local:local + 8, :]
    part.wait_send()
    all_of(hid_s.at[pl.ds(0, n - 1)], hid_send)
    all_of(ids_s.at[pl.ds(0, n - 1)], ids_send)
    all_of(st_rx, st_send)


def update_kernel(e_v, m_v, v_v, dz_v, x_v, e_o, m_o, v_o, e_s, m_s, v_s, sem):
    rows = e_v.shape[0]
    blocks = row_blocks(rows)
    shift = blocks[EARLY][0]
    outs = (e_o, m_o, v_o)
    for base, size in blocks[:EARLY]:
        for k, src in enumerate((e_v, m_v, v_v)):
            pltpu.make_async_copy(src.at[pl.ds(base, size)], outs[k].at[pl.ds(base, size)], sem.at[k]).start()
    for base, size in blocks[EARLY:]:
        adam_rows(base, size, e_v, m_v, v_v, dz_v, x_v, e_s, m_s, v_s, shift)
        for k, src in enumerate((e_s, m_s, v_s)):
            pltpu.make_async_copy(
                src.at[pl.ds(base - shift, size)], outs[k].at[pl.ds(base, size)], sem.at[k]).start()
    for k, src in enumerate((e_v, m_v, v_v)):
        pltpu.make_async_copy(src, outs[k], sem.at[k]).wait()


def finish_kernel(n, keep_ref, xh_ref, rs_ref, lse_ref, msk_ref, lns_ref, got_ref,
                  tok_o, mean_o, dh_o, ln_o, lmo, lvo):
    _, core, _ = place()
    local, dim = xh_ref.shape
    wide = n * local // 2
    keep, got = keep_ref[...], got_ref[...]
    both = keep + got
    dx, extra = both[0:local], both[local:local + 8]
    near, far = keep[local + 2:local + 4], got[local + 2:local + 4]
    tgt_z = jnp.concatenate([near[0:1] + far[1:2], near[1:2] + far[0:1]], axis=1)
    msk = msk_ref[...]
    loss = (lse_ref[...] - tgt_z) * msk
    mean_o[...] = jnp.sum(loss[:, :wide] + loss[:, wide:], axis=1, keepdims=True) / jnp.sum(msk, axis=1, keepdims=True)
    tok_o[...] = jnp.where(core == 0, loss[:, :local], loss[:, local:wide])
    xhat = xh_ref[...]
    dxh = dx * lns_ref[0, 0:1, :]
    dh = rs_ref[...] * (dxh - jnp.mean(dxh, axis=-1, keepdims=True)
                        - xhat * jnp.mean(dxh * xhat, axis=-1, keepdims=True))
    dh_o[...] = dh.astype(BF16)
    p_new, m_new, v_new = adam(lns_ref[0], extra[0:2], lns_ref[1], lns_ref[2], 0.0)
    ln_o[...] = p_new
    lmo[...] = m_new
    lvo[...] = v_new


def solution(mesh):
    n = mesh.shape["tp"]
    row_spec = P(("dp", "tp"), None)
    tok_spec = P(("dp", "tp"))
    vocab_spec = P("tp", None)
    repl_spec = P()
    part_spec = P("dp", None)
    vmem = pl.BlockSpec(memory_space=pltpu.VMEM)
    hbm = pl.BlockSpec(memory_space=pltpu.HBM)

    def device_step(hidden, targets, loss_mask, ln_params, out_embed, ln_mom1, ln_mom2, embed_mom1, embed_mom2):
        local, dim = hidden.shape
        rows = out_embed.shape[0]
        toks = n * local
        half = rows // 2
        blocks = row_blocks(rows)
        late = rows - blocks[EARLY][0]
        big = [((rows, dim), BF16), ((rows, dim), F32), ((rows, dim), F32)]
        pack = ((local + 8, dim), F32)
        mid = big + [((rows, toks), BF16), ((toks, dim), BF16), pack, pack, ((local, dim), F32), ((local, dim), F32),
                     ((1, toks), F32), ((1, toks), F32), ((3, 2, dim), F32)]
        small = [((1, local), F32), ((1, 1), F32), ((local, dim), BF16), ((2, dim), F32), ((2, dim), F32),
                 ((2, dim), F32)]
        dma = pltpu.SemaphoreType.DMA
        peers = n - 1
        mids = pl.pallas_call(
            functools.partial(forward_kernel, n),
            name="forward",
            out_shape=[pltpu.VMEM(*s) for s in mid],
            in_specs=[hbm] * 9,
            out_specs=[vmem] * len(mid),
            scratch_shapes=[
                pltpu.VMEM((n, local, dim), BF16), pltpu.VMEM((n, 2, 1, local), jnp.int32),
                pltpu.VMEM((toks, dim), F32), pltpu.VMEM((toks, dim), F32), pltpu.VMEM((toks, dim), F32),
                pltpu.VMEM((2, 2 * dim, toks), BF16), pltpu.VMEM((2, half, toks), F32),
                pltpu.VMEM((2, -(-half // SUB), 8, toks), F32), pltpu.VMEM((dim, -(-rows // 128) * 128), BF16),
                pltpu.VMEM((2, toks), F32), pltpu.VMEM((peers, 2, toks), F32),
                pltpu.VMEM((n // 2, local + 8, dim), F32), pltpu.VMEM((n // 2, local + 8, dim), F32),
                dma((4,)), dma, dma, dma, dma, dma, dma, dma, dma, dma,
            ],
            compiler_params=pltpu.CompilerParams(
                collective_id=0, has_side_effects=True, vmem_limit_bytes=26 << 20),
        )(*[pltpu.with_memory_space_constraint(a, pltpu.HBM) for a in (
            hidden, targets.reshape(1, local), loss_mask.reshape(1, local), ln_params, ln_mom1, ln_mom2,
            out_embed, embed_mom1, embed_mom2)])
        got = lax.ppermute(mids[6], "tp", [(i, (i + n // 2) % n) for i in range(n)])
        e_new, m_new, v_new = pl.pallas_call(
            update_kernel,
            name="update",
            out_shape=[jax.ShapeDtypeStruct(*s) for s in big],
            in_specs=[vmem] * 5,
            out_specs=[hbm] * 3,
            scratch_shapes=[
                pltpu.VMEM((late, dim), BF16), pltpu.VMEM((late, dim), F32), pltpu.VMEM((late, dim), F32),
                dma((3,))],
            compiler_params=pltpu.CompilerParams(vmem_limit_bytes=20 << 20),
            cost_estimate=pl.CostEstimate(flops=50_000_000_000, bytes_accessed=32_000_000, transcendentals=0),
        )(*[pltpu.with_memory_space_constraint(a, pltpu.VMEM) for a in mids[:5]])
        tok, mean, dh, ln_new, lm_new, lv_new = pl.pallas_call(
            functools.partial(finish_kernel, n),
            name="finish",
            out_shape=[jax.ShapeDtypeStruct(*s) for s in small],
            in_specs=[vmem] * 7,
            out_specs=[vmem] * 6,
            compiler_params=pltpu.CompilerParams(vmem_limit_bytes=4 << 20),
        )(mids[5], *mids[7:], got)
        return (tok.reshape(local), mean.reshape(1), dh, ln_new, lm_new, lv_new, e_new, m_new, v_new)

    return jax.shard_map(device_step, mesh=mesh, in_specs=(row_spec, tok_spec, tok_spec, repl_spec, vocab_spec, repl_spec, repl_spec, vocab_spec, vocab_spec), out_specs=(tok_spec, P("dp"), row_spec, part_spec, part_spec, part_spec, row_spec, row_spec, row_spec), check_vma=False)
```

```python
import functools

import jax
import jax.numpy as jnp
from jax import lax
from jax.experimental import pallas as pl
from jax.experimental.pallas import tpu as pltpu
from jax.sharding import PartitionSpec as P

LN_EPS = 1e-5
BETA_ONE = 0.9
BETA_TWO = 0.95
ADAM_EPS = 1e-8
LEARN_RATE = 1e-3
WEIGHT_DECAY = 0.1
ADAM_STEP = 10
LOG2E = 1.4426950408889634
TINY = 1e-37
SUB = 128
CHUNK = 256
EARLY = 7
DOT = 896
MESH = pl.DeviceIdType.MESH
F32 = jnp.float32
BF16 = jnp.bfloat16


def pair_plan(rows):
    half = rows // 2
    return half, half // SUB, half % SUB


def row_blocks(rows):
    full = rows // CHUNK
    return [(i * CHUNK, CHUNK) for i in range(full)] + ([(full * CHUNK, rows - full * CHUNK)] if rows % CHUNK else [])


def adam_const():
    one = 1.0 - BETA_ONE ** ADAM_STEP
    two = 1.0 - BETA_TWO ** ADAM_STEP
    root = two ** 0.5
    return LEARN_RATE * root / one, ADAM_EPS * root


def adam(param, grad, m_old, v_old, decay):
    scale, eps = adam_const()
    m_new = BETA_ONE * m_old + (1.0 - BETA_ONE) * grad
    v_new = BETA_TWO * v_old + ((1.0 - BETA_TWO) * grad) * grad
    root = v_new * lax.rsqrt(v_new + TINY)
    kept = param if decay == 0.0 else (1.0 - LEARN_RATE * decay) * param
    return kept - (scale * m_new) / (root + eps), m_new, v_new


def adam_rows(base, size, e_in, m_in, v_in, dz_v, x_v, e_out, m_out, v_out, shift):
    sl, to = pl.ds(base, size), pl.ds(base - shift, size)
    g = jnp.dot(dz_v[sl, :], x_v[...], preferred_element_type=F32)
    p_new, m_new, v_new = adam(e_in[sl, :].astype(F32), g, m_in[sl, :], v_in[sl, :], WEIGHT_DECAY)
    e_out[to, :] = p_new.astype(BF16)
    m_out[to, :] = m_new
    v_out[to, :] = v_new


def place():
    me = lax.axis_index("tp")
    side, core = me // 2, lax.rem(me, 2)
    far = 2 - 2 * side
    return me, core, (me + 1 - 2 * core, far + core, far + 1 - core)


def swap(v):
    half = v.shape[1] // 2
    return jnp.concatenate([v[:, half:], v[:, :half]], axis=1)


def forward_kernel(n, hid_hbm, tgt_hbm, msk_hbm, ln_hbm, lm_hbm, lv_hbm, e_hbm, m_hbm, v_hbm,
                   e_v, m_v, v_v, dz_v, x_v, keep_o, away_o, xh_o, rs_o, lse_o, msk_o, lns_o,
                   hid_s, ids_s, xhat_s, rstd_s, dx_s, xd_s, ebuf, mbuf, et_s, st_tx, st_rx, pk_tx, pk_rx,
                   load_sem, hid_send, near_recv, far_recv, ids_send, ids_recv, st_send, st_recv, pk_send, pk_recv):
    me, core, peers = place()
    rows, dim = e_v.shape
    local = hid_hbm.shape[0]
    toks = n * local
    wide = toks // 2
    half, subs, tail = pair_plan(rows)
    units = [((i // subs) * half + (i % subs) * SUB, i * SUB, SUB) for i in range(2 * subs)]

    barrier = pltpu.get_barrier_semaphore()
    for peer in peers:
        pl.semaphore_signal(barrier, inc=1, device_id={"tp": peer}, device_id_type=MESH)
    e_copy = pltpu.make_async_copy(e_hbm, e_v, load_sem.at[0])
    m_copy = pltpu.make_async_copy(m_hbm, m_v, load_sem.at[1])
    v_copy = pltpu.make_async_copy(v_hbm, v_v, load_sem.at[2])
    pltpu.make_async_copy(hid_hbm, hid_s.at[core], near_recv).start()
    e_copy.start()
    for k, src in enumerate((ln_hbm, lm_hbm, lv_hbm)):
        pltpu.make_async_copy(src, lns_o.at[k], load_sem.at[3]).start()
    for k, src in enumerate((tgt_hbm, msk_hbm)):
        pltpu.make_async_copy(src, ids_s.at[core, k], ids_recv).start()
    pl.semaphore_wait(barrier, n - 1)

    def send(src, dst, peer, send_sem, recv_sem):
        copy = pltpu.make_async_remote_copy(src_ref=src, dst_ref=dst, send_sem=send_sem, recv_sem=recv_sem,
                                            device_id={"tp": peer}, device_id_type=MESH)
        copy.start()
        return copy

    def all_of(ref, sem):
        pltpu.make_async_copy(ref, ref, sem).wait()

    for r in (1, 2, 0):
        send(hid_hbm, hid_s.at[2 + core if r else core], peers[r], hid_send, far_recv if r else near_recv)
    for k, src in enumerate((tgt_hbm, msk_hbm)):
        for r, peer in enumerate(peers):
            send(src, ids_s.at[2 + core if r else core, k], peer, ids_send, ids_recv)
    xd_s[...] = jnp.zeros(xd_s.shape, BF16)
    e_copy.wait()
    m_copy.start()
    v_copy.start()

    def norm(h):
        lanes = slice(h * wide, (h + 1) * wide)
        hid = hid_s[2 * h:2 * h + 2].reshape(wide, dim).astype(F32)
        cent = hid - jnp.mean(hid, axis=-1, keepdims=True)
        rstd = lax.rsqrt(jnp.mean(cent * cent, axis=-1, keepdims=True) + LN_EPS)
        xhat = cent * rstd
        x_b = (xhat * lns_o[0, 0:1, :] + lns_o[0, 1:2, :]).astype(BF16)
        x_v[lanes, :] = x_b
        x_t = x_b.T
        xd_s[h, 0:dim, 0:wide] = x_t
        xd_s[h, dim:2 * dim, wide:2 * wide] = x_t
        xhat_s[lanes, :] = xhat
        rstd_s[lanes, :] = jnp.broadcast_to(rstd, (wide, dim))

    def forward(h):
        top = jnp.full((8, toks), -jnp.inf, F32)
        total = jnp.zeros((8, toks), F32)
        for first in range(0, half, DOT):
            span = min(DOT, half - first)
            pair = jnp.concatenate([e_v[pl.ds(first, span), :], e_v[pl.ds(half + first, span), :]], axis=1)
            z = jnp.dot(pair, xd_s[h], preferred_element_type=F32)
            for k in range(0, span, SUB):
                size = min(SUB, span - k)
                zk = z[k:k + size].reshape(size // 8, 8, toks)
                new = jnp.maximum(top, jnp.max(zk, axis=0))
                ek = jnp.exp2((zk - new[None]) * LOG2E)
                ebuf[h, pl.ds(first + k, size), :] = ek.reshape(size, toks)
                mbuf[h, (first + k) // SUB] = new * LOG2E
                total = total * jnp.exp2((top - new) * LOG2E) + jnp.sum(ek, axis=0)
                top = new
        peak = jnp.max(top, axis=0, keepdims=True)
        peak = jnp.maximum(peak[:, :wide], peak[:, wide:])
        peak2 = jnp.concatenate([peak, peak], axis=1)
        total = jnp.sum(total * jnp.exp2((top - peak2) * LOG2E), axis=0, keepdims=True)
        st_tx[0:1, h * wide:(h + 1) * wide] = peak
        st_tx[1:2, h * wide:(h + 1) * wide] = total[:, :wide] + total[:, wide:]

    all_of(lns_o, load_sem.at[3])
    all_of(hid_s.at[pl.ds(0, 2)], near_recv)
    norm(0)
    forward(0)
    all_of(hid_s.at[pl.ds(2, 2)], far_recv)
    norm(1)
    forward(1)
    for r, peer in enumerate(peers):
        send(st_tx, st_rx.at[r], peer, st_send, st_recv)
    all_of(ids_s, ids_recv)

    tgt = jnp.concatenate([ids_s[j, 0] for j in range(n)], axis=1)
    msk = jnp.concatenate([ids_s[j, 1] for j in range(n)], axis=1).astype(F32)
    count = jnp.sum(msk, axis=1, keepdims=True)
    scale = msk / count
    rel = tgt - me * rows
    inside = (rel >= 0) & (rel < rows)
    near = jnp.where(inside, rel, -15000)
    for low, col, size in units:
        et_s[:, pl.ds(col, size)] = e_v[pl.ds(low, size), :].T
    ends = [h * half + subs * SUB for h in range(2)]
    if tail:
        et_s[:, pl.ds(2 * subs * SUB, 2 * tail)] = jnp.concatenate([e_v[pl.ds(low, tail), :] for low in ends], axis=0).T

    flat = jnp.zeros((16, toks), jnp.int32)
    iota16 = lax.broadcasted_iota(jnp.int32, (SUB, toks), 0).astype(jnp.int16).reshape(SUB // 16, 16, toks)

    def hit(low, size):
        return iota16[:size // 16] == (flat + (near - low)).astype(jnp.int16)[None]

    def gather_sum(value):
        accs = [jnp.zeros((dim, toks), F32)] * 2
        groups = [units[i:i + 2] for i in range(0, len(units), 2)]
        if tail:
            groups.append([(low, 2 * subs * SUB + h * tail, tail) for h, low in enumerate(ends)])
        for i, group in enumerate(groups):
            vals = jnp.concatenate([value(low, size) for low, _, size in group], axis=0)
            accs[i % 2] = accs[i % 2] + jnp.dot(et_s[:, pl.ds(group[0][1], vals.shape[0])], vals,
                                                preferred_element_type=F32)
        return accs[0] - accs[1] * -1.0

    ones, none = jnp.ones((1, 16, toks), BF16), jnp.zeros((1, 16, toks), BF16)
    rows_t = gather_sum(lambda low, size: jnp.where(hit(low, size), ones, none).reshape(size, toks))
    tgt_z = jnp.sum(x_v[...].astype(F32).T * rows_t, axis=0, keepdims=True)
    tgt_z = jnp.where(inside, tgt_z, 0.0)

    all_of(st_rx, st_recv)
    both = [st_tx[...], st_rx[0], swap(st_rx[1]), swap(st_rx[2])]
    peak = jnp.maximum(jnp.maximum(both[0][0:1], both[1][0:1]), jnp.maximum(both[2][0:1], both[3][0:1]))
    sums = [v[1:2] * jnp.exp2((v[0:1] - peak) * LOG2E) for v in both]
    lse = peak + jnp.log((sums[0] + sums[1]) + (sums[2] + sums[3]))
    shift = jnp.broadcast_to(lse * LOG2E - jnp.log2(scale), (8, toks))
    hot_val = (jnp.exp2((tgt_z - lse) * LOG2E) - 1.0) * scale
    hot16 = jnp.broadcast_to(hot_val, (16, toks)).astype(BF16)[None]

    def grads(low, size):
        h, first = low // half, low % half
        sides = slice(h * wide, (h + 1) * wide)
        seen = jnp.concatenate([mbuf[c, first // SUB, :, sides] for c in range(2)], axis=1)
        fac = jnp.exp2(seen - shift)
        ek = jnp.concatenate([ebuf[c, pl.ds(first, size), sides] for c in range(2)], axis=1)
        dz = (ek.reshape(size // 8, 8, toks) * fac[None]).reshape(size // 16, 16, toks).astype(BF16)
        dz = jnp.where(hit(low, size), hot16, dz).reshape(size, toks)
        dz_v[pl.ds(low, size), :] = dz
        return dz

    dx = gather_sum(grads).T
    extra = jnp.concatenate(
        [jnp.sum(dx * xhat_s[...], axis=0, keepdims=True), jnp.sum(dx, axis=0, keepdims=True)]
        + [tgt_z[:, c * dim:(c + 1) * dim] for c in range(toks // dim)]
        + [jnp.zeros((6 - toks // dim, dim), F32)], axis=0)
    dx_s[...] = dx
    for c in range(2):
        pk_tx[c, 0:local, :] = dx_s[pl.ds(pl.multiple_of(c * wide + (1 - core) * local, local), local), :]
        pk_tx[c, local:local + 8, :] = extra
    part = send(pk_tx, pk_rx, peers[0], pk_send, pk_recv)

    own = pl.ds(pl.multiple_of(core * local, local), local)
    xh_o[...] = xhat_s[own, :]
    rs_o[...] = rstd_s[own, :]
    msk_o[...] = msk
    lse_o[...] = lse
    m_copy.wait()
    v_copy.wait()
    for base, size in row_blocks(rows)[:EARLY]:
        adam_rows(base, size, e_v, m_v, v_v, dz_v, x_v, e_v, m_v, v_v, 0)

    part.wait_recv()
    for c, out in enumerate((keep_o, away_o)):
        mine = pl.ds(pl.multiple_of(c * wide + core * local, local), local)
        out[0:local, :] = dx_s[mine, :] + pk_rx[c, 0:local, :]
        out[local:local + 8, :] = extra + pk_rx[c, local:local + 8, :]
    part.wait_send()
    all_of(hid_s.at[pl.ds(0, n - 1)], hid_send)
    all_of(ids_s.at[pl.ds(0, n - 1)], ids_send)
    all_of(st_rx, st_send)


def update_kernel(e_v, m_v, v_v, dz_v, x_v, e_o, m_o, v_o, e_s, m_s, v_s, sem):
    rows = e_v.shape[0]
    blocks = row_blocks(rows)
    shift = blocks[EARLY][0]
    outs = (e_o, m_o, v_o)
    for base, size in blocks[:EARLY]:
        for k, src in enumerate((e_v, m_v, v_v)):
            pltpu.make_async_copy(src.at[pl.ds(base, size)], outs[k].at[pl.ds(base, size)], sem.at[k]).start()
    for base, size in blocks[EARLY:]:
        adam_rows(base, size, e_v, m_v, v_v, dz_v, x_v, e_s, m_s, v_s, shift)
        for k, src in enumerate((e_s, m_s, v_s)):
            pltpu.make_async_copy(
                src.at[pl.ds(base - shift, size)], outs[k].at[pl.ds(base, size)], sem.at[k]).start()
    for k, src in enumerate((e_v, m_v, v_v)):
        pltpu.make_async_copy(src, outs[k], sem.at[k]).wait()


def finish_kernel(n, keep_ref, xh_ref, rs_ref, lse_ref, msk_ref, lns_ref, got_ref,
                  tok_o, mean_o, dh_o, ln_o, lmo, lvo):
    _, core, _ = place()
    local, dim = xh_ref.shape
    wide = n * local // 2
    keep, got = keep_ref[...], got_ref[...]
    both = keep + got
    dx, extra = both[0:local], both[local:local + 8]
    near, far = keep[local + 2:local + 4], got[local + 2:local + 4]
    tgt_z = jnp.concatenate([near[0:1] + far[1:2], near[1:2] + far[0:1]], axis=1)
    msk = msk_ref[...]
    loss = (lse_ref[...] - tgt_z) * msk
    mean_o[...] = jnp.sum(loss[:, :wide] + loss[:, wide:], axis=1, keepdims=True) / jnp.sum(msk, axis=1, keepdims=True)
    tok_o[...] = jnp.where(core == 0, loss[:, :local], loss[:, local:wide])
    xhat = xh_ref[...]
    dxh = dx * lns_ref[0, 0:1, :]
    dh = rs_ref[...] * (dxh - jnp.mean(dxh, axis=-1, keepdims=True)
                        - xhat * jnp.mean(dxh * xhat, axis=-1, keepdims=True))
    dh_o[...] = dh.astype(BF16)
    p_new, m_new, v_new = adam(lns_ref[0], extra[0:2], lns_ref[1], lns_ref[2], 0.0)
    ln_o[...] = p_new
    lmo[...] = m_new
    lvo[...] = v_new


def solution(mesh):
    n = mesh.shape["tp"]
    row_spec = P(("dp", "tp"), None)
    tok_spec = P(("dp", "tp"))
    vocab_spec = P("tp", None)
    repl_spec = P()
    part_spec = P("dp", None)
    vmem = pl.BlockSpec(memory_space=pltpu.VMEM)
    hbm = pl.BlockSpec(memory_space=pltpu.HBM)

    def device_step(hidden, targets, loss_mask, ln_params, out_embed, ln_mom1, ln_mom2, embed_mom1, embed_mom2):
        local, dim = hidden.shape
        rows = out_embed.shape[0]
        toks = n * local
        half = rows // 2
        blocks = row_blocks(rows)
        late = rows - blocks[EARLY][0]
        big = [((rows, dim), BF16), ((rows, dim), F32), ((rows, dim), F32)]
        pack = ((local + 8, dim), F32)
        mid = big + [((rows, toks), BF16), ((toks, dim), BF16), pack, pack, ((local, dim), F32), ((local, dim), F32),
                     ((1, toks), F32), ((1, toks), F32), ((3, 2, dim), F32)]
        small = [((1, local), F32), ((1, 1), F32), ((local, dim), BF16), ((2, dim), F32), ((2, dim), F32),
                 ((2, dim), F32)]
        dma = pltpu.SemaphoreType.DMA
        peers = n - 1
        mids = pl.pallas_call(
            functools.partial(forward_kernel, n),
            name="forward",
            out_shape=[pltpu.VMEM(*s) for s in mid],
            in_specs=[hbm] * 9,
            out_specs=[vmem] * len(mid),
            scratch_shapes=[
                pltpu.VMEM((n, local, dim), BF16), pltpu.VMEM((n, 2, 1, local), jnp.int32),
                pltpu.VMEM((toks, dim), F32), pltpu.VMEM((toks, dim), F32), pltpu.VMEM((toks, dim), F32),
                pltpu.VMEM((2, 2 * dim, toks), BF16), pltpu.VMEM((2, half, toks), F32),
                pltpu.VMEM((2, -(-half // SUB), 8, toks), F32), pltpu.VMEM((dim, -(-rows // 128) * 128), BF16),
                pltpu.VMEM((2, toks), F32), pltpu.VMEM((peers, 2, toks), F32),
                pltpu.VMEM((n // 2, local + 8, dim), F32), pltpu.VMEM((n // 2, local + 8, dim), F32),
                dma((4,)), dma, dma, dma, dma, dma, dma, dma, dma, dma,
            ],
            compiler_params=pltpu.CompilerParams(
                collective_id=0, has_side_effects=True, vmem_limit_bytes=26 << 20),
        )(*[pltpu.with_memory_space_constraint(a, pltpu.HBM) for a in (
            hidden, targets.reshape(1, local), loss_mask.reshape(1, local), ln_params, ln_mom1, ln_mom2,
            out_embed, embed_mom1, embed_mom2)])
        got = lax.ppermute(mids[6], "tp", [(i, (i + n // 2) % n) for i in range(n)])
        e_new, m_new, v_new = pl.pallas_call(
            update_kernel,
            name="update",
            out_shape=[jax.ShapeDtypeStruct(*s) for s in big],
            in_specs=[vmem] * 5,
            out_specs=[hbm] * 3,
            scratch_shapes=[
                pltpu.VMEM((late, dim), BF16), pltpu.VMEM((late, dim), F32), pltpu.VMEM((late, dim), F32),
                dma((3,))],
            compiler_params=pltpu.CompilerParams(vmem_limit_bytes=20 << 20),
            cost_estimate=pl.CostEstimate(flops=50_000_000_000, bytes_accessed=32_000_000, transcendentals=0),
        )(*[pltpu.with_memory_space_constraint(a, pltpu.VMEM) for a in mids[:5]])
        tok, mean, dh, ln_new, lm_new, lv_new = pl.pallas_call(
            functools.partial(finish_kernel, n),
            name="finish",
            out_shape=[jax.ShapeDtypeStruct(*s) for s in small],
            in_specs=[vmem] * 7,
            out_specs=[vmem] * 6,
            compiler_params=pltpu.CompilerParams(vmem_limit_bytes=4 << 20),
        )(mids[5], *mids[7:], got)
        return (tok.reshape(local), mean.reshape(1), dh, ln_new, lm_new, lv_new, e_new, m_new, v_new)

    return jax.shard_map(device_step, mesh=mesh, in_specs=(row_spec, tok_spec, tok_spec, repl_spec, vocab_spec, repl_spec, repl_spec, vocab_spec, vocab_spec), out_specs=(tok_spec, P("dp"), row_spec, part_spec, part_spec, part_spec, row_spec, row_spec, row_spec), check_vma=False)
```

```python
import functools

import jax
import jax.numpy as jnp
from jax import lax
from jax.experimental import pallas as pl
from jax.experimental.pallas import tpu as pltpu
from jax.sharding import PartitionSpec as P

LN_EPS = 1e-5
BETA_ONE = 0.9
BETA_TWO = 0.95
ADAM_EPS = 1e-8
LEARN_RATE = 1e-3
WEIGHT_DECAY = 0.1
ADAM_STEP = 10
LOG2E = 1.4426950408889634
TINY = 1e-37
SUB = 128
CHUNK = 256
EARLY = 7
DOT = 896
MESH = pl.DeviceIdType.MESH
F32 = jnp.float32
BF16 = jnp.bfloat16


def pair_plan(rows):
    half = rows // 2
    return half, half // SUB, half % SUB


def row_blocks(rows):
    full = rows // CHUNK
    return [(i * CHUNK, CHUNK) for i in range(full)] + ([(full * CHUNK, rows - full * CHUNK)] if rows % CHUNK else [])


def adam_const():
    one = 1.0 - BETA_ONE ** ADAM_STEP
    two = 1.0 - BETA_TWO ** ADAM_STEP
    root = two ** 0.5
    return LEARN_RATE * root / one, ADAM_EPS * root


def adam(param, grad, m_old, v_old, decay):
    scale, eps = adam_const()
    m_new = BETA_ONE * m_old + (1.0 - BETA_ONE) * grad
    v_new = BETA_TWO * v_old + ((1.0 - BETA_TWO) * grad) * grad
    root = v_new * lax.rsqrt(v_new + TINY)
    kept = param if decay == 0.0 else (1.0 - LEARN_RATE * decay) * param
    return kept - (scale * m_new) / (root + eps), m_new, v_new


def adam_rows(base, size, e_in, m_in, v_in, dz_v, x_v, e_out, m_out, v_out, shift):
    sl, to = pl.ds(base, size), pl.ds(base - shift, size)
    g = jnp.dot(dz_v[sl, :], x_v[...], preferred_element_type=F32)
    p_new, m_new, v_new = adam(e_in[sl, :].astype(F32), g, m_in[sl, :], v_in[sl, :], WEIGHT_DECAY)
    e_out[to, :] = p_new.astype(BF16)
    m_out[to, :] = m_new
    v_out[to, :] = v_new


def place():
    me = lax.axis_index("tp")
    side, core = me // 2, lax.rem(me, 2)
    far = 2 - 2 * side
    return me, core, (me + 1 - 2 * core, far + core, far + 1 - core)


def swap(v):
    half = v.shape[1] // 2
    return jnp.concatenate([v[:, half:], v[:, :half]], axis=1)


def forward_kernel(n, hid_hbm, tgt_hbm, msk_hbm, ln_hbm, lm_hbm, lv_hbm, e_hbm, m_hbm, v_hbm,
                   e_v, m_v, v_v, dz_v, x_v, keep_o, away_o, xh_o, rs_o, lse_o, msk_o, lns_o,
                   hid_s, ids_s, xhat_s, rstd_s, dx_s, xd_s, ebuf, mbuf, et_s, st_tx, st_rx, pk_tx, pk_rx,
                   load_sem, hid_send, near_recv, far_recv, ids_send, ids_recv, st_send, st_recv, pk_send, pk_recv):
    me, core, peers = place()
    rows, dim = e_v.shape
    local = hid_hbm.shape[0]
    toks = n * local
    wide = toks // 2
    half, subs, tail = pair_plan(rows)
    units = [((i // subs) * half + (i % subs) * SUB, i * SUB, SUB) for i in range(2 * subs)]

    barrier = pltpu.get_barrier_semaphore()
    for peer in peers:
        pl.semaphore_signal(barrier, inc=1, device_id={"tp": peer}, device_id_type=MESH)
    e_copy = pltpu.make_async_copy(e_hbm, e_v, load_sem.at[0])
    m_copy = pltpu.make_async_copy(m_hbm, m_v, load_sem.at[1])
    v_copy = pltpu.make_async_copy(v_hbm, v_v, load_sem.at[2])
    pltpu.make_async_copy(hid_hbm, hid_s.at[core], near_recv).start()
    e_copy.start()
    for k, src in enumerate((ln_hbm, lm_hbm, lv_hbm)):
        pltpu.make_async_copy(src, lns_o.at[k], load_sem.at[3]).start()
    for k, src in enumerate((tgt_hbm, msk_hbm)):
        pltpu.make_async_copy(src, ids_s.at[core, k], ids_recv).start()
    pl.semaphore_wait(barrier, n - 1)

    def send(src, dst, peer, send_sem, recv_sem):
        copy = pltpu.make_async_remote_copy(src_ref=src, dst_ref=dst, send_sem=send_sem, recv_sem=recv_sem,
                                            device_id={"tp": peer}, device_id_type=MESH)
        copy.start()
        return copy

    def all_of(ref, sem):
        pltpu.make_async_copy(ref, ref, sem).wait()

    for r in (1, 2, 0):
        send(hid_hbm, hid_s.at[2 + core if r else core], peers[r], hid_send, far_recv if r else near_recv)
    for k, src in enumerate((tgt_hbm, msk_hbm)):
        for r, peer in enumerate(peers):
            send(src, ids_s.at[2 + core if r else core, k], peer, ids_send, ids_recv)
    xd_s[...] = jnp.zeros(xd_s.shape, BF16)
    e_copy.wait()
    m_copy.start()
    v_copy.start()

    def norm(h):
        lanes = slice(h * wide, (h + 1) * wide)
        hid = hid_s[2 * h:2 * h + 2].reshape(wide, dim).astype(F32)
        cent = hid - jnp.mean(hid, axis=-1, keepdims=True)
        rstd = lax.rsqrt(jnp.mean(cent * cent, axis=-1, keepdims=True) + LN_EPS)
        xhat = cent * rstd
        x_b = (xhat * lns_o[0, 0:1, :] + lns_o[0, 1:2, :]).astype(BF16)
        x_v[lanes, :] = x_b
        x_t = x_b.T
        xd_s[h, 0:dim, 0:wide] = x_t
        xd_s[h, dim:2 * dim, wide:2 * wide] = x_t
        xhat_s[lanes, :] = xhat
        rstd_s[lanes, :] = jnp.broadcast_to(rstd, (wide, dim))

    def forward(h):
        top = jnp.full((8, toks), -jnp.inf, F32)
        total = jnp.zeros((8, toks), F32)
        for first in range(0, half, DOT):
            span = min(DOT, half - first)
            pair = jnp.concatenate([e_v[pl.ds(first, span), :], e_v[pl.ds(half + first, span), :]], axis=1)
            z = jnp.dot(pair, xd_s[h], preferred_element_type=F32)
            for k in range(0, span, SUB):
                size = min(SUB, span - k)
                zk = z[k:k + size].reshape(size // 8, 8, toks)
                new = jnp.maximum(top, jnp.max(zk, axis=0))
                ek = jnp.exp2((zk - new[None]) * LOG2E)
                ebuf[h, pl.ds(first + k, size), :] = ek.reshape(size, toks)
                mbuf[h, (first + k) // SUB] = new * LOG2E
                total = total * jnp.exp2((top - new) * LOG2E) + jnp.sum(ek, axis=0)
                top = new
        peak = jnp.max(top, axis=0, keepdims=True)
        peak = jnp.maximum(peak[:, :wide], peak[:, wide:])
        peak2 = jnp.concatenate([peak, peak], axis=1)
        total = jnp.sum(total * jnp.exp2((top - peak2) * LOG2E), axis=0, keepdims=True)
        st_tx[0:1, h * wide:(h + 1) * wide] = peak
        st_tx[1:2, h * wide:(h + 1) * wide] = total[:, :wide] + total[:, wide:]

    all_of(lns_o, load_sem.at[3])
    all_of(hid_s.at[pl.ds(0, 2)], near_recv)
    norm(0)
    forward(0)
    all_of(hid_s.at[pl.ds(2, 2)], far_recv)
    norm(1)
    forward(1)
    for r, peer in enumerate(peers):
        send(st_tx, st_rx.at[r], peer, st_send, st_recv)
    all_of(ids_s, ids_recv)

    tgt = jnp.concatenate([ids_s[j, 0] for j in range(n)], axis=1)
    msk = jnp.concatenate([ids_s[j, 1] for j in range(n)], axis=1).astype(F32)
    count = jnp.sum(msk, axis=1, keepdims=True)
    scale = msk / count
    rel = tgt - me * rows
    inside = (rel >= 0) & (rel < rows)
    near = jnp.where(inside, rel, -15000)
    for low, col, size in units:
        et_s[:, pl.ds(col, size)] = e_v[pl.ds(low, size), :].T
    ends = [h * half + subs * SUB for h in range(2)]
    if tail:
        et_s[:, pl.ds(2 * subs * SUB, 2 * tail)] = jnp.concatenate([e_v[pl.ds(low, tail), :] for low in ends], axis=0).T

    flat = jnp.zeros((16, toks), jnp.int32)
    iota16 = lax.broadcasted_iota(jnp.int32, (SUB, toks), 0).astype(jnp.int16).reshape(SUB // 16, 16, toks)

    def hit(low, size):
        return iota16[:size // 16] == (flat + (near - low)).astype(jnp.int16)[None]

    def gather_sum(value):
        accs = [jnp.zeros((dim, toks), F32)] * 2
        groups = [units[i:i + 2] for i in range(0, len(units), 2)]
        if tail:
            groups.append([(low, 2 * subs * SUB + h * tail, tail) for h, low in enumerate(ends)])
        for i, group in enumerate(groups):
            vals = jnp.concatenate([value(low, size) for low, _, size in group], axis=0)
            accs[i % 2] = accs[i % 2] + jnp.dot(et_s[:, pl.ds(group[0][1], vals.shape[0])], vals,
                                                preferred_element_type=F32)
        return accs[0] - accs[1] * -1.0

    ones, none = jnp.ones((1, 16, toks), BF16), jnp.zeros((1, 16, toks), BF16)
    rows_t = gather_sum(lambda low, size: jnp.where(hit(low, size), ones, none).reshape(size, toks))
    cross = jnp.dot(x_v[...], rows_t.astype(BF16), preferred_element_type=F32)
    diag = lax.broadcasted_iota(jnp.int32, (toks, toks), 0) == lax.broadcasted_iota(jnp.int32, (toks, toks), 1)
    tgt_z = jnp.sum(jnp.where(diag, cross, 0.0), axis=0, keepdims=True)
    tgt_z = jnp.where(inside, tgt_z, 0.0)

    all_of(st_rx, st_recv)
    both = [st_tx[...], st_rx[0], swap(st_rx[1]), swap(st_rx[2])]
    peak = jnp.maximum(jnp.maximum(both[0][0:1], both[1][0:1]), jnp.maximum(both[2][0:1], both[3][0:1]))
    sums = [v[1:2] * jnp.exp2((v[0:1] - peak) * LOG2E) for v in both]
    lse = peak + jnp.log((sums[0] + sums[1]) + (sums[2] + sums[3]))
    shift = jnp.broadcast_to(lse * LOG2E - jnp.log2(scale), (8, toks))
    hot_val = (jnp.exp2((tgt_z - lse) * LOG2E) - 1.0) * scale
    hot16 = jnp.broadcast_to(hot_val, (16, toks)).astype(BF16)[None]

    def grads(low, size):
        h, first = low // half, low % half
        sides = slice(h * wide, (h + 1) * wide)
        seen = jnp.concatenate([mbuf[c, first // SUB, :, sides] for c in range(2)], axis=1)
        fac = jnp.exp2(seen - shift)
        ek = jnp.concatenate([ebuf[c, pl.ds(first, size), sides] for c in range(2)], axis=1)
        dz = (ek.reshape(size // 8, 8, toks) * fac[None]).reshape(size // 16, 16, toks).astype(BF16)
        dz = jnp.where(hit(low, size), hot16, dz).reshape(size, toks)
        dz_v[pl.ds(low, size), :] = dz
        return dz

    dx = gather_sum(grads).T
    extra = jnp.concatenate(
        [jnp.sum(dx * xhat_s[...], axis=0, keepdims=True), jnp.sum(dx, axis=0, keepdims=True)]
        + [tgt_z[:, c * dim:(c + 1) * dim] for c in range(toks // dim)]
        + [jnp.zeros((6 - toks // dim, dim), F32)], axis=0)
    dx_s[...] = dx
    for c in range(2):
        pk_tx[c, 0:local, :] = dx_s[pl.ds(pl.multiple_of(c * wide + (1 - core) * local, local), local), :]
        pk_tx[c, local:local + 8, :] = extra
    part = send(pk_tx, pk_rx, peers[0], pk_send, pk_recv)

    own = pl.ds(pl.multiple_of(core * local, local), local)
    xh_o[...] = xhat_s[own, :]
    rs_o[...] = rstd_s[own, :]
    msk_o[...] = msk
    lse_o[...] = lse
    m_copy.wait()
    v_copy.wait()
    for base, size in row_blocks(rows)[:EARLY]:
        adam_rows(base, size, e_v, m_v, v_v, dz_v, x_v, e_v, m_v, v_v, 0)

    part.wait_recv()
    for c, out in enumerate((keep_o, away_o)):
        mine = pl.ds(pl.multiple_of(c * wide + core * local, local), local)
        out[0:local, :] = dx_s[mine, :] + pk_rx[c, 0:local, :]
        out[local:local + 8, :] = extra + pk_rx[c, local:local + 8, :]
    part.wait_send()
    all_of(hid_s.at[pl.ds(0, n - 1)], hid_send)
    all_of(ids_s.at[pl.ds(0, n - 1)], ids_send)
    all_of(st_rx, st_send)


def update_kernel(e_v, m_v, v_v, dz_v, x_v, e_o, m_o, v_o, e_s, m_s, v_s, sem):
    rows = e_v.shape[0]
    blocks = row_blocks(rows)
    shift = blocks[EARLY][0]
    outs = (e_o, m_o, v_o)
    for base, size in blocks[:EARLY]:
        for k, src in enumerate((e_v, m_v, v_v)):
            pltpu.make_async_copy(src.at[pl.ds(base, size)], outs[k].at[pl.ds(base, size)], sem.at[k]).start()
    for base, size in blocks[EARLY:]:
        adam_rows(base, size, e_v, m_v, v_v, dz_v, x_v, e_s, m_s, v_s, shift)
        for k, src in enumerate((e_s, m_s, v_s)):
            pltpu.make_async_copy(
                src.at[pl.ds(base - shift, size)], outs[k].at[pl.ds(base, size)], sem.at[k]).start()
    for k, src in enumerate((e_v, m_v, v_v)):
        pltpu.make_async_copy(src, outs[k], sem.at[k]).wait()


def finish_kernel(n, keep_ref, xh_ref, rs_ref, lse_ref, msk_ref, lns_ref, got_ref,
                  tok_o, mean_o, dh_o, ln_o, lmo, lvo):
    _, core, _ = place()
    local, dim = xh_ref.shape
    wide = n * local // 2
    keep, got = keep_ref[...], got_ref[...]
    both = keep + got
    dx, extra = both[0:local], both[local:local + 8]
    near, far = keep[local + 2:local + 4], got[local + 2:local + 4]
    tgt_z = jnp.concatenate([near[0:1] + far[1:2], near[1:2] + far[0:1]], axis=1)
    msk = msk_ref[...]
    loss = (lse_ref[...] - tgt_z) * msk
    mean_o[...] = jnp.sum(loss[:, :wide] + loss[:, wide:], axis=1, keepdims=True) / jnp.sum(msk, axis=1, keepdims=True)
    tok_o[...] = jnp.where(core == 0, loss[:, :local], loss[:, local:wide])
    xhat = xh_ref[...]
    dxh = dx * lns_ref[0, 0:1, :]
    dh = rs_ref[...] * (dxh - jnp.mean(dxh, axis=-1, keepdims=True)
                        - xhat * jnp.mean(dxh * xhat, axis=-1, keepdims=True))
    dh_o[...] = dh.astype(BF16)
    p_new, m_new, v_new = adam(lns_ref[0], extra[0:2], lns_ref[1], lns_ref[2], 0.0)
    ln_o[...] = p_new
    lmo[...] = m_new
    lvo[...] = v_new


def solution(mesh):
    n = mesh.shape["tp"]
    row_spec = P(("dp", "tp"), None)
    tok_spec = P(("dp", "tp"))
    vocab_spec = P("tp", None)
    repl_spec = P()
    part_spec = P("dp", None)
    vmem = pl.BlockSpec(memory_space=pltpu.VMEM)
    hbm = pl.BlockSpec(memory_space=pltpu.HBM)

    def device_step(hidden, targets, loss_mask, ln_params, out_embed, ln_mom1, ln_mom2, embed_mom1, embed_mom2):
        local, dim = hidden.shape
        rows = out_embed.shape[0]
        toks = n * local
        half = rows // 2
        blocks = row_blocks(rows)
        late = rows - blocks[EARLY][0]
        big = [((rows, dim), BF16), ((rows, dim), F32), ((rows, dim), F32)]
        pack = ((local + 8, dim), F32)
        mid = big + [((rows, toks), BF16), ((toks, dim), BF16), pack, pack, ((local, dim), F32), ((local, dim), F32),
                     ((1, toks), F32), ((1, toks), F32), ((3, 2, dim), F32)]
        small = [((1, local), F32), ((1, 1), F32), ((local, dim), BF16), ((2, dim), F32), ((2, dim), F32),
                 ((2, dim), F32)]
        dma = pltpu.SemaphoreType.DMA
        peers = n - 1
        mids = pl.pallas_call(
            functools.partial(forward_kernel, n),
            name="forward",
            out_shape=[pltpu.VMEM(*s) for s in mid],
            in_specs=[hbm] * 9,
            out_specs=[vmem] * len(mid),
            scratch_shapes=[
                pltpu.VMEM((n, local, dim), BF16), pltpu.VMEM((n, 2, 1, local), jnp.int32),
                pltpu.VMEM((toks, dim), F32), pltpu.VMEM((toks, dim), F32), pltpu.VMEM((toks, dim), F32),
                pltpu.VMEM((2, 2 * dim, toks), BF16), pltpu.VMEM((2, half, toks), F32),
                pltpu.VMEM((2, -(-half // SUB), 8, toks), F32), pltpu.VMEM((dim, -(-rows // 128) * 128), BF16),
                pltpu.VMEM((2, toks), F32), pltpu.VMEM((peers, 2, toks), F32),
                pltpu.VMEM((n // 2, local + 8, dim), F32), pltpu.VMEM((n // 2, local + 8, dim), F32),
                dma((4,)), dma, dma, dma, dma, dma, dma, dma, dma, dma,
            ],
            compiler_params=pltpu.CompilerParams(
                collective_id=0, has_side_effects=True, vmem_limit_bytes=26 << 20),
        )(*[pltpu.with_memory_space_constraint(a, pltpu.HBM) for a in (
            hidden, targets.reshape(1, local), loss_mask.reshape(1, local), ln_params, ln_mom1, ln_mom2,
            out_embed, embed_mom1, embed_mom2)])
        got = lax.ppermute(mids[6], "tp", [(i, (i + n // 2) % n) for i in range(n)])
        e_new, m_new, v_new = pl.pallas_call(
            update_kernel,
            name="update",
            out_shape=[jax.ShapeDtypeStruct(*s) for s in big],
            in_specs=[vmem] * 5,
            out_specs=[hbm] * 3,
            scratch_shapes=[
                pltpu.VMEM((late, dim), BF16), pltpu.VMEM((late, dim), F32), pltpu.VMEM((late, dim), F32),
                dma((3,))],
            compiler_params=pltpu.CompilerParams(vmem_limit_bytes=20 << 20),
            cost_estimate=pl.CostEstimate(flops=50_000_000_000, bytes_accessed=32_000_000, transcendentals=0),
        )(*[pltpu.with_memory_space_constraint(a, pltpu.VMEM) for a in mids[:5]])
        tok, mean, dh, ln_new, lm_new, lv_new = pl.pallas_call(
            functools.partial(finish_kernel, n),
            name="finish",
            out_shape=[jax.ShapeDtypeStruct(*s) for s in small],
            in_specs=[vmem] * 7,
            out_specs=[vmem] * 6,
            compiler_params=pltpu.CompilerParams(vmem_limit_bytes=4 << 20),
        )(mids[5], *mids[7:], got)
        return (tok.reshape(local), mean.reshape(1), dh, ln_new, lm_new, lv_new, e_new, m_new, v_new)

    return jax.shard_map(device_step, mesh=mesh, in_specs=(row_spec, tok_spec, tok_spec, repl_spec, vocab_spec, repl_spec, repl_spec, vocab_spec, vocab_spec), out_specs=(tok_spec, P("dp"), row_spec, part_spec, part_spec, part_spec, row_spec, row_spec, row_spec), check_vma=False)
```

```python
import functools

import jax
import jax.numpy as jnp
from jax import lax
from jax.experimental import pallas as pl
from jax.experimental.pallas import tpu as pltpu
from jax.sharding import PartitionSpec as P

LN_EPS = 1e-5
BETA_ONE = 0.9
BETA_TWO = 0.95
ADAM_EPS = 1e-8
LEARN_RATE = 1e-3
WEIGHT_DECAY = 0.1
ADAM_STEP = 10
LOG2E = 1.4426950408889634
TINY = 1e-37
SUB = 128
CHUNK = 128
EARLY = 14
DOT = 896
MESH = pl.DeviceIdType.MESH
F32 = jnp.float32
BF16 = jnp.bfloat16


def pair_plan(rows):
    half = rows // 2
    return half, half // SUB, half % SUB


def row_blocks(rows):
    full = rows // CHUNK
    return [(i * CHUNK, CHUNK) for i in range(full)] + ([(full * CHUNK, rows - full * CHUNK)] if rows % CHUNK else [])


def adam_const():
    one = 1.0 - BETA_ONE ** ADAM_STEP
    two = 1.0 - BETA_TWO ** ADAM_STEP
    root = two ** 0.5
    return LEARN_RATE * root / one, ADAM_EPS * root


def adam(param, grad, m_old, v_old, decay):
    scale, eps = adam_const()
    m_new = BETA_ONE * m_old + (1.0 - BETA_ONE) * grad
    v_new = BETA_TWO * v_old + ((1.0 - BETA_TWO) * grad) * grad
    root = v_new * lax.rsqrt(v_new + TINY)
    kept = param if decay == 0.0 else (1.0 - LEARN_RATE * decay) * param
    return kept - (scale * m_new) / (root + eps), m_new, v_new


def adam_rows(base, size, e_in, m_in, v_in, dz_v, x_v, e_out, m_out, v_out, shift):
    sl, to = pl.ds(base, size), pl.ds(base - shift, size)
    g = jnp.dot(dz_v[sl, :], x_v[...], preferred_element_type=F32)
    p_new, m_new, v_new = adam(e_in[sl, :].astype(F32), g, m_in[sl, :], v_in[sl, :], WEIGHT_DECAY)
    e_out[to, :] = p_new.astype(BF16)
    m_out[to, :] = m_new
    v_out[to, :] = v_new


def place():
    me = lax.axis_index("tp")
    side, core = me // 2, lax.rem(me, 2)
    far = 2 - 2 * side
    return me, core, (me + 1 - 2 * core, far + core, far + 1 - core)


def swap(v):
    half = v.shape[1] // 2
    return jnp.concatenate([v[:, half:], v[:, :half]], axis=1)


def forward_kernel(n, hid_hbm, tgt_hbm, msk_hbm, ln_hbm, lm_hbm, lv_hbm, e_hbm, m_hbm, v_hbm,
                   e_v, m_v, v_v, dz_v, x_v, keep_o, away_o, xh_o, rs_o, lse_o, msk_o, lns_o,
                   hid_s, ids_s, xhat_s, rstd_s, dx_s, xd_s, ebuf, mbuf, et_s, st_tx, st_rx, pk_tx, pk_rx,
                   load_sem, hid_send, near_recv, far_recv, ids_send, ids_recv, st_send, st_recv, pk_send, pk_recv):
    me, core, peers = place()
    rows, dim = e_v.shape
    local = hid_hbm.shape[0]
    toks = n * local
    wide = toks // 2
    half, subs, tail = pair_plan(rows)
    units = [((i // subs) * half + (i % subs) * SUB, i * SUB, SUB) for i in range(2 * subs)]

    barrier = pltpu.get_barrier_semaphore()
    for peer in peers:
        pl.semaphore_signal(barrier, inc=1, device_id={"tp": peer}, device_id_type=MESH)
    e_copy = pltpu.make_async_copy(e_hbm, e_v, load_sem.at[0])
    m_copy = pltpu.make_async_copy(m_hbm, m_v, load_sem.at[1])
    v_copy = pltpu.make_async_copy(v_hbm, v_v, load_sem.at[2])
    pltpu.make_async_copy(hid_hbm, hid_s.at[core], near_recv).start()
    e_copy.start()
    for k, src in enumerate((ln_hbm, lm_hbm, lv_hbm)):
        pltpu.make_async_copy(src, lns_o.at[k], load_sem.at[3]).start()
    for k, src in enumerate((tgt_hbm, msk_hbm)):
        pltpu.make_async_copy(src, ids_s.at[core, k], ids_recv).start()
    pl.semaphore_wait(barrier, n - 1)

    def send(src, dst, peer, send_sem, recv_sem):
        copy = pltpu.make_async_remote_copy(src_ref=src, dst_ref=dst, send_sem=send_sem, recv_sem=recv_sem,
                                            device_id={"tp": peer}, device_id_type=MESH)
        copy.start()
        return copy

    def all_of(ref, sem):
        pltpu.make_async_copy(ref, ref, sem).wait()

    for r in (1, 2, 0):
        send(hid_hbm, hid_s.at[2 + core if r else core], peers[r], hid_send, far_recv if r else near_recv)
    for k, src in enumerate((tgt_hbm, msk_hbm)):
        for r, peer in enumerate(peers):
            send(src, ids_s.at[2 + core if r else core, k], peer, ids_send, ids_recv)
    xd_s[...] = jnp.zeros(xd_s.shape, BF16)
    e_copy.wait()
    m_copy.start()
    v_copy.start()

    def norm(h):
        lanes = slice(h * wide, (h + 1) * wide)
        hid = hid_s[2 * h:2 * h + 2].reshape(wide, dim).astype(F32)
        cent = hid - jnp.mean(hid, axis=-1, keepdims=True)
        rstd = lax.rsqrt(jnp.mean(cent * cent, axis=-1, keepdims=True) + LN_EPS)
        xhat = cent * rstd
        x_b = (xhat * lns_o[0, 0:1, :] + lns_o[0, 1:2, :]).astype(BF16)
        x_v[lanes, :] = x_b
        x_t = x_b.T
        xd_s[h, 0:dim, 0:wide] = x_t
        xd_s[h, dim:2 * dim, wide:2 * wide] = x_t
        xhat_s[lanes, :] = xhat
        rstd_s[lanes, :] = jnp.broadcast_to(rstd, (wide, dim))

    def forward(h):
        top = jnp.full((8, toks), -jnp.inf, F32)
        total = jnp.zeros((8, toks), F32)
        for first in range(0, half, DOT):
            span = min(DOT, half - first)
            pair = jnp.concatenate([e_v[pl.ds(first, span), :], e_v[pl.ds(half + first, span), :]], axis=1)
            z = jnp.dot(pair, xd_s[h], preferred_element_type=F32)
            for k in range(0, span, SUB):
                size = min(SUB, span - k)
                zk = z[k:k + size].reshape(size // 8, 8, toks)
                new = jnp.maximum(top, jnp.max(zk, axis=0))
                ek = jnp.exp2((zk - new[None]) * LOG2E)
                ebuf[h, pl.ds(first + k, size), :] = ek.reshape(size, toks)
                mbuf[h, (first + k) // SUB] = new * LOG2E
                total = total * jnp.exp2((top - new) * LOG2E) + jnp.sum(ek, axis=0)
                top = new
        peak = jnp.max(top, axis=0, keepdims=True)
        peak = jnp.maximum(peak[:, :wide], peak[:, wide:])
        peak2 = jnp.concatenate([peak, peak], axis=1)
        total = jnp.sum(total * jnp.exp2((top - peak2) * LOG2E), axis=0, keepdims=True)
        st_tx[0:1, h * wide:(h + 1) * wide] = peak
        st_tx[1:2, h * wide:(h + 1) * wide] = total[:, :wide] + total[:, wide:]

    all_of(lns_o, load_sem.at[3])
    all_of(hid_s.at[pl.ds(0, 2)], near_recv)
    norm(0)
    forward(0)
    all_of(hid_s.at[pl.ds(2, 2)], far_recv)
    norm(1)
    forward(1)
    for r, peer in enumerate(peers):
        send(st_tx, st_rx.at[r], peer, st_send, st_recv)
    all_of(ids_s, ids_recv)

    tgt = jnp.concatenate([ids_s[j, 0] for j in range(n)], axis=1)
    msk = jnp.concatenate([ids_s[j, 1] for j in range(n)], axis=1).astype(F32)
    count = jnp.sum(msk, axis=1, keepdims=True)
    scale = msk / count
    rel = tgt - me * rows
    inside = (rel >= 0) & (rel < rows)
    near = jnp.where(inside, rel, -15000)
    for low, col, size in units:
        et_s[:, pl.ds(col, size)] = e_v[pl.ds(low, size), :].T
    ends = [h * half + subs * SUB for h in range(2)]
    if tail:
        et_s[:, pl.ds(2 * subs * SUB, 2 * tail)] = jnp.concatenate([e_v[pl.ds(low, tail), :] for low in ends], axis=0).T

    flat = jnp.zeros((16, toks), jnp.int32)
    iota16 = lax.broadcasted_iota(jnp.int32, (SUB, toks), 0).astype(jnp.int16).reshape(SUB // 16, 16, toks)

    def hit(low, size):
        return iota16[:size // 16] == (flat + (near - low)).astype(jnp.int16)[None]

    def gather_sum(value):
        accs = [jnp.zeros((dim, toks), F32)] * 2
        groups = [units[i:i + 2] for i in range(0, len(units), 2)]
        if tail:
            groups.append([(low, 2 * subs * SUB + h * tail, tail) for h, low in enumerate(ends)])
        for i, group in enumerate(groups):
            vals = jnp.concatenate([value(low, size) for low, _, size in group], axis=0)
            accs[i % 2] = accs[i % 2] + jnp.dot(et_s[:, pl.ds(group[0][1], vals.shape[0])], vals,
                                                preferred_element_type=F32)
        return accs[0] - accs[1] * -1.0

    ones, none = jnp.ones((1, 16, toks), BF16), jnp.zeros((1, 16, toks), BF16)
    rows_t = gather_sum(lambda low, size: jnp.where(hit(low, size), ones, none).reshape(size, toks))
    cross = jnp.dot(x_v[...], rows_t.astype(BF16), preferred_element_type=F32)
    diag = lax.broadcasted_iota(jnp.int32, (toks, toks), 0) == lax.broadcasted_iota(jnp.int32, (toks, toks), 1)
    tgt_z = jnp.sum(jnp.where(diag, cross, 0.0), axis=0, keepdims=True)
    tgt_z = jnp.where(inside, tgt_z, 0.0)

    all_of(st_rx, st_recv)
    both = [st_tx[...], st_rx[0], swap(st_rx[1]), swap(st_rx[2])]
    peak = jnp.maximum(jnp.maximum(both[0][0:1], both[1][0:1]), jnp.maximum(both[2][0:1], both[3][0:1]))
    sums = [v[1:2] * jnp.exp2((v[0:1] - peak) * LOG2E) for v in both]
    lse = peak + jnp.log((sums[0] + sums[1]) + (sums[2] + sums[3]))
    shift = jnp.broadcast_to(lse * LOG2E - jnp.log2(scale), (8, toks))
    hot_val = (jnp.exp2((tgt_z - lse) * LOG2E) - 1.0) * scale
    hot16 = jnp.broadcast_to(hot_val, (16, toks)).astype(BF16)[None]

    def grads(low, size):
        h, first = low // half, low % half
        sides = slice(h * wide, (h + 1) * wide)
        seen = jnp.concatenate([mbuf[c, first // SUB, :, sides] for c in range(2)], axis=1)
        fac = jnp.exp2(seen - shift)
        ek = jnp.concatenate([ebuf[c, pl.ds(first, size), sides] for c in range(2)], axis=1)
        dz = (ek.reshape(size // 8, 8, toks) * fac[None]).reshape(size // 16, 16, toks).astype(BF16)
        dz = jnp.where(hit(low, size), hot16, dz).reshape(size, toks)
        dz_v[pl.ds(low, size), :] = dz
        return dz

    dx = gather_sum(grads).T
    extra = jnp.concatenate(
        [jnp.sum(dx * xhat_s[...], axis=0, keepdims=True), jnp.sum(dx, axis=0, keepdims=True)]
        + [tgt_z[:, c * dim:(c + 1) * dim] for c in range(toks // dim)]
        + [jnp.zeros((6 - toks // dim, dim), F32)], axis=0)
    dx_s[...] = dx
    for c in range(2):
        pk_tx[c, 0:local, :] = dx_s[pl.ds(pl.multiple_of(c * wide + (1 - core) * local, local), local), :]
        pk_tx[c, local:local + 8, :] = extra
    part = send(pk_tx, pk_rx, peers[0], pk_send, pk_recv)

    own = pl.ds(pl.multiple_of(core * local, local), local)
    xh_o[...] = xhat_s[own, :]
    rs_o[...] = rstd_s[own, :]
    msk_o[...] = msk
    lse_o[...] = lse
    m_copy.wait()
    v_copy.wait()
    for base, size in row_blocks(rows)[:EARLY]:
        adam_rows(base, size, e_v, m_v, v_v, dz_v, x_v, e_v, m_v, v_v, 0)

    part.wait_recv()
    for c, out in enumerate((keep_o, away_o)):
        mine = pl.ds(pl.multiple_of(c * wide + core * local, local), local)
        out[0:local, :] = dx_s[mine, :] + pk_rx[c, 0:local, :]
        out[local:local + 8, :] = extra + pk_rx[c, local:local + 8, :]
    part.wait_send()
    all_of(hid_s.at[pl.ds(0, n - 1)], hid_send)
    all_of(ids_s.at[pl.ds(0, n - 1)], ids_send)
    all_of(st_rx, st_send)


def update_kernel(e_v, m_v, v_v, dz_v, x_v, e_o, m_o, v_o, e_s, m_s, v_s, sem):
    rows = e_v.shape[0]
    blocks = row_blocks(rows)
    shift = blocks[EARLY][0]
    outs = (e_o, m_o, v_o)
    for base, size in blocks[:EARLY]:
        for k, src in enumerate((e_v, m_v, v_v)):
            pltpu.make_async_copy(src.at[pl.ds(base, size)], outs[k].at[pl.ds(base, size)], sem.at[k]).start()
    for base, size in blocks[EARLY:]:
        adam_rows(base, size, e_v, m_v, v_v, dz_v, x_v, e_s, m_s, v_s, shift)
        for k, src in enumerate((e_s, m_s, v_s)):
            pltpu.make_async_copy(
                src.at[pl.ds(base - shift, size)], outs[k].at[pl.ds(base, size)], sem.at[k]).start()
    for k, src in enumerate((e_v, m_v, v_v)):
        pltpu.make_async_copy(src, outs[k], sem.at[k]).wait()


def finish_kernel(n, keep_ref, xh_ref, rs_ref, lse_ref, msk_ref, lns_ref, got_ref,
                  tok_o, mean_o, dh_o, ln_o, lmo, lvo):
    _, core, _ = place()
    local, dim = xh_ref.shape
    wide = n * local // 2
    keep, got = keep_ref[...], got_ref[...]
    both = keep + got
    dx, extra = both[0:local], both[local:local + 8]
    near, far = keep[local + 2:local + 4], got[local + 2:local + 4]
    tgt_z = jnp.concatenate([near[0:1] + far[1:2], near[1:2] + far[0:1]], axis=1)
    msk = msk_ref[...]
    loss = (lse_ref[...] - tgt_z) * msk
    mean_o[...] = jnp.sum(loss[:, :wide] + loss[:, wide:], axis=1, keepdims=True) / jnp.sum(msk, axis=1, keepdims=True)
    tok_o[...] = jnp.where(core == 0, loss[:, :local], loss[:, local:wide])
    xhat = xh_ref[...]
    dxh = dx * lns_ref[0, 0:1, :]
    dh = rs_ref[...] * (dxh - jnp.mean(dxh, axis=-1, keepdims=True)
                        - xhat * jnp.mean(dxh * xhat, axis=-1, keepdims=True))
    dh_o[...] = dh.astype(BF16)
    p_new, m_new, v_new = adam(lns_ref[0], extra[0:2], lns_ref[1], lns_ref[2], 0.0)
    ln_o[...] = p_new
    lmo[...] = m_new
    lvo[...] = v_new


def solution(mesh):
    n = mesh.shape["tp"]
    row_spec = P(("dp", "tp"), None)
    tok_spec = P(("dp", "tp"))
    vocab_spec = P("tp", None)
    repl_spec = P()
    part_spec = P("dp", None)
    vmem = pl.BlockSpec(memory_space=pltpu.VMEM)
    hbm = pl.BlockSpec(memory_space=pltpu.HBM)

    def device_step(hidden, targets, loss_mask, ln_params, out_embed, ln_mom1, ln_mom2, embed_mom1, embed_mom2):
        local, dim = hidden.shape
        rows = out_embed.shape[0]
        toks = n * local
        half = rows // 2
        blocks = row_blocks(rows)
        late = rows - blocks[EARLY][0]
        big = [((rows, dim), BF16), ((rows, dim), F32), ((rows, dim), F32)]
        pack = ((local + 8, dim), F32)
        mid = big + [((rows, toks), BF16), ((toks, dim), BF16), pack, pack, ((local, dim), F32), ((local, dim), F32),
                     ((1, toks), F32), ((1, toks), F32), ((3, 2, dim), F32)]
        small = [((1, local), F32), ((1, 1), F32), ((local, dim), BF16), ((2, dim), F32), ((2, dim), F32),
                 ((2, dim), F32)]
        dma = pltpu.SemaphoreType.DMA
        peers = n - 1
        mids = pl.pallas_call(
            functools.partial(forward_kernel, n),
            name="forward",
            out_shape=[pltpu.VMEM(*s) for s in mid],
            in_specs=[hbm] * 9,
            out_specs=[vmem] * len(mid),
            scratch_shapes=[
                pltpu.VMEM((n, local, dim), BF16), pltpu.VMEM((n, 2, 1, local), jnp.int32),
                pltpu.VMEM((toks, dim), F32), pltpu.VMEM((toks, dim), F32), pltpu.VMEM((toks, dim), F32),
                pltpu.VMEM((2, 2 * dim, toks), BF16), pltpu.VMEM((2, half, toks), F32),
                pltpu.VMEM((2, -(-half // SUB), 8, toks), F32), pltpu.VMEM((dim, -(-rows // 128) * 128), BF16),
                pltpu.VMEM((2, toks), F32), pltpu.VMEM((peers, 2, toks), F32),
                pltpu.VMEM((n // 2, local + 8, dim), F32), pltpu.VMEM((n // 2, local + 8, dim), F32),
                dma((4,)), dma, dma, dma, dma, dma, dma, dma, dma, dma,
            ],
            compiler_params=pltpu.CompilerParams(
                collective_id=0, has_side_effects=True, vmem_limit_bytes=26 << 20),
        )(*[pltpu.with_memory_space_constraint(a, pltpu.HBM) for a in (
            hidden, targets.reshape(1, local), loss_mask.reshape(1, local), ln_params, ln_mom1, ln_mom2,
            out_embed, embed_mom1, embed_mom2)])
        got = lax.ppermute(mids[6], "tp", [(i, (i + n // 2) % n) for i in range(n)])
        e_new, m_new, v_new = pl.pallas_call(
            update_kernel,
            name="update",
            out_shape=[jax.ShapeDtypeStruct(*s) for s in big],
            in_specs=[vmem] * 5,
            out_specs=[hbm] * 3,
            scratch_shapes=[
                pltpu.VMEM((late, dim), BF16), pltpu.VMEM((late, dim), F32), pltpu.VMEM((late, dim), F32),
                dma((3,))],
            compiler_params=pltpu.CompilerParams(vmem_limit_bytes=20 << 20),
            cost_estimate=pl.CostEstimate(flops=50_000_000_000, bytes_accessed=32_000_000, transcendentals=0),
        )(*[pltpu.with_memory_space_constraint(a, pltpu.VMEM) for a in mids[:5]])
        tok, mean, dh, ln_new, lm_new, lv_new = pl.pallas_call(
            functools.partial(finish_kernel, n),
            name="finish",
            out_shape=[jax.ShapeDtypeStruct(*s) for s in small],
            in_specs=[vmem] * 7,
            out_specs=[vmem] * 6,
            compiler_params=pltpu.CompilerParams(vmem_limit_bytes=4 << 20),
        )(mids[5], *mids[7:], got)
        return (tok.reshape(local), mean.reshape(1), dh, ln_new, lm_new, lv_new, e_new, m_new, v_new)

    return jax.shard_map(device_step, mesh=mesh, in_specs=(row_spec, tok_spec, tok_spec, repl_spec, vocab_spec, repl_spec, repl_spec, vocab_spec, vocab_spec), out_specs=(tok_spec, P("dp"), row_spec, part_spec, part_spec, part_spec, row_spec, row_spec, row_spec), check_vma=False)
```

```python
import functools

import jax
import jax.numpy as jnp
from jax import lax
from jax.experimental import pallas as pl
from jax.experimental.pallas import tpu as pltpu
from jax.sharding import PartitionSpec as P

LN_EPS = 1e-5
BETA_ONE = 0.9
BETA_TWO = 0.95
ADAM_EPS = 1e-8
LEARN_RATE = 1e-3
WEIGHT_DECAY = 0.1
ADAM_STEP = 10
LOG2E = 1.4426950408889634
TINY = 1e-37
SUB = 128
CHUNK = 128
EARLY = 14
DOT = 896
MESH = pl.DeviceIdType.MESH
F32 = jnp.float32
BF16 = jnp.bfloat16


def pair_plan(rows):
    half = rows // 2
    return half, half // SUB, half % SUB


def row_blocks(rows):
    full = rows // CHUNK
    return [(i * CHUNK, CHUNK) for i in range(full)] + ([(full * CHUNK, rows - full * CHUNK)] if rows % CHUNK else [])


def adam_const():
    one = 1.0 - BETA_ONE ** ADAM_STEP
    two = 1.0 - BETA_TWO ** ADAM_STEP
    root = two ** 0.5
    return LEARN_RATE * root / one, ADAM_EPS * root


def adam(param, grad, m_old, v_old, decay):
    scale, eps = adam_const()
    m_new = BETA_ONE * m_old + (1.0 - BETA_ONE) * grad
    v_new = BETA_TWO * v_old + ((1.0 - BETA_TWO) * grad) * grad
    root = v_new * lax.rsqrt(v_new + TINY)
    kept = param if decay == 0.0 else (1.0 - LEARN_RATE * decay) * param
    return kept - (scale * m_new) / (root + eps), m_new, v_new


def adam_rows(base, size, e_in, m_in, v_in, dz_v, x_v, e_out, m_out, v_out, shift):
    sl, to = pl.ds(base, size), pl.ds(base - shift, size)
    g = jnp.dot(dz_v[sl, :], x_v[...], preferred_element_type=F32)
    p_new, m_new, v_new = adam(e_in[sl, :].astype(F32), g, m_in[sl, :], v_in[sl, :], WEIGHT_DECAY)
    e_out[to, :] = p_new.astype(BF16)
    m_out[to, :] = m_new
    v_out[to, :] = v_new


def place():
    me = lax.axis_index("tp")
    side, core = me // 2, lax.rem(me, 2)
    far = 2 - 2 * side
    return me, core, (me + 1 - 2 * core, far + core, far + 1 - core)


def swap(v):
    half = v.shape[1] // 2
    return jnp.concatenate([v[:, half:], v[:, :half]], axis=1)


def forward_kernel(n, hid_hbm, tgt_hbm, msk_hbm, ln_hbm, lm_hbm, lv_hbm, e_hbm, m_hbm, v_hbm,
                   e_v, m_v, v_v, dz_v, x_v, keep_o, away_o, xh_o, rs_o, lse_o, msk_o, lns_o,
                   hid_s, ids_s, xhat_s, rstd_s, dx_s, xd_s, ebuf, mbuf, et_s, st_tx, st_rx, pk_tx, pk_rx,
                   load_sem, hid_send, near_recv, far_recv, ids_send, ids_recv, st_send, st_recv, pk_send, pk_recv):
    me, core, peers = place()
    rows, dim = e_v.shape
    local = hid_hbm.shape[0]
    toks = n * local
    wide = toks // 2
    half, subs, tail = pair_plan(rows)
    units = [((i // subs) * half + (i % subs) * SUB, i * SUB, SUB) for i in range(2 * subs)]

    barrier = pltpu.get_barrier_semaphore()
    for peer in peers:
        pl.semaphore_signal(barrier, inc=1, device_id={"tp": peer}, device_id_type=MESH)
    e_copy = pltpu.make_async_copy(e_hbm, e_v, load_sem.at[0])
    m_copy = pltpu.make_async_copy(m_hbm, m_v, load_sem.at[1])
    v_copy = pltpu.make_async_copy(v_hbm, v_v, load_sem.at[2])
    pltpu.make_async_copy(hid_hbm, hid_s.at[core], near_recv).start()
    e_copy.start()
    for k, src in enumerate((ln_hbm, lm_hbm, lv_hbm)):
        pltpu.make_async_copy(src, lns_o.at[k], load_sem.at[3]).start()
    for k, src in enumerate((tgt_hbm, msk_hbm)):
        pltpu.make_async_copy(src, ids_s.at[core, k], ids_recv).start()
    pl.semaphore_wait(barrier, n - 1)

    def send(src, dst, peer, send_sem, recv_sem):
        copy = pltpu.make_async_remote_copy(src_ref=src, dst_ref=dst, send_sem=send_sem, recv_sem=recv_sem,
                                            device_id={"tp": peer}, device_id_type=MESH)
        copy.start()
        return copy

    def all_of(ref, sem):
        pltpu.make_async_copy(ref, ref, sem).wait()

    for r in (1, 2, 0):
        send(hid_hbm, hid_s.at[2 + core if r else core], peers[r], hid_send, far_recv if r else near_recv)
    for k, src in enumerate((tgt_hbm, msk_hbm)):
        for r, peer in enumerate(peers):
            send(src, ids_s.at[2 + core if r else core, k], peer, ids_send, ids_recv)
    xd_s[...] = jnp.zeros(xd_s.shape, BF16)
    e_copy.wait()
    m_copy.start()
    v_copy.start()

    def norm(h):
        lanes = slice(h * wide, (h + 1) * wide)
        hid = hid_s[2 * h:2 * h + 2].reshape(wide, dim).astype(F32)
        cent = hid - jnp.mean(hid, axis=-1, keepdims=True)
        rstd = lax.rsqrt(jnp.mean(cent * cent, axis=-1, keepdims=True) + LN_EPS)
        xhat = cent * rstd
        x_b = (xhat * lns_o[0, 0:1, :] + lns_o[0, 1:2, :]).astype(BF16)
        x_v[lanes, :] = x_b
        xd_s[h, 0:wide, 0:dim] = x_b
        xd_s[h, wide:2 * wide, dim:2 * dim] = x_b
        xhat_s[lanes, :] = xhat
        rstd_s[lanes, :] = jnp.broadcast_to(rstd, (wide, dim))

    def forward(h):
        top = jnp.full((8, toks), -jnp.inf, F32)
        total = jnp.zeros((8, toks), F32)
        for first in range(0, half, DOT):
            span = min(DOT, half - first)
            pair = jnp.concatenate([e_v[pl.ds(first, span), :], e_v[pl.ds(half + first, span), :]], axis=1)
            z = lax.dot_general(pair, xd_s[h], (((1,), (1,)), ((), ())), preferred_element_type=F32)
            for k in range(0, span, SUB):
                size = min(SUB, span - k)
                zk = z[k:k + size].reshape(size // 8, 8, toks)
                new = jnp.maximum(top, jnp.max(zk, axis=0))
                ek = jnp.exp2((zk - new[None]) * LOG2E)
                ebuf[h, pl.ds(first + k, size), :] = ek.reshape(size, toks)
                mbuf[h, (first + k) // SUB] = new * LOG2E
                total = total * jnp.exp2((top - new) * LOG2E) + jnp.sum(ek, axis=0)
                top = new
        peak = jnp.max(top, axis=0, keepdims=True)
        peak = jnp.maximum(peak[:, :wide], peak[:, wide:])
        peak2 = jnp.concatenate([peak, peak], axis=1)
        total = jnp.sum(total * jnp.exp2((top - peak2) * LOG2E), axis=0, keepdims=True)
        st_tx[0:1, h * wide:(h + 1) * wide] = peak
        st_tx[1:2, h * wide:(h + 1) * wide] = total[:, :wide] + total[:, wide:]

    all_of(lns_o, load_sem.at[3])
    all_of(hid_s.at[pl.ds(0, 2)], near_recv)
    norm(0)
    forward(0)
    all_of(hid_s.at[pl.ds(2, 2)], far_recv)
    norm(1)
    forward(1)
    for r in (1, 2, 0):
        send(st_tx, st_rx.at[r], peers[r], st_send, st_recv)
    all_of(ids_s, ids_recv)

    tgt = jnp.concatenate([ids_s[j, 0] for j in range(n)], axis=1)
    msk = jnp.concatenate([ids_s[j, 1] for j in range(n)], axis=1).astype(F32)
    count = jnp.sum(msk, axis=1, keepdims=True)
    scale = msk / count
    rel = tgt - me * rows
    inside = (rel >= 0) & (rel < rows)
    near = jnp.where(inside, rel, -15000)
    for low, col, size in units:
        et_s[:, pl.ds(col, size)] = e_v[pl.ds(low, size), :].T
    ends = [h * half + subs * SUB for h in range(2)]
    if tail:
        et_s[:, pl.ds(2 * subs * SUB, 2 * tail)] = jnp.concatenate([e_v[pl.ds(low, tail), :] for low in ends], axis=0).T

    flat = jnp.zeros((16, toks), jnp.int32)
    iota16 = lax.broadcasted_iota(jnp.int32, (SUB, toks), 0).astype(jnp.int16).reshape(SUB // 16, 16, toks)

    near16 = (flat + near).astype(jnp.int16)

    def hit(low, size):
        return iota16[:size // 16] == (near16 - jnp.int16(low))[None]

    def gather_sum(value):
        accs = [jnp.zeros((dim, toks), F32)] * 2
        groups = [units[i:i + 2] for i in range(0, len(units), 2)]
        if tail:
            groups.append([(low, 2 * subs * SUB + h * tail, tail) for h, low in enumerate(ends)])
        for i, group in enumerate(groups):
            vals = jnp.concatenate([value(low, size) for low, _, size in group], axis=0)
            accs[i % 2] = accs[i % 2] + jnp.dot(et_s[:, pl.ds(group[0][1], vals.shape[0])], vals,
                                                preferred_element_type=F32)
        return accs[0] - accs[1] * -1.0

    ones, none = jnp.ones((1, 16, toks), BF16), jnp.zeros((1, 16, toks), BF16)
    rows_t = gather_sum(lambda low, size: jnp.where(hit(low, size), ones, none).reshape(size, toks))
    cross = jnp.dot(x_v[...], rows_t.astype(BF16), preferred_element_type=F32)
    diag = lax.broadcasted_iota(jnp.int32, (toks, toks), 0) == lax.broadcasted_iota(jnp.int32, (toks, toks), 1)
    tgt_z = jnp.sum(jnp.where(diag, cross, 0.0), axis=0, keepdims=True)
    tgt_z = jnp.where(inside, tgt_z, 0.0)

    all_of(st_rx, st_recv)
    both = [st_tx[...], st_rx[0], swap(st_rx[1]), swap(st_rx[2])]
    peak = jnp.maximum(jnp.maximum(both[0][0:1], both[1][0:1]), jnp.maximum(both[2][0:1], both[3][0:1]))
    sums = [v[1:2] * jnp.exp2((v[0:1] - peak) * LOG2E) for v in both]
    lse = peak + jnp.log((sums[0] + sums[1]) + (sums[2] + sums[3]))
    shift = jnp.broadcast_to(lse * LOG2E - jnp.log2(scale), (8, toks))
    hot_val = (jnp.exp2((tgt_z - lse) * LOG2E) - 1.0) * scale
    hot16 = jnp.broadcast_to(hot_val, (16, toks)).astype(BF16)[None]

    def grads(low, size):
        h, first = low // half, low % half
        sides = slice(h * wide, (h + 1) * wide)
        seen = jnp.concatenate([mbuf[c, first // SUB, :, sides] for c in range(2)], axis=1)
        fac = jnp.exp2(seen - shift)
        ek = jnp.concatenate([ebuf[c, pl.ds(first, size), sides] for c in range(2)], axis=1)
        dz = (ek.reshape(size // 8, 8, toks) * fac[None]).reshape(size // 16, 16, toks).astype(BF16)
        dz = jnp.where(hit(low, size), hot16, dz).reshape(size, toks)
        dz_v[pl.ds(low, size), :] = dz
        return dz

    dx = gather_sum(grads).T
    extra = jnp.concatenate(
        [jnp.sum(dx * xhat_s[...], axis=0, keepdims=True), jnp.sum(dx, axis=0, keepdims=True)]
        + [tgt_z[:, c * dim:(c + 1) * dim] for c in range(toks // dim)]
        + [jnp.zeros((6 - toks // dim, dim), F32)], axis=0)
    dx_s[...] = dx
    for c in range(2):
        pk_tx[c, 0:local, :] = dx_s[pl.ds(pl.multiple_of(c * wide + (1 - core) * local, local), local), :]
        pk_tx[c, local:local + 8, :] = extra
    part = send(pk_tx, pk_rx, peers[0], pk_send, pk_recv)

    own = pl.ds(pl.multiple_of(core * local, local), local)
    xh_o[...] = xhat_s[own, :]
    rs_o[...] = rstd_s[own, :]
    msk_o[...] = msk
    lse_o[...] = lse
    m_copy.wait()
    v_copy.wait()
    for base, size in row_blocks(rows)[:EARLY]:
        adam_rows(base, size, e_v, m_v, v_v, dz_v, x_v, e_v, m_v, v_v, 0)

    part.wait_recv()
    for c, out in enumerate((keep_o, away_o)):
        mine = pl.ds(pl.multiple_of(c * wide + core * local, local), local)
        out[0:local, :] = dx_s[mine, :] + pk_rx[c, 0:local, :]
        out[local:local + 8, :] = extra + pk_rx[c, local:local + 8, :]
    part.wait_send()
    all_of(hid_s.at[pl.ds(0, n - 1)], hid_send)
    all_of(ids_s.at[pl.ds(0, n - 1)], ids_send)
    all_of(st_rx, st_send)


def update_kernel(e_v, m_v, v_v, dz_v, x_v, e_o, m_o, v_o, e_s, m_s, v_s, sem):
    rows = e_v.shape[0]
    blocks = row_blocks(rows)
    shift = blocks[EARLY][0]
    outs = (e_o, m_o, v_o)
    for base, size in blocks[:EARLY]:
        for k, src in enumerate((e_v, m_v, v_v)):
            pltpu.make_async_copy(src.at[pl.ds(base, size)], outs[k].at[pl.ds(base, size)], sem.at[k]).start()
    for base, size in blocks[EARLY:]:
        adam_rows(base, size, e_v, m_v, v_v, dz_v, x_v, e_s, m_s, v_s, shift)
        for k, src in enumerate((e_s, m_s, v_s)):
            pltpu.make_async_copy(
                src.at[pl.ds(base - shift, size)], outs[k].at[pl.ds(base, size)], sem.at[k]).start()
    for k, src in enumerate((e_v, m_v, v_v)):
        pltpu.make_async_copy(src, outs[k], sem.at[k]).wait()


def finish_kernel(n, keep_ref, xh_ref, rs_ref, lse_ref, msk_ref, lns_ref, got_ref,
                  tok_o, mean_o, dh_o, ln_o, lmo, lvo):
    _, core, _ = place()
    local, dim = xh_ref.shape
    wide = n * local // 2
    keep, got = keep_ref[...], got_ref[...]
    both = keep + got
    dx, extra = both[0:local], both[local:local + 8]
    near, far = keep[local + 2:local + 4], got[local + 2:local + 4]
    tgt_z = jnp.concatenate([near[0:1] + far[1:2], near[1:2] + far[0:1]], axis=1)
    msk = msk_ref[...]
    loss = (lse_ref[...] - tgt_z) * msk
    mean_o[...] = jnp.sum(loss[:, :wide] + loss[:, wide:], axis=1, keepdims=True) / jnp.sum(msk, axis=1, keepdims=True)
    tok_o[...] = jnp.where(core == 0, loss[:, :local], loss[:, local:wide])
    xhat = xh_ref[...]
    dxh = dx * lns_ref[0, 0:1, :]
    dh = rs_ref[...] * (dxh - jnp.mean(dxh, axis=-1, keepdims=True)
                        - xhat * jnp.mean(dxh * xhat, axis=-1, keepdims=True))
    dh_o[...] = dh.astype(BF16)
    p_new, m_new, v_new = adam(lns_ref[0], extra[0:2], lns_ref[1], lns_ref[2], 0.0)
    ln_o[...] = p_new
    lmo[...] = m_new
    lvo[...] = v_new


def solution(mesh):
    n = mesh.shape["tp"]
    row_spec = P(("dp", "tp"), None)
    tok_spec = P(("dp", "tp"))
    vocab_spec = P("tp", None)
    repl_spec = P()
    part_spec = P("dp", None)
    vmem = pl.BlockSpec(memory_space=pltpu.VMEM)
    hbm = pl.BlockSpec(memory_space=pltpu.HBM)

    def device_step(hidden, targets, loss_mask, ln_params, out_embed, ln_mom1, ln_mom2, embed_mom1, embed_mom2):
        local, dim = hidden.shape
        rows = out_embed.shape[0]
        toks = n * local
        half = rows // 2
        blocks = row_blocks(rows)
        late = rows - blocks[EARLY][0]
        big = [((rows, dim), BF16), ((rows, dim), F32), ((rows, dim), F32)]
        pack = ((local + 8, dim), F32)
        mid = big + [((rows, toks), BF16), ((toks, dim), BF16), pack, pack, ((local, dim), F32), ((local, dim), F32),
                     ((1, toks), F32), ((1, toks), F32), ((3, 2, dim), F32)]
        small = [((1, local), F32), ((1, 1), F32), ((local, dim), BF16), ((2, dim), F32), ((2, dim), F32),
                 ((2, dim), F32)]
        dma = pltpu.SemaphoreType.DMA
        peers = n - 1
        mids = pl.pallas_call(
            functools.partial(forward_kernel, n),
            name="forward",
            out_shape=[pltpu.VMEM(*s) for s in mid],
            in_specs=[hbm] * 9,
            out_specs=[vmem] * len(mid),
            scratch_shapes=[
                pltpu.VMEM((n, local, dim), BF16), pltpu.VMEM((n, 2, 1, local), jnp.int32),
                pltpu.VMEM((toks, dim), F32), pltpu.VMEM((toks, dim), F32), pltpu.VMEM((toks, dim), F32),
                pltpu.VMEM((2, toks, 2 * dim), BF16), pltpu.VMEM((2, half, toks), F32),
                pltpu.VMEM((2, -(-half // SUB), 8, toks), F32), pltpu.VMEM((dim, -(-rows // 128) * 128), BF16),
                pltpu.VMEM((2, toks), F32), pltpu.VMEM((peers, 2, toks), F32),
                pltpu.VMEM((n // 2, local + 8, dim), F32), pltpu.VMEM((n // 2, local + 8, dim), F32),
                dma((4,)), dma, dma, dma, dma, dma, dma, dma, dma, dma,
            ],
            compiler_params=pltpu.CompilerParams(
                collective_id=0, has_side_effects=True, vmem_limit_bytes=26 << 20),
        )(*[pltpu.with_memory_space_constraint(a, pltpu.HBM) for a in (
            hidden, targets.reshape(1, local), loss_mask.reshape(1, local), ln_params, ln_mom1, ln_mom2,
            out_embed, embed_mom1, embed_mom2)])
        got = lax.ppermute(mids[6], "tp", [(i, (i + n // 2) % n) for i in range(n)])
        e_new, m_new, v_new = pl.pallas_call(
            update_kernel,
            name="update",
            out_shape=[jax.ShapeDtypeStruct(*s) for s in big],
            in_specs=[vmem] * 5,
            out_specs=[hbm] * 3,
            scratch_shapes=[
                pltpu.VMEM((late, dim), BF16), pltpu.VMEM((late, dim), F32), pltpu.VMEM((late, dim), F32),
                dma((3,))],
            compiler_params=pltpu.CompilerParams(vmem_limit_bytes=20 << 20),
            cost_estimate=pl.CostEstimate(flops=50_000_000_000, bytes_accessed=32_000_000, transcendentals=0),
        )(*[pltpu.with_memory_space_constraint(a, pltpu.VMEM) for a in mids[:5]])
        tok, mean, dh, ln_new, lm_new, lv_new = pl.pallas_call(
            functools.partial(finish_kernel, n),
            name="finish",
            out_shape=[jax.ShapeDtypeStruct(*s) for s in small],
            in_specs=[vmem] * 7,
            out_specs=[vmem] * 6,
            compiler_params=pltpu.CompilerParams(vmem_limit_bytes=4 << 20),
        )(mids[5], *mids[7:], got)
        return (tok.reshape(local), mean.reshape(1), dh, ln_new, lm_new, lv_new, e_new, m_new, v_new)

    return jax.shard_map(device_step, mesh=mesh, in_specs=(row_spec, tok_spec, tok_spec, repl_spec, vocab_spec, repl_spec, repl_spec, vocab_spec, vocab_spec), out_specs=(tok_spec, P("dp"), row_spec, part_spec, part_spec, part_spec, row_spec, row_spec, row_spec), check_vma=False)
```

```python
import functools

import jax
import jax.numpy as jnp
from jax import lax
from jax.experimental import pallas as pl
from jax.experimental.pallas import tpu as pltpu
from jax.sharding import PartitionSpec as P

LN_EPS = 1e-5
BETA_ONE = 0.9
BETA_TWO = 0.95
ADAM_EPS = 1e-8
LEARN_RATE = 1e-3
WEIGHT_DECAY = 0.1
ADAM_STEP = 10
LOG2E = 1.4426950408889634
TINY = 1e-37
SUB = 128
CHUNK = 128
EARLY = 14
DOT = 1792
MESH = pl.DeviceIdType.MESH
F32 = jnp.float32
BF16 = jnp.bfloat16


def pair_plan(rows):
    half = rows // 2
    return half, half // SUB, half % SUB


def row_blocks(rows):
    full = rows // CHUNK
    return [(i * CHUNK, CHUNK) for i in range(full)] + ([(full * CHUNK, rows - full * CHUNK)] if rows % CHUNK else [])


def adam_const():
    one = 1.0 - BETA_ONE ** ADAM_STEP
    two = 1.0 - BETA_TWO ** ADAM_STEP
    root = two ** 0.5
    return LEARN_RATE * root / one, ADAM_EPS * root


def adam(param, grad, m_old, v_old, decay):
    scale, eps = adam_const()
    m_new = BETA_ONE * m_old + (1.0 - BETA_ONE) * grad
    v_new = BETA_TWO * v_old + ((1.0 - BETA_TWO) * grad) * grad
    root = v_new * lax.rsqrt(v_new + TINY)
    kept = param if decay == 0.0 else (1.0 - LEARN_RATE * decay) * param
    return kept - (scale * m_new) / (root + eps), m_new, v_new


def adam_rows(base, size, e_in, m_in, v_in, dz_v, x_v, e_out, m_out, v_out, shift):
    sl, to = pl.ds(base, size), pl.ds(base - shift, size)
    g = jnp.dot(dz_v[sl, :], x_v[...], preferred_element_type=F32)
    p_new, m_new, v_new = adam(e_in[sl, :].astype(F32), g, m_in[sl, :], v_in[sl, :], WEIGHT_DECAY)
    e_out[to, :] = p_new.astype(BF16)
    m_out[to, :] = m_new
    v_out[to, :] = v_new


def place():
    me = lax.axis_index("tp")
    side, core = me // 2, lax.rem(me, 2)
    far = 2 - 2 * side
    return me, core, (me + 1 - 2 * core, far + core, far + 1 - core)


def swap(v):
    half = v.shape[1] // 2
    return jnp.concatenate([v[:, half:], v[:, :half]], axis=1)


def forward_kernel(n, hid_hbm, tgt_hbm, msk_hbm, ln_hbm, lm_hbm, lv_hbm, e_hbm, m_hbm, v_hbm,
                   e_v, m_v, v_v, dz_v, x_v, keep_o, away_o, xh_o, rs_o, lse_o, msk_o, lns_o,
                   hid_s, ids_s, xhat_s, rstd_s, dx_s, xd_s, ebuf, mbuf, et_s, st_tx, st_rx, pk_tx, pk_rx,
                   load_sem, hid_send, near_recv, far_recv, ids_send, ids_recv, st_send, st_recv, pk_send, pk_recv):
    me, core, peers = place()
    rows, dim = e_v.shape
    local = hid_hbm.shape[0]
    toks = n * local
    wide = toks // 2
    half, subs, tail = pair_plan(rows)
    units = [((i // subs) * half + (i % subs) * SUB, i * SUB, SUB) for i in range(2 * subs)]

    barrier = pltpu.get_barrier_semaphore()
    for peer in peers:
        pl.semaphore_signal(barrier, inc=1, device_id={"tp": peer}, device_id_type=MESH)
    e_copy = pltpu.make_async_copy(e_hbm, e_v, load_sem.at[0])
    m_copy = pltpu.make_async_copy(m_hbm, m_v, load_sem.at[1])
    v_copy = pltpu.make_async_copy(v_hbm, v_v, load_sem.at[1])
    pltpu.make_async_copy(hid_hbm, hid_s.at[core], near_recv).start()
    e_copy.start()
    for k, src in enumerate((ln_hbm, lm_hbm, lv_hbm)):
        pltpu.make_async_copy(src, lns_o.at[k], load_sem.at[2]).start()
    for k, src in enumerate((tgt_hbm, msk_hbm)):
        pltpu.make_async_copy(src, ids_s.at[core, k], ids_recv).start()
    pl.semaphore_wait(barrier, n - 1)

    def send(src, dst, peer, send_sem, recv_sem):
        copy = pltpu.make_async_remote_copy(src_ref=src, dst_ref=dst, send_sem=send_sem, recv_sem=recv_sem,
                                            device_id={"tp": peer}, device_id_type=MESH)
        copy.start()
        return copy

    def all_of(ref, sem):
        pltpu.make_async_copy(ref, ref, sem).wait()

    for r in (1, 2, 0):
        send(hid_hbm, hid_s.at[2 + core if r else core], peers[r], hid_send, far_recv if r else near_recv)
    for k, src in enumerate((tgt_hbm, msk_hbm)):
        for r, peer in enumerate(peers):
            send(src, ids_s.at[2 + core if r else core, k], peer, ids_send, ids_recv)
    xd_s[...] = jnp.zeros(xd_s.shape, BF16)
    e_copy.wait()
    m_copy.start()
    v_copy.start()

    def norm(h):
        lanes = slice(h * wide, (h + 1) * wide)
        hid = hid_s[2 * h:2 * h + 2].reshape(wide, dim).astype(F32)
        cent = hid - jnp.mean(hid, axis=-1, keepdims=True)
        rstd = lax.rsqrt(jnp.mean(cent * cent, axis=-1, keepdims=True) + LN_EPS)
        xhat = cent * rstd
        x_b = (xhat * lns_o[0, 0:1, :] + lns_o[0, 1:2, :]).astype(BF16)
        x_v[lanes, :] = x_b
        xd_s[h, 0:wide, 0:dim] = x_b
        xd_s[h, wide:2 * wide, dim:2 * dim] = x_b
        xhat_s[lanes, :] = xhat
        rstd_s[lanes, :] = jnp.broadcast_to(rstd, (wide, dim))

    def forward(h):
        top = jnp.full((8, toks), -jnp.inf, F32)
        total = jnp.zeros((8, toks), F32)
        for first in range(0, half, DOT):
            span = min(DOT, half - first)
            pair = jnp.concatenate([e_v[pl.ds(first, span), :], e_v[pl.ds(half + first, span), :]], axis=1)
            z = lax.dot_general(pair, xd_s[h], (((1,), (1,)), ((), ())), preferred_element_type=F32)
            for k in range(0, span, SUB):
                size = min(SUB, span - k)
                zk = z[k:k + size].reshape(size // 8, 8, toks)
                new = jnp.maximum(top, jnp.max(zk, axis=0))
                ek = jnp.exp2((zk - new[None]) * LOG2E)
                ebuf[h, pl.ds(first + k, size), :] = ek.reshape(size, toks)
                mbuf[h, (first + k) // SUB] = new * LOG2E
                total = total * jnp.exp2((top - new) * LOG2E) + jnp.sum(ek, axis=0)
                top = new
        peak = jnp.max(top, axis=0, keepdims=True)
        peak = jnp.maximum(peak[:, :wide], peak[:, wide:])
        peak2 = jnp.concatenate([peak, peak], axis=1)
        total = jnp.sum(total * jnp.exp2((top - peak2) * LOG2E), axis=0, keepdims=True)
        st_tx[0:1, h * wide:(h + 1) * wide] = peak
        st_tx[1:2, h * wide:(h + 1) * wide] = total[:, :wide] + total[:, wide:]

    all_of(lns_o, load_sem.at[2])
    all_of(hid_s.at[pl.ds(0, 2)], near_recv)
    norm(0)
    forward(0)
    all_of(hid_s.at[pl.ds(2, 2)], far_recv)
    norm(1)
    forward(1)
    for r in (1, 2, 0):
        send(st_tx, st_rx.at[r], peers[r], st_send, st_recv)
    all_of(ids_s, ids_recv)

    tgt = jnp.concatenate([ids_s[j, 0] for j in range(n)], axis=1)
    msk = jnp.concatenate([ids_s[j, 1] for j in range(n)], axis=1).astype(F32)
    count = jnp.sum(msk, axis=1, keepdims=True)
    scale = msk / count
    rel = tgt - me * rows
    inside = (rel >= 0) & (rel < rows)
    near = jnp.where(inside, rel, -15000)
    for low, col, size in units:
        et_s[:, pl.ds(col, size)] = e_v[pl.ds(low, size), :].T
    ends = [h * half + subs * SUB for h in range(2)]
    if tail:
        et_s[:, pl.ds(2 * subs * SUB, 2 * tail)] = jnp.concatenate([e_v[pl.ds(low, tail), :] for low in ends], axis=0).T

    flat = jnp.zeros((16, toks), jnp.int32)
    iota16 = lax.broadcasted_iota(jnp.int32, (SUB, toks), 0).astype(jnp.int16).reshape(SUB // 16, 16, toks)

    near16 = (flat + near).astype(jnp.int16)

    def hit(low, size):
        return iota16[:size // 16] == (near16 - jnp.int16(low))[None]

    def gather_sum(value):
        accs = [jnp.zeros((dim, toks), F32)] * 2
        groups = [units[i:i + 2] for i in range(0, len(units), 2)]
        if tail:
            groups.append([(low, 2 * subs * SUB + h * tail, tail) for h, low in enumerate(ends)])
        for i, group in enumerate(groups):
            vals = jnp.concatenate([value(low, size) for low, _, size in group], axis=0)
            accs[i % 2] = accs[i % 2] + jnp.dot(et_s[:, pl.ds(group[0][1], vals.shape[0])], vals,
                                                preferred_element_type=F32)
        return accs[0] - accs[1] * -1.0

    ones, none = jnp.ones((1, 16, toks), BF16), jnp.zeros((1, 16, toks), BF16)
    rows_t = gather_sum(lambda low, size: jnp.where(hit(low, size), ones, none).reshape(size, toks))
    cross = jnp.dot(x_v[...], rows_t.astype(BF16), preferred_element_type=F32)
    diag = lax.broadcasted_iota(jnp.int32, (toks, toks), 0) == lax.broadcasted_iota(jnp.int32, (toks, toks), 1)
    tgt_z = jnp.sum(jnp.where(diag, cross, 0.0), axis=0, keepdims=True)
    tgt_z = jnp.where(inside, tgt_z, 0.0)

    all_of(st_rx, st_recv)
    both = [st_tx[...], st_rx[0], swap(st_rx[1]), swap(st_rx[2])]
    peak = jnp.maximum(jnp.maximum(both[0][0:1], both[1][0:1]), jnp.maximum(both[2][0:1], both[3][0:1]))
    sums = [v[1:2] * jnp.exp2((v[0:1] - peak) * LOG2E) for v in both]
    lse = peak + jnp.log((sums[0] + sums[1]) + (sums[2] + sums[3]))
    shift = jnp.broadcast_to(lse * LOG2E - jnp.log2(scale), (8, toks))
    hot_val = (jnp.exp2((tgt_z - lse) * LOG2E) - 1.0) * scale
    hot16 = jnp.broadcast_to(hot_val, (16, toks)).astype(BF16)[None]

    def grads(low, size):
        h, first = low // half, low % half
        sides = slice(h * wide, (h + 1) * wide)
        seen = jnp.concatenate([mbuf[c, first // SUB, :, sides] for c in range(2)], axis=1)
        fac = jnp.exp2(seen - shift)
        ek = jnp.concatenate([ebuf[c, pl.ds(first, size), sides] for c in range(2)], axis=1)
        dz = (ek.reshape(size // 8, 8, toks) * fac[None]).reshape(size // 16, 16, toks).astype(BF16)
        dz = jnp.where(hit(low, size), hot16, dz).reshape(size, toks)
        dz_v[pl.ds(low, size), :] = dz
        return dz

    dx = gather_sum(grads).T
    extra = jnp.concatenate(
        [jnp.sum(dx * xhat_s[...], axis=0, keepdims=True), jnp.sum(dx, axis=0, keepdims=True)]
        + [tgt_z[:, c * dim:(c + 1) * dim] for c in range(toks // dim)]
        + [jnp.zeros((6 - toks // dim, dim), F32)], axis=0)
    dx_s[...] = dx
    for c in range(2):
        pk_tx[c, 0:local, :] = dx_s[pl.ds(pl.multiple_of(c * wide + (1 - core) * local, local), local), :]
        pk_tx[c, local:local + 8, :] = extra
    part = send(pk_tx, pk_rx, peers[0], pk_send, pk_recv)

    own = pl.ds(pl.multiple_of(core * local, local), local)
    xh_o[...] = xhat_s[own, :]
    rs_o[...] = rstd_s[own, :]
    msk_o[...] = msk
    lse_o[...] = lse
    all_of(ebuf, load_sem.at[1])
    for base, size in row_blocks(rows)[:EARLY]:
        adam_rows(base, size, e_v, m_v, v_v, dz_v, x_v, e_v, m_v, v_v, 0)

    part.wait_recv()
    for c, out in enumerate((keep_o, away_o)):
        mine = pl.ds(pl.multiple_of(c * wide + core * local, local), local)
        out[0:local, :] = dx_s[mine, :] + pk_rx[c, 0:local, :]
        out[local:local + 8, :] = extra + pk_rx[c, local:local + 8, :]
    part.wait_send()
    all_of(hid_s.at[pl.ds(0, n - 1)], hid_send)
    all_of(ids_s.at[pl.ds(0, n - 1)], ids_send)
    all_of(st_rx, st_send)


def update_kernel(e_v, m_v, v_v, dz_v, x_v, e_o, m_o, v_o, e_s, m_s, v_s, sem):
    rows = e_v.shape[0]
    blocks = row_blocks(rows)
    shift = blocks[EARLY][0]
    outs = (e_o, m_o, v_o)
    for base, size in blocks[:EARLY]:
        for k, src in enumerate((e_v, m_v, v_v)):
            pltpu.make_async_copy(src.at[pl.ds(base, size)], outs[k].at[pl.ds(base, size)], sem.at[k]).start()
    for base, size in blocks[EARLY:]:
        adam_rows(base, size, e_v, m_v, v_v, dz_v, x_v, e_s, m_s, v_s, shift)
        for k, src in enumerate((e_s, m_s, v_s)):
            pltpu.make_async_copy(
                src.at[pl.ds(base - shift, size)], outs[k].at[pl.ds(base, size)], sem.at[k]).start()
    for k, src in enumerate((e_v, m_v, v_v)):
        pltpu.make_async_copy(src, outs[k], sem.at[k]).wait()


def finish_kernel(n, keep_ref, xh_ref, rs_ref, lse_ref, msk_ref, lns_ref, got_ref,
                  tok_o, mean_o, dh_o, ln_o, lmo, lvo):
    _, core, _ = place()
    local, dim = xh_ref.shape
    wide = n * local // 2
    keep, got = keep_ref[...], got_ref[...]
    both = keep + got
    dx, extra = both[0:local], both[local:local + 8]
    near, far = keep[local + 2:local + 4], got[local + 2:local + 4]
    tgt_z = jnp.concatenate([near[0:1] + far[1:2], near[1:2] + far[0:1]], axis=1)
    msk = msk_ref[...]
    loss = (lse_ref[...] - tgt_z) * msk
    mean_o[...] = jnp.sum(loss[:, :wide] + loss[:, wide:], axis=1, keepdims=True) / jnp.sum(msk, axis=1, keepdims=True)
    tok_o[...] = jnp.where(core == 0, loss[:, :local], loss[:, local:wide])
    xhat = xh_ref[...]
    dxh = dx * lns_ref[0, 0:1, :]
    dh = rs_ref[...] * (dxh - jnp.mean(dxh, axis=-1, keepdims=True)
                        - xhat * jnp.mean(dxh * xhat, axis=-1, keepdims=True))
    dh_o[...] = dh.astype(BF16)
    p_new, m_new, v_new = adam(lns_ref[0], extra[0:2], lns_ref[1], lns_ref[2], 0.0)
    ln_o[...] = p_new
    lmo[...] = m_new
    lvo[...] = v_new


def solution(mesh):
    n = mesh.shape["tp"]
    row_spec = P(("dp", "tp"), None)
    tok_spec = P(("dp", "tp"))
    vocab_spec = P("tp", None)
    repl_spec = P()
    part_spec = P("dp", None)
    vmem = pl.BlockSpec(memory_space=pltpu.VMEM)
    hbm = pl.BlockSpec(memory_space=pltpu.HBM)

    def device_step(hidden, targets, loss_mask, ln_params, out_embed, ln_mom1, ln_mom2, embed_mom1, embed_mom2):
        local, dim = hidden.shape
        rows = out_embed.shape[0]
        toks = n * local
        half = rows // 2
        blocks = row_blocks(rows)
        late = rows - blocks[EARLY][0]
        big = [((rows, dim), BF16), ((rows, dim), F32), ((rows, dim), F32)]
        pack = ((local + 8, dim), F32)
        mid = big + [((rows, toks), BF16), ((toks, dim), BF16), pack, pack, ((local, dim), F32), ((local, dim), F32),
                     ((1, toks), F32), ((1, toks), F32), ((3, 2, dim), F32)]
        small = [((1, local), F32), ((1, 1), F32), ((local, dim), BF16), ((2, dim), F32), ((2, dim), F32),
                 ((2, dim), F32)]
        dma = pltpu.SemaphoreType.DMA
        peers = n - 1
        mids = pl.pallas_call(
            functools.partial(forward_kernel, n),
            name="forward",
            out_shape=[pltpu.VMEM(*s) for s in mid],
            in_specs=[hbm] * 9,
            out_specs=[vmem] * len(mid),
            scratch_shapes=[
                pltpu.VMEM((n, local, dim), BF16), pltpu.VMEM((n, 2, 1, local), jnp.int32),
                pltpu.VMEM((toks, dim), F32), pltpu.VMEM((toks, dim), F32), pltpu.VMEM((toks, dim), F32),
                pltpu.VMEM((2, toks, 2 * dim), BF16), pltpu.VMEM((2, half, toks), F32),
                pltpu.VMEM((2, -(-half // SUB), 8, toks), F32), pltpu.VMEM((dim, -(-rows // 128) * 128), BF16),
                pltpu.VMEM((2, toks), F32), pltpu.VMEM((peers, 2, toks), F32),
                pltpu.VMEM((n // 2, local + 8, dim), F32), pltpu.VMEM((n // 2, local + 8, dim), F32),
                dma((3,)), dma, dma, dma, dma, dma, dma, dma, dma, dma,
            ],
            compiler_params=pltpu.CompilerParams(
                collective_id=0, has_side_effects=True, vmem_limit_bytes=26 << 20),
        )(*[pltpu.with_memory_space_constraint(a, pltpu.HBM) for a in (
            hidden, targets.reshape(1, local), loss_mask.reshape(1, local), ln_params, ln_mom1, ln_mom2,
            out_embed, embed_mom1, embed_mom2)])
        got = lax.ppermute(mids[6], "tp", [(i, (i + n // 2) % n) for i in range(n)])
        e_new, m_new, v_new = pl.pallas_call(
            update_kernel,
            name="update",
            out_shape=[jax.ShapeDtypeStruct(*s) for s in big],
            in_specs=[vmem] * 5,
            out_specs=[hbm] * 3,
            scratch_shapes=[
                pltpu.VMEM((late, dim), BF16), pltpu.VMEM((late, dim), F32), pltpu.VMEM((late, dim), F32),
                dma((3,))],
            compiler_params=pltpu.CompilerParams(vmem_limit_bytes=20 << 20),
            cost_estimate=pl.CostEstimate(flops=50_000_000_000, bytes_accessed=32_000_000, transcendentals=0),
        )(*[pltpu.with_memory_space_constraint(a, pltpu.VMEM) for a in mids[:5]])
        tok, mean, dh, ln_new, lm_new, lv_new = pl.pallas_call(
            functools.partial(finish_kernel, n),
            name="finish",
            out_shape=[jax.ShapeDtypeStruct(*s) for s in small],
            in_specs=[vmem] * 7,
            out_specs=[vmem] * 6,
            compiler_params=pltpu.CompilerParams(vmem_limit_bytes=4 << 20),
        )(mids[5], *mids[7:], got)
        return (tok.reshape(local), mean.reshape(1), dh, ln_new, lm_new, lv_new, e_new, m_new, v_new)

    return jax.shard_map(device_step, mesh=mesh, in_specs=(row_spec, tok_spec, tok_spec, repl_spec, vocab_spec, repl_spec, repl_spec, vocab_spec, vocab_spec), out_specs=(tok_spec, P("dp"), row_spec, part_spec, part_spec, part_spec, row_spec, row_spec, row_spec), check_vma=False)
```
